128 devices in a mesh: tile: 32 (over x, z, core), dir: 4 (over y).
Axes of the slice: x: 4, y: 4, z: 4, core: 2. Of those that a mesh axis runs over, the one named last changes fastest.
Arguments:
- probes: float32 [32, 256, 32, 128], P('dir', 'tile'), may hold values from -6 to 6
- base_sens: float32 [256, 32, 128], P('tile'), may hold values from -12 to 12
- obs_weight: float32 [256, 32, 128], P('tile'), may hold values from 1 to 10
- perm: float32 [256, 32, 128], P('tile'), may hold values from 0.25 to 4
- material: int32 [256, 32, 128], P('tile'), may hold values from 0 to 7
- class_storage: float32 [8], replicated, may hold values from 0.2 to 2
- class_alpha: float32 [8], replicated, may hold values from 0.5 to 1
- class_bulk: float32 [8], replicated, may hold values from 0.25 to 2
- class_shear: float32 [8], replicated, may hold values from 0.5 to 4
Outputs:
- hess_block: float32 [32, 256, 32, 128], P('dir', 'tile')
- r_factor: float32 [32, 32], replicated
The draws below stay inside these ranges and needn't reach their ends.
All inputs are finite; a program needn't handle non-finite values.
Results may differ from the reference program's by a relative error of at most 0.00016.
Values sent between devices are 32-bit elements; how exact they have to be, the bound alone decides.
A program may use at most 64 MiB of HBM per device.

```python
import math
import jax
import jax.numpy as jnp
from jax import lax

NY = 32
NZ = 128
DIR_DEV = 8
NCLASS = 8
SWEEPS = 2
STEPS = 2
NX = 256
DIRS = 32


def with_ends(drawn, key, low, largest):
    extent = drawn.shape
    index_at = [jax.random.randint(jax.random.fold_in(key, axis), (), 0, extent[axis]) for axis in range(len(extent))]
    drawn = drawn.at[tuple(index_at)].set(low)
    longest = extent.index(max(extent))
    index_at[longest] = (index_at[longest] + 1) % extent[longest]
    return drawn.at[tuple(index_at)].set(largest)


def shard_levels(own_key, shape, split, low, high):
    level = 1.0
    for dim, parts in split:
        steps = jax.random.uniform(jax.random.fold_in(jax.random.fold_in(own_key, 6), dim), (parts,), jnp.float32, low / len(split), high / len(split))
        level = level * jnp.repeat(jnp.exp(steps), shape[dim] // parts).reshape((-1,) + (1,) * (len(shape) - 1 - dim))
    return level


def scatter_about(rng, dims, scale, bound, split=(), kind=jnp.bfloat16):
    level = shard_levels(rng, dims, split, -0.22, 0.18) if split else 1.0
    drawn = jax.random.normal(rng, dims, jnp.float32) * scale * level
    return jnp.minimum(jnp.maximum(drawn, -bound), bound).astype(kind)


def setup_inputs(seed: int = 0) -> dict:
    seeds = jax.random.split(jax.random.key(seed), 10)
    probes = scatter_about(seeds[0], (DIRS, NX, NY, NZ), 1.0, 6.0, ((0, 4), (1, 32)), jnp.float32)
    base_sens = scatter_about(seeds[1], (NX, NY, NZ), 2.0, 12.0, ((0, 32),), jnp.float32)
    obs_weight = jnp.clip(jnp.exp(math.log(10.0) - 2.3025851 * jax.random.uniform(seeds[2], (NX, NY, NZ), jnp.float32) ** shard_levels(seeds[2], (NX, NY, NZ), ((0, 32),), -0.2, 0.2)), 1.0, 10.0)
    perm = jnp.clip(jnp.exp(math.log(4.0) - 2.7725887 * jax.random.uniform(seeds[3], (NX, NY, NZ), jnp.float32) ** shard_levels(seeds[3], (NX, NY, NZ), ((0, 32),), -0.2, 0.2)), 0.25, 4.0)
    material = with_ends(jax.random.randint(seeds[4], (NX, NY, NZ), 0, NCLASS), jax.random.fold_in(seeds[4], 1), 0, NCLASS - 1).astype(jnp.int32)
    class_storage = jnp.clip(jnp.exp(jax.random.uniform(seeds[5], (NCLASS,), jnp.float32, math.log(0.2), math.log(2.0))), 0.2, 2.0)
    class_alpha = jnp.clip(jax.random.uniform(seeds[6], (NCLASS,), jnp.float32, 0.5, 1.0), 0.5, 1.0)
    class_bulk = jnp.clip(jnp.exp(jax.random.uniform(seeds[7], (NCLASS,), jnp.float32, math.log(0.25), math.log(2.0))), 0.25, 2.0)
    class_shear = jnp.clip(jnp.exp(jax.random.uniform(seeds[8], (NCLASS,), jnp.float32, math.log(0.5), math.log(4.0))), 0.5, 4.0)
    return {"probes": probes, "base_sens": base_sens, "obs_weight": obs_weight, "perm": perm, "material": material, "class_storage": class_storage, "class_alpha": class_alpha, "class_bulk": class_bulk, "class_shear": class_shear}


def pad_first(field):
    return jnp.pad(field, [(0, 0)] * (field.ndim - 3) + [(1, 1), (0, 0), (0, 0)])

def pad_second(field):
    return jnp.pad(field, [(0, 0)] * (field.ndim - 2) + [(1, 1), (0, 0)])

def pad_third(field):
    return jnp.pad(field, [(0, 0)] * (field.ndim - 1) + [(1, 1)])

def face_flux(padded, coef_pad):
    center = padded[..., 1:-1, :, :]
    coef_mid = coef_pad[1:-1]
    result = 0.5 * (coef_mid + coef_pad[2:]) * (center - padded[..., 2:, :, :])
    result = result + 0.5 * (coef_mid + coef_pad[:-2]) * (center - padded[..., :-2, :, :])
    field_y = pad_second(center)
    coef_y = pad_second(coef_mid)
    result = result + 0.5 * (coef_mid + coef_y[:, 2:]) * (center - field_y[..., 2:, :])
    result = result + 0.5 * (coef_mid + coef_y[:, :-2]) * (center - field_y[..., :-2, :])
    field_z = pad_third(center)
    coef_z = pad_third(coef_mid)
    result = result + 0.5 * (coef_mid + coef_z[:, :, 2:]) * (center - field_z[..., 2:])
    result = result + 0.5 * (coef_mid + coef_z[:, :, :-2]) * (center - field_z[..., :-2])
    return result

def gradient(press_pad, biot):
    first = 0.5 * biot * (press_pad[..., 2:, :, :] - press_pad[..., :-2, :, :])
    center = press_pad[..., 1:-1, :, :]
    field_y = pad_second(center)
    second = 0.5 * biot * (field_y[..., 2:, :] - field_y[..., :-2, :])
    field_z = pad_third(center)
    third = 0.5 * biot * (field_z[..., 2:] - field_z[..., :-2])
    return jnp.stack([first, second, third])

def divergence(first_pad, others, biot_pad):
    weighted = biot_pad * first_pad
    result = 0.5 * (weighted[..., :-2, :, :] - weighted[..., 2:, :, :])
    biot = biot_pad[1:-1]
    second = pad_second(biot * others[0])
    result = result + 0.5 * (second[..., :-2, :] - second[..., 2:, :])
    third = pad_third(biot * others[1])
    result = result + 0.5 * (third[..., :-2] - third[..., 2:])
    return result

def inner(left, right):
    summed = lax.optimization_barrier(jnp.sum(left * right, axis=(-3, -2, -1)))
    if summed.ndim == 2:
        summed = lax.optimization_barrier(jnp.sum(summed, axis=0))
    return summed

def spread(values):
    return values[:, None, None, None]

def conj_grad(operate, target, iterate):
    if iterate is None:
        residual = target
        iterate = jnp.zeros_like(target)
    else:
        residual = target - operate(pad_first(iterate))
    direction = residual
    norm_now = inner(residual, residual)
    for step in range(STEPS):
        image = operate(pad_first(direction))
        step_len = norm_now / inner(direction, image)
        iterate = iterate + spread(step_len) * direction
        if step + 1 < STEPS:
            residual = residual - spread(step_len) * image
            norm_next = inner(residual, residual)
            direction = residual + spread(norm_next / norm_now) * direction
            norm_now = norm_next
    return iterate

def solve(source, orient, tables):
    perm_pad, biot, biot_pad, shear_pad, stab_term, diagonal = tables

    def press_apply(padded):
        return diagonal * padded[..., 1:-1, :, :] + face_flux(padded, perm_pad)

    def elast_apply(padded):
        return face_flux(padded, shear_pad)
    pressure = None
    displace = None
    for sweep in range(SWEEPS):
        source_term = source
        if displace is not None:
            source_term = source - orient * divergence(pad_first(displace[0]), (displace[1], displace[2]), biot_pad) + stab_term * pressure
        pressure = conj_grad(press_apply, source_term, pressure)
        elastic_term = orient * gradient(pad_first(pressure), biot)
        displace = conj_grad(elast_apply, elastic_term, displace)
    return pressure

def reference(probes, base_sens, obs_weight, perm, material, class_storage, class_alpha, class_bulk, class_shear):
    class_mask = (material[None] == jnp.arange(NCLASS, dtype=jnp.int32)[:, None, None, None]).astype(jnp.float32)
    storage = lax.optimization_barrier(jnp.sum(class_storage[:, None, None, None] * class_mask, axis=0))
    biot = lax.optimization_barrier(jnp.sum(class_alpha[:, None, None, None] * class_mask, axis=0))
    bulk = lax.optimization_barrier(jnp.sum(class_bulk[:, None, None, None] * class_mask, axis=0))
    shear = lax.optimization_barrier(jnp.sum(class_shear[:, None, None, None] * class_mask, axis=0))
    stab_term = biot * biot / bulk
    diagonal = storage + stab_term
    tables = (pad_first(perm), biot, pad_first(biot), pad_first(shear), stab_term, diagonal)

    def one_block(probe_block):
        tangent = solve(base_sens * probe_block, 1.0, tables)
        adjoint = solve(obs_weight * tangent, -1.0, tables)
        return base_sens * adjoint
    blocks = probes.reshape((-1, DIR_DEV) + probes.shape[1:])
    hess_block = lax.map(one_block, blocks).reshape(probes.shape)
    columns = hess_block.reshape(DIRS, -1)
    gram = jnp.dot(columns.astype(jnp.float32), columns.T.astype(jnp.float32), precision=lax.Precision.HIGHEST, preferred_element_type=jnp.float32) / (NX * NY * NZ)
    r_factor = jnp.linalg.cholesky(gram).T
    return (hess_block, r_factor)
```

```python
import functools

import jax
import jax.numpy as jnp
from jax import lax
from jax.experimental import pallas as pl
from jax.experimental.pallas import tpu as pltpu
from jax.sharding import PartitionSpec as P

MESH = pl.DeviceIdType.MESH
F32 = jnp.float32
NCLASS = 8
LANES = 128
SUB = 8
OWN = 8
NL = 16
K = 7
O = K
E = K + NL
LT = NL + 2 * K
HV = 2
ND = SUB // HV
NEAR = 2
NRED = 6


def kernel(
    ns,
    nd,
    cells,
    probes,
    bs_in,
    obs_in,
    perm_in,
    mat_in,
    t_storage,
    t_alpha,
    t_bulk,
    t_shear,
    hess,
    gram,
    praw,
    c_bs,
    c_obs,
    c_perm,
    c_mat,
    c_diag,
    c_stab,
    c_hb,
    c_shear,
    c_tmp,
    pd,
    px,
    py,
    pz,
    pm,
    ed,
    ex,
    ey,
    ez,
    em,
    hb,
    st,
    f,
    w,
    v,
    p1,
    b,
    we,
    r2,
    w2,
    ybuf,
    hraw,
    grecv,
    red_src,
    red_buf,
    ga_src,
    ga_buf,
    gb_src,
    gb_buf,
    sem_init_send,
    sem_part,
    sem_halo,
    sem_loc,
    sem_red_send,
    sem_red,
    sem_ga_send,
    sem_ga,
    sem_gb_send,
    sem_gb,
    sem_g_send,
    sem_g,
    sem_h,
    sem_f_send,
    sem_f,
):
    yh = probes.shape[2] // HV
    ny = probes.shape[2]
    t = lax.axis_index("tile")
    d = lax.axis_index("dir")
    s = t // 2
    c = lax.rem(t, 2)
    partner = s * 2 + (1 - c)
    has_low = s > 0
    has_high = s < ns - 1

    barrier = pltpu.get_barrier_semaphore()

    def greet(tile, dr):
        pl.semaphore_signal(barrier, inc=1, device_id=(tile, dr), device_id_type=MESH)

    for j in range(1, ns):
        greet(lax.rem(s + j, ns) * 2 + c, d)
    greet(partner, d)
    for j in range(1, nd):
        dj = lax.rem(d + j, nd)
        greet(t, dj)
        greet(partner, dj)
    cross = jnp.where(c == 0, s - 1, s + 1)
    has_cross = jnp.where(c == 0, has_low, has_high)

    @pl.when(has_cross)
    def _():
        greet(cross * 2 + (1 - c), d)

    own_at = O + OWN * c
    locals_ = []
    for i, (src, dst) in enumerate(
        (
            (probes.at[pl.ds(ND * c, ND)], praw.at[:, pl.ds(own_at, OWN)]),
            (perm_in, c_perm.at[pl.ds(own_at, OWN)]),
            (mat_in, c_mat.at[pl.ds(own_at, OWN)]),
            (bs_in, c_bs.at[pl.ds(own_at, OWN)]),
            (obs_in, c_obs.at[pl.ds(own_at, OWN)]),
        )
    ):
        cp = pltpu.make_async_copy(src, dst, sem_loc.at[i])
        cp.start()
        locals_.append(cp)

    zero8 = jnp.zeros((SUB, LANES), F32)
    zc = jnp.zeros((ny, LANES), F32)
    zi = jnp.zeros((ny, LANES), jnp.int32)

    def zero_side(lo):
        def layer(i, carry):
            l = lo + i
            for ref in (c_perm, c_bs):
                ref[l] = zc
            c_mat[l] = zi
            for dd in range(ND):
                praw[dd, l] = zc
            for y in range(yh):
                w[l, y] = zero8
                v[l, y] = zero8
                r2[l, y] = zero8
                w2[l, y] = zero8
                for k in range(3):
                    we[k, l, y] = zero8
            return carry

        lax.fori_loop(0, K, layer, 0)

    @pl.when(jnp.logical_not(has_low))
    def _():
        zero_side(0)
        for i in range(NEAR):
            c_obs[O - 1 - i] = zc

    @pl.when(jnp.logical_not(has_high))
    def _():
        zero_side(E)
        for i in range(NEAR):
            c_obs[E + i] = zc

    pl.semaphore_wait(barrier, (ns - 1) + 1 + 2 * (nd - 1) + jnp.where(has_cross, 1, 0))

    def remote(src, dst, ssem, rsem, tile, dr):
        return pltpu.make_async_remote_copy(
            src_ref=src,
            dst_ref=dst,
            send_sem=ssem,
            recv_sem=rsem,
            device_id=(tile, dr),
            device_id_type=MESH,
        )

    part = [
        remote(
            probes.at[pl.ds(ND * (1 - c), ND)],
            praw.at[:, pl.ds(own_at, OWN)],
            sem_init_send.at[0],
            sem_part.at[0],
            partner,
            d,
        )
    ]
    for i, (src, dst) in enumerate(
        ((perm_in, c_perm), (mat_in, c_mat), (bs_in, c_bs), (obs_in, c_obs))
    ):
        part.append(
            remote(
                src,
                dst.at[pl.ds(own_at, OWN)],
                sem_init_send.at[1 + i],
                sem_part.at[1 + i],
                partner,
                d,
            )
        )
    for cp in part:
        cp.start()

    side = 1 - c

    def halo_copies(side, src_near, dst_near, src_far, dst_far, slab):
        out = []
        n = 0
        for far in (False, True):
            at, to, size = (src_far, dst_far, K - NEAR) if far else (src_near, dst_near, NEAR)
            m = 0
            for src, dst in (
                (perm_in, c_perm),
                (mat_in, c_mat),
                (bs_in, c_bs),
                (None, praw),
                (obs_in, c_obs),
            ):
                if far and src is obs_in:
                    continue
                for core in range(2):
                    if src is None:
                        a = probes.at[pl.ds(ND * core, ND), pl.ds(at, size)]
                        z = praw.at[:, pl.ds(to, size)]
                    else:
                        a = src.at[pl.ds(at, size)]
                        z = dst.at[pl.ds(to, size)]
                    out.append(
                        (
                            core,
                            far,
                            remote(
                                a,
                                z,
                                sem_init_send.at[5 + n],
                                sem_halo.at[side, (5 if far else 0) + m],
                                slab * 2 + core,
                                d,
                            ),
                        )
                    )
                    n += 1
                m += 1
        return out

    sends = halo_copies(
        side,
        (OWN - NEAR) * c,
        jnp.where(c == 0, E, O - NEAR),
        jnp.where(c == 0, NEAR, OWN - K),
        jnp.where(c == 0, E + NEAR, 0),
        cross,
    )

    @pl.when(has_cross)
    def _():
        for _, _, cp in sends:
            cp.start()

    low_recv = halo_copies(0, OWN - NEAR, O - NEAR, OWN - K, 0, s)
    high_recv = halo_copies(1, 0, E, NEAR, E + NEAR, s)

    def wait_halo(far):
        @pl.when(has_low)
        def _():
            for core, fr, cp in low_recv:
                if core == 0 and fr == far:
                    cp.wait_recv()

        @pl.when(has_high)
        def _():
            for core, fr, cp in high_recv:
                if core == 0 and fr == far:
                    cp.wait_recv()

    for cp in locals_:
        cp.wait()
    for cp in part:
        cp.wait_recv()
    wait_halo(False)
    wait_halo(True)

    lane = lax.broadcasted_iota(jnp.int32, (SUB, LANES), 1)
    sub = lax.broadcasted_iota(jnp.int32, (SUB, LANES), 0)
    part_of = sub // ND
    lane_c = lax.broadcasted_iota(jnp.int32, (ny, LANES), 1)
    row_c = lax.broadcasted_iota(jnp.int32, (ny, LANES), 0)
    last_z = lane == LANES - 1
    first_z = lane == 0

    def tables(l, carry):
        m = c_mat[l]
        inside = jnp.logical_and(
            jnp.logical_or(has_low, l >= O), jnp.logical_or(has_high, l < E)
        )
        gate = jnp.where(inside, F32(1.0), F32(0.0))

        def look(table):
            val = jnp.full((ny, LANES), table[0], F32)
            for k in range(1, NCLASS):
                val = jnp.where(m == k, table[k], val)
            return val

        storage = look(t_storage)
        biot = look(t_alpha)
        bulk = look(t_bulk)
        shear = look(t_shear)
        stab = biot * biot / bulk
        c_stab[l] = stab
        c_diag[l] = (storage + stab) * gate
        c_hb[l] = 0.5 * biot * gate
        c_shear[l] = shear * gate
        return carry

    lax.fori_loop(0, LT, tables, 0)

    def spread_rows(dst, l, idx, rows=None):
        for y in range(yh if rows is None else rows):
            val = jnp.broadcast_to(c_tmp[idx, pl.ds(y, 1), :], (SUB, LANES))
            for h in range(1, HV):
                more = jnp.broadcast_to(c_tmp[idx, pl.ds(y + h * yh, 1), :], (SUB, LANES))
                val = jnp.where(part_of >= h, more, val)
            dst[l, y] = val

    def faces(src, diag, dd, dx, dy, dz, dm):
        def layer(i, carry):
            l = 1 + i
            mid = src[l]
            xp = 0.5 * (mid + src[l + 1])
            xm = 0.5 * (mid + src[l - 1])
            up = jnp.where(row_c == ny - 1, 0.0, pltpu.roll(mid, ny - 1, 0))
            dn = jnp.where(row_c == 0, 0.0, pltpu.roll(mid, 1, 0))
            yp = 0.5 * (mid + up)
            ym = 0.5 * (mid + dn)
            rt = jnp.where(lane_c == LANES - 1, 0.0, pltpu.roll(mid, LANES - 1, 1))
            lf = jnp.where(lane_c == 0, 0.0, pltpu.roll(mid, 1, 1))
            zp = 0.5 * (mid + rt)
            zm = 0.5 * (mid + lf)
            total = xp + xm + yp + ym + zp + zm
            if diag is not None:
                total = total + diag[l]
            c_tmp[0, 0:ny] = total
            c_tmp[1, 0:ny] = xp
            c_tmp[2, 0:ny] = ym
            c_tmp[2, ny : ny + SUB] = jnp.zeros((SUB, LANES), F32)
            c_tmp[3, 0:ny] = jnp.where(lane_c == LANES - 1, 0.0, zp)
            c_tmp[4, 0:ny] = jnp.where(lane_c == 0, 0.0, zm)
            spread_rows(dd, l, 0)
            spread_rows(dx, l, 1)
            spread_rows(dy, l, 2, yh + 1)
            spread_rows(dz, l, 3)
            spread_rows(dm, l, 4)
            return carry

        lax.fori_loop(0, LT - 2, layer, 0)
        c_tmp[1, 0:ny] = 0.5 * (src[0] + src[1])
        spread_rows(dx, 0, 1)

    faces(c_perm, c_diag, pd, px, py, pz, pm)
    faces(c_shear, None, ed, ex, ey, ez, em)

    def plain(i, carry):
        l = 1 + i
        c_tmp[0, 0:ny] = c_hb[l]
        c_tmp[1, 0:ny] = c_stab[l]
        spread_rows(hb, l, 0)
        spread_rows(st, l, 1)
        return carry

    lax.fori_loop(0, LT - 2, plain, 0)

    def row_of(ref, l, y):
        val = jnp.broadcast_to(ref[l, pl.ds(y, 1), :], (SUB, LANES))
        for h in range(1, HV):
            more = jnp.broadcast_to(ref[l, pl.ds(y + h * yh, 1), :], (SUB, LANES))
            val = jnp.where(part_of >= h, more, val)
        return val

    flat = praw.reshape(ND * LT * ny, LANES)

    def source(l, carry):
        for y in range(yh):
            pieces = [
                flat[pl.ds(l * ny + h * yh + y, ND, stride=LT * ny), :] for h in range(HV)
            ]
            f[l, y] = jnp.concatenate(pieces, axis=0) * row_of(c_bs, l, y)
        return carry

    lax.fori_loop(0, LT, source, 0)

    class Rows:
        def __init__(self, ref, l0, pre=()):
            self.ref, self.l0, self.pre, self.got = ref, l0, pre, {}

        def __call__(self, g, y):
            if (g, y) not in self.got:
                if y == -1:
                    self.got[g, y] = jnp.where(
                        part_of > 0, pltpu.roll(self(g, yh - 1), ND, 0), 0.0
                    )
                elif y == yh:
                    self.got[g, y] = jnp.where(
                        part_of < HV - 1, pltpu.roll(self(g, 0), SUB - ND, 0), 0.0
                    )
                else:
                    self.got[g, y] = self.ref[(*self.pre, self.l0 + g, y)]
            return self.got[g, y]

    def left(x):
        return pltpu.roll(x, 1, 1)

    def right(x):
        return pltpu.roll(x, LANES - 1, 1)

    class Coef:
        def __init__(self, ref, l0):
            self.ref, self.l0, self.got = ref, l0, {}

        def __call__(self, g, y):
            if (g, y) not in self.got:
                self.got[g, y] = self.ref[self.l0 + g, y]
            return self.got[g, y]

    p_ops = (pd, px, py, pz, pm)
    e_ops = (ed, ex, ey, ez, em)

    def group(ops, vals, l0, n, emit):
        cd, cx, cy, cz, cm = (Coef(o, l0) for o in ops)
        for y in range(yh):
            for g in range(n):
                for k, val in enumerate(vals):
                    x = val(g, y)
                    out = cd(g, y) * x
                    out = out - cz(g, y) * right(x)
                    out = out - cm(g, y) * left(x)
                    out = out - cx(g, y) * val(g + 1, y)
                    out = out - cx(g - 1, y) * val(g - 1, y)
                    out = out - cy(g, y + 1) * val(g, y + 1)
                    out = out - cy(g, y) * val(g, y - 1)
                    emit(k, g, y, x, out)

    def rows(ref, l0, k=None):
        return Rows(ref, l0, () if k is None else (k,))

    def own_loop(n, body, init):
        return lax.fori_loop(0, NL // n, lambda i, a: body(O + i * n, n, a), init)

    def halo_loop(k, n, body, far=0):
        trips = (k - far) // n

        @pl.when(has_low)
        def _():
            lax.fori_loop(0, trips, lambda i, a: body(O - k + i * n, n, a), 0)

        @pl.when(has_high)
        def _():
            lax.fori_loop(0, trips, lambda i, a: body(E + far + i * n, n, a), 0)

    zeros = (zero8,)

    def first_pass(ops, src, dst, comps, n):
        def body(l0, n, acc):
            acc = list(acc)

            def emit(k, g, y, x, out):
                if comps is None:
                    dst[l0 + g, y] = out
                else:
                    dst[k, l0 + g, y] = out
                acc[0] = acc[0] + x * x
                acc[1] = acc[1] + x * out
                acc[2] = acc[2] + out * out

            ks = [None] if comps is None else range(comps)
            group(ops, [rows(src, l0, k) for k in ks], l0, n, emit)
            return tuple(acc)

        return own_loop(n, body, zeros * 3)

    def halo_pass(ops, src, dst, comps, k, n, far=0):
        def body(l0, n, acc):
            def emit(kk, g, y, x, out):
                if comps is None:
                    dst[l0 + g, y] = out
                else:
                    dst[kk, l0 + g, y] = out

            ks = [None] if comps is None else range(comps)
            group(ops, [rows(src, l0, kk) for kk in ks], l0, n, emit)
            return acc

        halo_loop(k, n, body, far)

    def second_pass(ops, src, comps, n, dst=None):
        def body(l0, n, acc):
            acc = list(acc)

            def emit(k, g, y, x, out):
                acc[0] = acc[0] + x * out
                if dst is not None:
                    dst[l0 + g, y] = out

            ks = [None] if comps is None else range(comps)
            group(ops, [rows(src, l0, k) for k in ks], l0, n, emit)
            return tuple(acc)

        return own_loop(n, body, zeros)

    GAP = LANES // SUB
    packed_at = lane // GAP == sub

    def red_copy(r, j):
        peer = lax.rem(s + j, ns)
        return remote(
            red_src.at[r],
            red_buf.at[r, s],
            sem_red_send.at[r, j],
            sem_red.at[r, s],
            peer * 2 + c,
            d,
        )

    def red_start(r, moments):
        row = jnp.zeros((SUB, LANES), F32)
        for m, acc in enumerate(moments):
            total = jnp.sum(acc, axis=1, keepdims=True)
            row = row + jnp.where(
                jnp.logical_and(packed_at, lax.rem(lane, GAP) == m), total, 0.0
            )
        packed = jnp.sum(row, axis=0, keepdims=True)
        red_src[r] = packed
        red_buf[r, s] = packed
        for j in range(1, ns):
            red_copy(r, j).start()

    def red_wait(r):
        for j in range(1, ns):
            peer = lax.rem(s + j, ns)
            remote(
                red_src.at[r],
                red_buf.at[r, peer],
                sem_red_send.at[r, j],
                sem_red.at[r, peer],
                peer * 2 + c,
                d,
            ).wait_recv()
        total = red_buf[r, 0]
        for j in range(1, ns):
            total = total + red_buf[r, j]
        full = jnp.where(packed_at, jnp.broadcast_to(total, (SUB, LANES)), 0.0)
        out = []
        for m in range(4):
            val = jnp.sum(
                jnp.where(lax.rem(lane, GAP) == m, full, 0.0), axis=1, keepdims=True
            )
            val = jnp.broadcast_to(val, (SUB, LANES))
            both = val
            for h in range(1, HV):
                both = both + pltpu.roll(val, ND * h, 0)
            out.append(both)
        return out

    def weights(moments):
        m0, m1, m2, m3 = moments
        a0 = m0 / m1
        rr = a0 * a0 * m2 - m0
        beta1 = 1.0 + rr / m0
        dw = beta1 * beta1 * m1 - 2.0 * beta1 * a0 * m2 + a0 * a0 * m3
        a1 = rr / dw
        return a0 + a1 * beta1, -a1 * a0

    def solve(idx, kf, before_halo):
        mo = first_pass(p_ops, f, w, None, 2)
        halo_pass(p_ops, f, w, None, 1, 1)
        (m3,) = second_pass(p_ops, w, None, 2, v)
        red_start(3 * idx, (*mo, m3))
        before_halo()
        halo_pass(p_ops, f, w, None, kf - 1, 1, 1)
        halo_pass(p_ops, w, v, None, kf - 4, 1)
        y0, y1 = weights(red_wait(3 * idx))

        def press(i, a):
            l = O - (kf - 1) + i
            for y in range(yh):
                p1[l, y] = y0 * f[l, y] + y1 * w[l, y]
            return a

        lax.fori_loop(0, NL + 2 * (kf - 1), press, 0)

        def grad(i, a):
            l0 = O - (kf - 2) + 2 * i
            val = rows(p1, l0)
            for y in range(yh):
                for g in range(2):
                    coef = hb[l0 + g, y]
                    x = val(g, y)
                    b[0, l0 + g, y] = coef * (val(g + 1, y) - val(g - 1, y))
                    b[1, l0 + g, y] = coef * (val(g, y + 1) - val(g, y - 1))
                    b[2, l0 + g, y] = coef * (
                        jnp.where(last_z, 0.0, right(x)) - jnp.where(first_z, 0.0, left(x))
                    )
            return a

        lax.fori_loop(0, (NL + 2 * (kf - 2)) // 2, grad, 0)
        mo = first_pass(e_ops, b, we, 3, 1)
        halo_pass(e_ops, b, we, 3, 1, 1)
        (m3,) = second_pass(e_ops, we, 3, 1)
        red_start(3 * idx + 1, (*mo, m3))
        halo_pass(e_ops, b, we, 3, kf - 3, 1, 1)
        z0, z1 = weights(red_wait(3 * idx + 1))

        def resid(l0, n, a):
            got = {}

            def flow(k, g, y):
                if (k, g, y) not in got:
                    if y == -1:
                        got[k, g, y] = jnp.where(
                            part_of > 0, pltpu.roll(flow(k, g, yh - 1), ND, 0), 0.0
                        )
                    elif y == yh:
                        got[k, g, y] = jnp.where(
                            part_of < HV - 1, pltpu.roll(flow(k, g, 0), SUB - ND, 0), 0.0
                        )
                    else:
                        l = l0 + g
                        got[k, g, y] = hb[l, y] * (z0 * b[k, l, y] + z1 * we[k, l, y])
                return got[k, g, y]

            for y in range(yh):
                for g in range(n):
                    l = l0 + g
                    tz = flow(2, g, y)
                    div = flow(0, g - 1, y) - flow(0, g + 1, y)
                    div = div + (flow(1, g, y - 1) - flow(1, g, y + 1))
                    div = div + (
                        jnp.where(first_z, 0.0, left(tz)) - jnp.where(last_z, 0.0, right(tz))
                    )
                    image = y0 * w[l, y] + y1 * v[l, y]
                    r2[l, y] = f[l, y] - div + st[l, y] * p1[l, y] - image
            return a

        own_loop(2, resid, 0)
        halo_loop(kf - 4, 1, resid)

        mo = first_pass(p_ops, r2, w2, None, 2)
        halo_pass(p_ops, r2, w2, None, 1, 1)
        (m3,) = second_pass(p_ops, w2, None, 2)
        red_start(3 * idx + 2, (*mo, m3))
        if kf - 5 > 1:
            halo_pass(p_ops, r2, w2, None, kf - 5, 1, 1)
        return weights(red_wait(3 * idx + 2))

    y0, y1 = solve(0, K, lambda: None)

    def update(i, a):
        l = O - NEAR + i
        for y in range(yh):
            p2 = p1[l, y] + y0 * r2[l, y] + y1 * w2[l, y]
            f[l, y] = p2 * row_of(c_obs, l, y)
        return a

    lax.fori_loop(0, NL + 2 * NEAR, update, 0)

    FAR = K - 1 - NEAR
    to_low = remote(
        f.at[pl.ds(O + NEAR, FAR)],
        f.at[pl.ds(E + NEAR, FAR)],
        sem_f_send.at[0],
        sem_f.at[1],
        jnp.where(has_low, t - 2, t + 2),
        d,
    )
    to_high = remote(
        f.at[pl.ds(E - NEAR - FAR, FAR)],
        f.at[pl.ds(O - NEAR - FAR, FAR)],
        sem_f_send.at[1],
        sem_f.at[0],
        jnp.where(has_high, t + 2, t - 2),
        d,
    )

    @pl.when(has_low)
    def _():
        to_low.start()

    @pl.when(has_high)
    def _():
        to_high.start()

    def new_halo():
        @pl.when(has_low)
        def _():
            to_high.wait_recv()

        @pl.when(has_high)
        def _():
            to_low.wait_recv()

    y0, y1 = solve(1, K - 1, new_halo)

    def finish(i, a):
        l = O + i
        for y in range(yh):
            p2 = p1[l, y] + y0 * r2[l, y] + y1 * w2[l, y]
            ybuf[i, y] = p2 * row_of(c_bs, l, y)
        return a

    lax.fori_loop(0, NL, finish, 0)

    me = d * 2 + c
    nq = 2 * nd
    per = NL // nq

    def gram_copy(q, slot):
        dq = q // 2
        cq = lax.rem(q, 2)
        return remote(
            ybuf.at[pl.ds(per * q, per)],
            grecv.at[slot],
            sem_g_send.at[q],
            sem_g.at[slot],
            s * 2 + cq,
            dq,
        )

    for j in range(1, nq):
        gram_copy(lax.rem(me + j, nq), me).start()

    hflat = hraw.reshape(ND * OWN * ny, LANES)
    oflat = hess.reshape(2 * ND * OWN * ny, LANES)

    def unpack(dst, base, at):
        def layer(i, a):
            for y in range(yh):
                val = ybuf[at + i, y]
                for h in range(HV):
                    dst[pl.ds(base + i * ny + h * yh + y, ND, stride=OWN * ny), :] = val[
                        h * ND : (h + 1) * ND
                    ]
            return a

        lax.fori_loop(0, OWN, layer, 0)

    unpack(hflat, 0, OWN * (1 - c))
    swap = remote(
        hraw,
        hess.at[pl.ds(ND * c, ND)],
        sem_h.at[0],
        sem_h.at[1],
        partner,
        d,
    )
    swap.start()
    unpack(oflat, ND * c * OWN * ny, OWN * c)

    for i in range(per):
        for y in range(yh):
            grecv[me, i, y] = ybuf[per * me + i, y]
    for j in range(1, nq):
        q = lax.rem(me + j, nq)
        gram_copy(q, q).wait_recv()

    width = nq * SUB

    def gram_part(i, acc):
        for l in range(per):
            z = grecv[:, l, i].reshape(width, LANES)
            acc = acc + lax.dot_general(
                z,
                z,
                (((1,), (1,)), ((), ())),
                precision=lax.Precision.HIGHEST,
                preferred_element_type=F32,
            )
        return acc

    g64 = lax.fori_loop(0, yh, gram_part, jnp.zeros((width, width), F32))
    ndir = nq * ND
    fold = jnp.zeros((ndir, LANES), F32)
    for h in range(HV):
        ri = lax.broadcasted_iota(jnp.int32, (ndir, width), 0)
        ci = lax.broadcasted_iota(jnp.int32, (ndir, width), 1)
        left_sel = jnp.where(ci == (ri // ND) * SUB + h * ND + lax.rem(ri, ND), 1.0, 0.0)
        rj = lax.broadcasted_iota(jnp.int32, (width, LANES), 0)
        cj = lax.broadcasted_iota(jnp.int32, (width, LANES), 1)
        right_sel = jnp.where(
            jnp.logical_and(rj == (cj // ND) * SUB + h * ND + lax.rem(cj, ND), cj < ndir),
            1.0,
            0.0,
        )
        mid = jnp.dot(
            left_sel, g64, precision=lax.Precision.HIGHEST, preferred_element_type=F32
        )
        fold = fold + jnp.dot(
            mid, right_sel, precision=lax.Precision.HIGHEST, preferred_element_type=F32
        )
    packed = fold[0:SUB]
    for k in range(1, ndir // SUB):
        packed = packed + pltpu.roll(fold[k * SUB : (k + 1) * SUB], ndir * k, 1)

    ga_src[...] = packed
    ga_buf[s] = packed

    def ga_copy(j, slot):
        peer = lax.rem(s + j, ns)
        return remote(
            ga_src, ga_buf.at[slot], sem_ga_send.at[j], sem_ga.at[slot], peer * 2 + c, d
        )

    for j in range(1, ns):
        ga_copy(j, s).start()
    for j in range(1, ns):
        ga_copy(j, lax.rem(s + j, ns)).wait_recv()
    total = ga_buf[0]
    for j in range(1, ns):
        total = total + ga_buf[j]
    gb_src[...] = total
    gb_buf[me] = total

    def gb_copy(j, slot):
        q = lax.rem(me + j, nq)
        return remote(
            gb_src,
            gb_buf.at[slot],
            sem_gb_send.at[j],
            sem_gb.at[slot],
            s * 2 + lax.rem(q, 2),
            q // 2,
        )

    for j in range(1, nq):
        gb_copy(j, me).start()
    for j in range(1, nq):
        gb_copy(j, lax.rem(me + j, nq)).wait_recv()
    total = gb_buf[0]
    for j in range(1, nq):
        total = total + gb_buf[j]
    total = total * (1.0 / cells)
    for k in range(ndir // SUB):
        row = total if k == 0 else pltpu.roll(total, LANES - ndir * k, 1)
        gram[k * SUB : (k + 1) * SUB] = row

    swap.wait_recv()
    swap.wait_send()
    for cp in part:
        cp.wait_send()

    @pl.when(has_cross)
    def _():
        for _, _, cp in sends:
            cp.wait_send()

    for r in range(NRED):
        for j in range(1, ns):
            red_copy(r, j).wait_send()

    @pl.when(has_low)
    def _():
        to_low.wait_send()

    @pl.when(has_high)
    def _():
        to_high.wait_send()

    for j in range(1, nq):
        gram_copy(lax.rem(me + j, nq), me).wait_send()
    for j in range(1, ns):
        ga_copy(j, s).wait_send()
    for j in range(1, nq):
        gb_copy(j, me).wait_send()


def solution(mesh):
    ns = mesh.shape["tile"] // 2
    nd = mesh.shape["dir"]
    nq = 2 * nd

    def body(probes, bs, obs, perm, mat, storage, alpha, bulk, shear):
        ny, nz = probes.shape[2:]
        yh = ny // HV
        cells = OWN * 2 * ns * ny * nz
        vm = pl.BlockSpec(memory_space=pltpu.VMEM)
        sm = pl.BlockSpec(memory_space=pltpu.SMEM)

        def compact(n=LT, kind=F32):
            return pltpu.VMEM((n, ny, nz), kind)

        def wide(rows=yh, pre=()):
            return pltpu.VMEM((*pre, LT, rows, SUB, nz), F32)

        dma = pltpu.SemaphoreType.DMA
        scratch = [
            pltpu.VMEM((ND, LT, ny, nz), F32),
            compact(),
            compact(),
            compact(),
            compact(kind=jnp.int32),
            compact(),
            compact(),
            compact(),
            compact(),
            pltpu.VMEM((5, ny + SUB, nz), F32),
            wide(),
            wide(),
            wide(yh + 1),
            wide(),
            wide(),
            wide(),
            wide(),
            wide(yh + 1),
            wide(),
            wide(),
            wide(),
            wide(),
            wide(),
            wide(),
            wide(),
            wide(),
            wide(pre=(3,)),
            wide(pre=(3,)),
            wide(),
            wide(),
            pltpu.VMEM((NL, yh, SUB, nz), F32),
            pltpu.VMEM((ND, OWN, ny, nz), F32),
            pltpu.VMEM((nq, NL // nq, yh, SUB, nz), F32),
            pltpu.VMEM((NRED, 1, nz), F32),
            pltpu.VMEM((NRED, ns, 1, nz), F32),
            pltpu.VMEM((SUB, nz), F32),
            pltpu.VMEM((ns, SUB, nz), F32),
            pltpu.VMEM((SUB, nz), F32),
            pltpu.VMEM((nq, SUB, nz), F32),
            dma((5 + 18,)),
            dma((5,)),
            dma((2, 9)),
            dma((5,)),
            dma((NRED, ns)),
            dma((NRED, ns)),
            dma((ns,)),
            dma((ns,)),
            dma((nq,)),
            dma((nq,)),
            dma((nq,)),
            dma((nq,)),
            dma((2,)),
            dma((2,)),
            dma((2,)),
        ]
        hess, gram = pl.pallas_call(
            functools.partial(kernel, ns, nd, cells),
            out_shape=(
                jax.ShapeDtypeStruct(probes.shape, F32),
                jax.ShapeDtypeStruct((nq * ND, nz), F32),
            ),
            in_specs=[vm] * 5 + [sm] * 4,
            out_specs=(vm, vm),
            scratch_shapes=scratch,
            compiler_params=pltpu.CompilerParams(
                collective_id=0, has_side_effects=True, vmem_limit_bytes=67043328
            ),
        )(probes, bs, obs, perm, mat, storage, alpha, bulk, shear)
        r_factor = jnp.linalg.cholesky(gram[:, : nq * ND]).T
        return hess, r_factor

    return jax.shard_map(
        body,
        mesh=mesh,
        in_specs=(
            P("dir", "tile", None, None),
            P("tile", None, None),
            P("tile", None, None),
            P("tile", None, None),
            P("tile", None, None),
            P(),
            P(),
            P(),
            P(),
        ),
        out_specs=(P("dir", "tile", None, None), P()),
        check_vma=False,
    )
```

```python
import functools

import jax
import jax.numpy as jnp
from jax import lax
from jax.experimental import pallas as pl
from jax.experimental.pallas import tpu as pltpu
from jax.sharding import PartitionSpec as P

MESH = pl.DeviceIdType.MESH
F32 = jnp.float32
NCLASS = 8
LANES = 128
SUB = 8
OWN = 8
NL = 16
K = 6
O = K
E = K + NL
LT = NL + 2 * K
NB = 2
HV = 4
ND = SUB // HV
NDEV = NB * ND
NEAR = 2
NRED = 6 * NB


def kernel(
    ns,
    nd,
    cells,
    probes,
    bs_in,
    obs_in,
    perm_in,
    mat_in,
    t_storage,
    t_alpha,
    t_bulk,
    t_shear,
    hess,
    gram,
    fraw,
    praw,
    c_bs,
    c_obs,
    c_perm,
    c_mat,
    c_diag,
    c_stab,
    c_hb,
    c_shear,
    c_tmp,
    pd,
    px,
    py,
    pz,
    pm,
    ed,
    ex,
    ey,
    ez,
    em,
    hb,
    st,
    f,
    w,
    v,
    p1,
    b,
    we,
    r2,
    w2,
    ybuf,
    hraw,
    grecv,
    wts,
    red_src,
    red_buf,
    ga_src,
    ga_buf,
    gb_src,
    gb_buf,
    sem_init_send,
    sem_part,
    sem_halo,
    sem_red_send,
    sem_red,
    sem_ga_send,
    sem_ga,
    sem_gb_send,
    sem_gb,
    sem_g_send,
    sem_g,
    sem_h,
    sem_f_send,
    sem_f,
    sem_r_send,
    sem_r,
):
    scope = []

    def phase(name=None):
        if scope:
            scope.pop().__exit__(None, None, None)
        if name is not None:
            scope.append(jax.named_scope(name))
            scope[0].__enter__()

    phase("a_start")
    ny = probes.shape[2]
    yh = ny // HV
    t = lax.axis_index("tile")
    d = lax.axis_index("dir")
    s = t // 2
    c = lax.rem(t, 2)
    partner = s * 2 + (1 - c)
    has_low = s > 0
    has_high = s < ns - 1

    barrier = pltpu.get_barrier_semaphore()

    def greet(tile, dr):
        pl.semaphore_signal(barrier, inc=1, device_id=(tile, dr), device_id_type=MESH)

    cross = jnp.where(c == 0, s - 1, s + 1)
    has_cross = jnp.where(c == 0, has_low, has_high)
    for j in range(1, ns):
        greet(lax.rem(s + j, ns) * 2 + c, d)
    greet(partner, d)
    for j in range(1, nd):
        dj = lax.rem(d + j, nd)
        greet(t, dj)
        greet(partner, dj)

    @pl.when(has_cross)
    def _():
        greet(cross * 2 + (1 - c), d)

    own_at = O + OWN * c
    zero8 = jnp.zeros((SUB, LANES), F32)
    zc = jnp.zeros((ny, LANES), F32)
    zi = jnp.zeros((ny, LANES), jnp.int32)

    def products(l, a):
        sens = bs_in[l]
        for dd in range(2 * NDEV):
            fraw[dd, l] = probes[dd, l] * sens
        c_bs[own_at + l] = sens
        c_obs[own_at + l] = obs_in[l]
        c_perm[own_at + l] = perm_in[l]
        c_mat[own_at + l] = mat_in[l]
        return a

    lax.fori_loop(0, OWN, products, 0)

    def zero_side(lo):
        def layer(i, carry):
            l = lo + i
            c_perm[l] = zc
            c_obs[l] = zc
            c_mat[l] = zi
            for dd in range(NDEV):
                praw[dd, l] = zc
            for q in range(NB):
                for y in range(yh):
                    w[q, l, y] = zero8
                    v[q, l, y] = zero8
                    r2[q, l, y] = zero8
                    w2[q, l, y] = zero8
                    for k in range(3):
                        we[q, k, l, y] = zero8
            return carry

        lax.fori_loop(0, K, layer, 0)

    @pl.when(jnp.logical_not(has_low))
    def _():
        zero_side(0)

    @pl.when(jnp.logical_not(has_high))
    def _():
        zero_side(E)

    lane = lax.broadcasted_iota(jnp.int32, (SUB, LANES), 1)
    sub = lax.broadcasted_iota(jnp.int32, (SUB, LANES), 0)
    part_of = sub // ND
    lane_c = lax.broadcasted_iota(jnp.int32, (ny, LANES), 1)
    row_c = lax.broadcasted_iota(jnp.int32, (ny, LANES), 0)
    last_z = lane == LANES - 1
    first_z = lane == 0

    def tables(lo, n):
        def layer(i, carry):
            l = lo + i
            m = c_mat[l]
            inside = jnp.logical_and(
                jnp.logical_or(has_low, l >= O), jnp.logical_or(has_high, l < E)
            )
            gate = jnp.where(inside, F32(1.0), F32(0.0))

            def look(table):
                val = jnp.full((ny, LANES), table[0], F32)
                for k in range(1, NCLASS):
                    val = jnp.where(m == k, table[k], val)
                return val

            biot = look(t_alpha)
            stab = biot * biot / look(t_bulk)
            c_stab[l] = stab
            c_diag[l] = (look(t_storage) + stab) * gate
            c_hb[l] = 0.5 * biot * gate
            c_shear[l] = look(t_shear) * gate
            return carry

        lax.fori_loop(0, n, layer, 0)

    phase("a_tables")
    tables(own_at, OWN)

    phase("b_barrier")
    pl.semaphore_wait(barrier, (ns - 1) + 1 + 2 * (nd - 1) + jnp.where(has_cross, 1, 0))

    def remote(src, dst, ssem, rsem, tile, dr):
        return pltpu.make_async_remote_copy(
            src_ref=src,
            dst_ref=dst,
            send_sem=ssem,
            recv_sem=rsem,
            device_id=(tile, dr),
            device_id_type=MESH,
        )

    def part_copies():
        pairs = ((perm_in, c_perm), (mat_in, c_mat), (None, praw), (bs_in, c_bs), (obs_in, c_obs))
        out = []
        for i, (src, dst) in enumerate(pairs):
            if src is None:
                src = fraw.at[pl.ds(NDEV * (1 - c), NDEV)]
                dst = dst.at[:, pl.ds(own_at, OWN)]
            else:
                dst = dst.at[pl.ds(own_at, OWN)]
            out.append(remote(src, dst, sem_init_send.at[i], sem_part.at[i], partner, d))
        return out

    def halo_copies(side, slab, near, far, cores, only=None):
        jobs = []
        for n, (src, dst) in enumerate(((perm_in, c_perm), (mat_in, c_mat), (None, praw))):
            jobs.append((n, src, dst, *near, NEAR))
        for n, (src, dst) in enumerate(((perm_in, c_perm), (mat_in, c_mat), (None, praw))):
            jobs.append((3 + n, src, dst, *far, K - NEAR))
        jobs.append((6, obs_in, c_obs, *near, NEAR))
        out = []
        for n, src, dst, at, to, size in jobs:
            if only is not None and n not in only:
                continue
            for core in cores:
                if src is None:
                    a = fraw.at[pl.ds(NDEV * core, NDEV), pl.ds(at, size)]
                    z = praw.at[:, pl.ds(to, size)]
                else:
                    a = src.at[pl.ds(at, size)]
                    z = dst.at[pl.ds(to, size)]
                out.append(
                    remote(
                        a,
                        z,
                        sem_init_send.at[5 + 2 * n + core],
                        sem_halo.at[side, n],
                        slab * 2 + core,
                        d,
                    )
                )
        return out

    def cross_copies():
        return halo_copies(
            1 - c,
            cross,
            ((OWN - NEAR) * c, jnp.where(c == 0, E, O - NEAR)),
            (jnp.where(c == 0, NEAR, OWN - K), jnp.where(c == 0, E + NEAR, 0)),
            (0, 1),
        )

    phase("c_sends")

    @pl.when(has_cross)
    def _():
        for cp in cross_copies():
            cp.start()

    for cp in part_copies():
        cp.start()

    def wait_halo(only):
        @pl.when(has_low)
        def _():
            for cp in halo_copies(0, s, (OWN - NEAR, O - NEAR), (OWN - K, 0), (0,), only):
                cp.wait_recv()

        @pl.when(has_high)
        def _():
            for cp in halo_copies(1, s, (0, E), (NEAR, E + NEAR), (0,), only):
                cp.wait_recv()

    def wide_row(read, y):
        val = jnp.broadcast_to(read(y), (SUB, LANES))
        for h in range(1, HV):
            more = jnp.broadcast_to(read(y + h * yh), (SUB, LANES))
            val = jnp.where(part_of >= h, more, val)
        return val

    def row_of(ref, l, y):
        return wide_row(lambda y: ref[l, pl.ds(y, 1), :], y)

    def spread_rows(dst, l, idx, rows=None):
        for y in range(yh if rows is None else rows):
            dst[l, y] = row_of(c_tmp, idx, y)

    def faces_layer(l, src, diag, dd, dx, dy, dz, dm, at):
        mid = src[l]
        xp = 0.5 * (mid + src[l + 1])
        xm = 0.5 * (mid + src[l - 1])
        up = jnp.where(row_c == ny - 1, 0.0, pltpu.roll(mid, ny - 1, 0))
        dn = jnp.where(row_c == 0, 0.0, pltpu.roll(mid, 1, 0))
        yp = 0.5 * (mid + up)
        ym = 0.5 * (mid + dn)
        rt = jnp.where(lane_c == LANES - 1, 0.0, pltpu.roll(mid, LANES - 1, 1))
        lf = jnp.where(lane_c == 0, 0.0, pltpu.roll(mid, 1, 1))
        zp = 0.5 * (mid + rt)
        zm = 0.5 * (mid + lf)
        total = xp + xm + yp + ym + zp + zm
        if diag is not None:
            total = total + diag[l]
        c_tmp[at, 0:ny] = total
        c_tmp[at + 1, 0:ny] = xp
        c_tmp[at + 2, 0:ny] = ym
        c_tmp[at + 2, ny : ny + SUB] = jnp.broadcast_to(
            0.5 * mid[ny - 1 : ny], (SUB, LANES)
        )
        c_tmp[at + 3, 0:ny] = jnp.where(lane_c == LANES - 1, 0.0, zp)
        c_tmp[at + 4, 0:ny] = jnp.where(lane_c == 0, 0.0, zm)
        return lambda: (
            spread_rows(dd, l, at),
            spread_rows(dx, l, at + 1),
            spread_rows(dy, l, at + 2, yh + 1),
            spread_rows(dz, l, at + 3),
            spread_rows(dm, l, at + 4),
        )

    def faces(lo, n):
        def layer(i, carry):
            l = lo + i
            done = (
                faces_layer(l, c_perm, c_diag, pd, px, py, pz, pm, 0),
                faces_layer(l, c_shear, None, ed, ex, ey, ez, em, 5),
            )
            for y in range(yh):
                hb[l, y] = row_of(c_hb, l, y)
                st[l, y] = row_of(c_stab, l, y)
            for make in done:
                make()
            return carry

        lax.fori_loop(0, n, layer, 0)

    def x_faces(l):
        c_tmp[1, 0:ny] = 0.5 * (c_perm[l] + c_perm[l + 1])
        c_tmp[6, 0:ny] = 0.5 * (c_shear[l] + c_shear[l + 1])
        spread_rows(px, l, 1)
        spread_rows(ex, l, 6)

    def source(lo, n, raw=praw, first=0, shift=0, layers=LT):
        flat = raw.reshape(raw.shape[0] * layers * ny, LANES)

        def layer(i, carry):
            l = lo + i
            for q in range(NB):
                for y in range(yh):
                    base = ((first + q * ND) * layers + (l - shift)) * ny + y
                    f[q, l, y] = jnp.concatenate(
                        [
                            flat[pl.ds(base + h * yh, ND, stride=layers * ny), :]
                            for h in range(HV)
                        ],
                        axis=0,
                    )
            return carry

        lax.fori_loop(0, n, layer, 0)

    phase("d_own")
    faces(own_at + 1, OWN - 2)
    source(own_at, OWN, fraw, NDEV * c, own_at, OWN)
    phase("d_wait_part")
    for cp in part_copies():
        cp.wait_recv()
    phase("d_other")
    other_at = O + OWN * (1 - c)
    tables(other_at, OWN)
    faces(jnp.where(c == 0, O + OWN - 1, O + 1), OWN)
    source(other_at, OWN)
    phase("d_wait_near")
    wait_halo((0, 1, 2))
    phase("d_near")
    tables(O - NEAR, NEAR)
    tables(E, NEAR)
    faces(O - 1, 2)
    faces(E - 1, 2)
    x_faces(O - 2)
    source(O - NEAR, NEAR)
    source(E, NEAR)

    def far_layers():
        wait_halo((3, 4, 5))
        tables(0, K - NEAR)
        tables(E + NEAR, K - NEAR)
        faces(1, K - NEAR)
        faces(E + 1, K - NEAR)
        x_faces(0)
        source(0, K - NEAR)
        source(E + NEAR, K - NEAR)

    class Rows:
        def __init__(self, ref, l0, pre=()):
            self.ref, self.l0, self.pre, self.got = ref, l0, pre, {}

        def load(self, g, y):
            return self.ref[(*self.pre, self.l0 + g, y)]

        def __call__(self, g, y):
            if (g, y) not in self.got:
                if y == -1:
                    self.got[g, y] = jnp.where(
                        part_of > 0, pltpu.roll(self(g, yh - 1), ND, 0), 0.0
                    )
                elif y == yh:
                    self.got[g, y] = jnp.where(
                        part_of < HV - 1, pltpu.roll(self(g, 0), SUB - ND, 0), 0.0
                    )
                else:
                    self.got[g, y] = self.load(g, y)
            return self.got[g, y]

    class Made(Rows):
        def __init__(self, make):
            self.make, self.got = make, {}

        def load(self, g, y):
            return self.make(g, y)

    def left(x):
        return pltpu.roll(x, 1, 1)

    def right(x):
        return pltpu.roll(x, LANES - 1, 1)

    p_ops = (pd, px, py, pz, pm)
    e_ops = (ed, ex, ey, ez, em)

    def group(ops, vals, l0, n, emit):
        cd, cx, cy, cz, cm = (Rows(o, l0).load for o in ops)
        cx, cy = Rows(ops[1], l0), Made(cy)
        for y in range(yh):
            for g in range(n):
                co = [
                    op(g, y) for op in (cd, cz, cm)
                ]
                c_up = ops[2][l0 + g, y + 1]
                c_dn = ops[2][l0 + g, y]
                for k, val in enumerate(vals):
                    x = val(g, y)
                    out = co[0] * x
                    out = out - co[1] * right(x)
                    out = out - co[2] * left(x)
                    out = out - cx(g, y) * val(g + 1, y)
                    out = out - cx(g - 1, y) * val(g - 1, y)
                    out = out - c_up * val(g, y + 1)
                    out = out - c_dn * val(g, y - 1)
                    emit(k, g, y, x, out)

    def own_loop(n, body, init):
        return lax.fori_loop(0, NL // n, lambda i, a: body(O + i * n, n, a), init)

    def halo_loop(k, n, body, far=0):
        trips = (k - far) // n

        @pl.when(has_low)
        def _():
            lax.fori_loop(0, trips, lambda i, a: body(O - k + i * n, n, a), 0)

        @pl.when(has_high)
        def _():
            lax.fori_loop(0, trips, lambda i, a: body(E + far + i * n, n, a), 0)

    def pres(q, comps):
        return [(q,)] if comps is None else [(q, k) for k in range(comps)]

    def first_pass(q, ops, src, dst, comps, n):
        pre = pres(q, comps)

        def body(l0, n, acc):
            acc = list(acc)

            def emit(k, g, y, x, out):
                dst[(*pre[k], l0 + g, y)] = out
                acc[0] = acc[0] + x * x
                acc[1] = acc[1] + x * out
                acc[2] = acc[2] + out * out

            group(ops, [Rows(src, l0, k) for k in pre], l0, n, emit)
            return tuple(acc)

        return own_loop(n, body, (zero8,) * 3)

    def halo_pass(q, ops, src, dst, comps, k, n, far=0):
        pre = pres(q, comps)

        def body(l0, n, acc):
            def emit(kk, g, y, x, out):
                dst[(*pre[kk], l0 + g, y)] = out

            group(ops, [Rows(src, l0, kk) for kk in pre], l0, n, emit)
            return acc

        halo_loop(k, n, body, far)

    def second_pass(q, ops, src, comps, n, dst=None):
        pre = pres(q, comps)

        def body(l0, n, acc):
            acc = list(acc)

            def emit(k, g, y, x, out):
                acc[0] = acc[0] + x * out
                if dst is not None:
                    dst[q, l0 + g, y] = out

            group(ops, [Rows(src, l0, k) for k in pre], l0, n, emit)
            return tuple(acc)

        return own_loop(n, body, (zero8,))

    GAP = LANES // SUB
    packed_at = lane // GAP == sub

    def red_copy(r, j, slot):
        peer = lax.rem(s + j, ns)
        return remote(
            red_src.at[r],
            red_buf.at[r, slot],
            sem_red_send.at[r, j],
            sem_red.at[r, slot],
            peer * 2 + c,
            d,
        )

    def red_start(r, moments):
        row = jnp.zeros((SUB, LANES), F32)
        for m, acc in enumerate(moments):
            total = jnp.sum(acc, axis=1, keepdims=True)
            row = row + jnp.where(
                jnp.logical_and(packed_at, lax.rem(lane, GAP) == m), total, 0.0
            )
        packed = jnp.sum(row, axis=0, keepdims=True)
        red_src[r] = packed
        red_buf[r, s] = packed
        for j in range(1, ns):
            red_copy(r, j, s).start()

    def red_wait(r):
        for j in range(1, ns):
            red_copy(r, j, lax.rem(s + j, ns)).wait_recv()
        total = red_buf[r, 0]
        for j in range(1, ns):
            total = total + red_buf[r, j]
        full = jnp.where(packed_at, jnp.broadcast_to(total, (SUB, LANES)), 0.0)
        out = []
        for m in range(4):
            val = jnp.sum(
                jnp.where(lax.rem(lane, GAP) == m, full, 0.0), axis=1, keepdims=True
            )
            val = jnp.broadcast_to(val, (SUB, LANES))
            both = val
            for h in range(1, HV):
                both = both + pltpu.roll(val, ND * h, 0)
            out.append(both)
        return out

    def weights(moments):
        m0, m1, m2, m3 = moments
        a0 = m0 / m1
        rr = a0 * a0 * m2 - m0
        beta1 = 1.0 + rr / m0
        dw = beta1 * beta1 * m1 - 2.0 * beta1 * a0 * m2 + a0 * a0 * m3
        a1 = rr / dw
        return a0 + a1 * beta1, -a1 * a0

    def strip(q, buf, at, to, size, ssem, rsem):
        low = remote(
            buf.at[q, pl.ds(O + at, size)],
            buf.at[q, pl.ds(E + to, size)],
            ssem.at[q, 0],
            rsem.at[q, 1],
            jnp.where(has_low, t - 2, t + 2),
            d,
        )
        high = remote(
            buf.at[q, pl.ds(E - at - size, size)],
            buf.at[q, pl.ds(O - to - size, size)],
            ssem.at[q, 1],
            rsem.at[q, 0],
            jnp.where(has_high, t + 2, t - 2),
            d,
        )
        return low, high

    def strip_do(args, start=False, recv=False, sent=False):
        low, high = strip(*args)

        @pl.when(has_low)
        def _():
            if start:
                low.start()
            if recv:
                high.wait_recv()
            if sent:
                low.wait_send()

        @pl.when(has_high)
        def _():
            if start:
                high.start()
            if recv:
                low.wait_recv()
            if sent:
                high.wait_send()

    def f_strip(q):
        return q, f, NEAR, NEAR, K - NEAR, sem_f_send, sem_f

    def r_strip(q):
        return q, r2, 2, 2, 1, sem_r_send, sem_r

    me = d * 2 + c
    nq = 2 * nd
    per = NL // nq

    def gram_copy(bt, l, q, slot):
        return remote(
            ybuf.at[bt, per * q + l],
            grecv.at[slot, bt, l],
            sem_g_send.at[bt, l, q],
            sem_g.at[bt, l, slot],
            s * 2 + lax.rem(q, 2),
            q // 2,
        )

    def each(stage, *args):
        def go(q, a):
            stage(q, *args)
            return a

        lax.fori_loop(0, NB, go, 0)

    def save(q, at, pair):
        for i in range(2):
            wts[q, at + i] = pair[i]

    def begin(q, base):
        mo = first_pass(q, p_ops, f, w, None, PN)
        halo_pass(q, p_ops, f, w, None, 1, 1)
        (m3,) = second_pass(q, p_ops, w, None, PN, v)
        red_start(base + q, (*mo, m3))

    def begin_far(q, idx):
        @pl.when(idx > 0)
        def _():
            strip_do(f_strip(q), recv=True)

        halo_pass(q, p_ops, f, w, None, K - 1, K - 2, 1)
        halo_pass(q, p_ops, w, v, None, 2, 2)

    def displace(q, base):
        y0, y1 = weights(red_wait(base + q))
        save(q, 0, (y0, y1))

        def press(i, a):
            for g in range(2):
                l = 1 + 2 * i + g
                for y in range(yh):
                    p1[q, l, y] = y0 * f[q, l, y] + y1 * w[q, l, y]
            return a

        lax.fori_loop(0, (LT - 2) // 2, press, 0)

        def grad(i, a):
            l0 = 2 + 4 * i
            val = Rows(p1, l0, (q,))
            for y in range(yh):
                for g in range(4):
                    coef = hb[l0 + g, y]
                    x = val(g, y)
                    b[q, 0, l0 + g, y] = coef * (val(g + 1, y) - val(g - 1, y))
                    b[q, 1, l0 + g, y] = coef * (val(g, y + 1) - val(g, y - 1))
                    b[q, 2, l0 + g, y] = coef * (
                        jnp.where(last_z, 0.0, right(x)) - jnp.where(first_z, 0.0, left(x))
                    )
            return a

        lax.fori_loop(0, (LT - 4) // 4, grad, 0)
        mo = first_pass(q, e_ops, b, we, 3, EN)
        halo_pass(q, e_ops, b, we, 3, 1, 1)
        (m3,) = second_pass(q, e_ops, we, 3, EN)
        red_start(base + NB + q, (*mo, m3))

    def displace_far(q):
        halo_pass(q, e_ops, b, we, 3, K - 3, 2, 1)

    def again(q, base, idx):
        z0, z1 = weights(red_wait(base + NB + q))
        y0, y1 = wts[q, 0], wts[q, 1]

        def resid(l0, n, a):
            def flow(k):
                def make(g, y):
                    l = l0 + g
                    return hb[l, y] * (z0 * b[q, k, l, y] + z1 * we[q, k, l, y])

                return Made(make)

            fx, fy, fz = flow(0), flow(1), flow(2)
            for y in range(yh):
                for g in range(n):
                    l = l0 + g
                    tz = fz(g, y)
                    div = fx(g - 1, y) - fx(g + 1, y)
                    div = div + (fy(g, y - 1) - fy(g, y + 1))
                    div = div + (
                        jnp.where(first_z, 0.0, left(tz)) - jnp.where(last_z, 0.0, right(tz))
                    )
                    image = y0 * w[q, l, y] + y1 * v[q, l, y]
                    r2[q, l, y] = f[q, l, y] - div + st[l, y] * p1[q, l, y] - image
            return a

        own_loop(4, resid, 0)
        halo_loop(2, 2, resid)
        mo = first_pass(q, p_ops, r2, w2, None, PN)

        @pl.when(idx == 0)
        def _():
            strip_do(r_strip(q), start=True)

        halo_pass(q, p_ops, r2, w2, None, 1, 1)
        (m3,) = second_pass(q, p_ops, w2, None, PN)
        red_start(base + 2 * NB + q, (*mo, m3))

    def again_far(q):
        strip_do(r_strip(q), recv=True, sent=True)
        halo_pass(q, p_ops, r2, w2, None, 2, 1, 1)

    def close(q, base, idx):
        x0, x1 = weights(red_wait(base + 2 * NB + q))

        def total(l, y):
            return p1[q, l, y] + x0 * r2[q, l, y] + x1 * w2[q, l, y]

        @pl.when(idx == 0)
        def _():
            def update(i, a):
                for g in range(2):
                    l = O - NEAR + 2 * i + g
                    for y in range(yh):
                        f[q, l, y] = total(l, y) * row_of(c_obs, l, y)
                return a

            lax.fori_loop(0, NL // 2 + NEAR, update, 0)
            strip_do(f_strip(q), start=True)

        @pl.when(idx > 0)
        def _():
            def finish(i, a):
                for g in range(2):
                    l = 2 * i + g
                    for y in range(yh):
                        ybuf[q, l, y] = total(O + l, y) * row_of(c_bs, O + l, y)
                return a

            lax.fori_loop(0, NL // 2, finish, 0)
            for l in range(per):
                for j in range(1, nq):
                    gram_copy(q, l, lax.rem(me + j, nq), me).start()

    def solve(idx, a):
        base = idx * NB * 3
        with jax.named_scope("g_P1"):
            each(begin, base)

        @pl.when(idx == 0)
        def _():
            far_layers()

        with jax.named_scope("g_far"):
            each(begin_far, idx)
        with jax.named_scope("h_E"):
            each(displace, base)
        with jax.named_scope("h_Efar"):
            each(displace_far)
        with jax.named_scope("i_P2"):
            each(again, base, idx)

        with jax.named_scope("j_far"):

            @pl.when(idx == 0)
            def _():
                each(again_far)
                wait_halo((6,))

        with jax.named_scope("k_close"):
            each(close, base, idx)
        return a

    phase()
    lax.fori_loop(0, 2, solve, 0)

    phase("l_unpack")
    hflat = hraw.reshape(NDEV * OWN * ny, LANES)
    oflat = hess.reshape(2 * NDEV * OWN * ny, LANES)

    def unpack(dst, base, at):
        def layer(i, a):
            for q in range(NB):
                for y in range(yh):
                    val = ybuf[q, at + i, y]
                    for h in range(HV):
                        dst[
                            pl.ds(
                                base + (q * ND * OWN + i) * ny + h * yh + y,
                                ND,
                                stride=OWN * ny,
                            ),
                            :,
                        ] = val[h * ND : (h + 1) * ND]
            return a

        lax.fori_loop(0, OWN, layer, 0)

    unpack(hflat, 0, OWN * (1 - c))

    def own_gram(i, a):
        for q in range(NB):
            for y in range(yh):
                grecv[me, q, i, y] = ybuf[q, per * me + i, y]
        return a

    lax.fori_loop(0, per, own_gram, 0)
    swap = remote(hraw, hess.at[pl.ds(NDEV * c, NDEV)], sem_h.at[0], sem_h.at[1], partner, d)
    swap.start()
    unpack(oflat, NDEV * c * OWN * ny, OWN * c)

    width = nq * NB * SUB
    g_all = jnp.zeros((width, width), F32)
    for l in range(per):
        phase("m_gramwait")
        for q in range(NB):
            for j in range(1, nq):
                slot = lax.rem(me + j, nq)
                gram_copy(q, l, slot, slot).wait_recv()
        phase("m_gramdot")
        for y in range(0, yh, 2):
            z = jnp.concatenate(
                [grecv[:, :, l, y + i].reshape(width, LANES) for i in range(2)], axis=1
            )
            g_all = g_all + lax.dot_general(
                z,
                z,
                (((1,), (1,)), ((), ())),
                precision=lax.Precision.HIGHEST,
                preferred_element_type=F32,
            )
    phase("m_fold")
    ndir = nq * NDEV
    fold = jnp.zeros((ndir, LANES), F32)
    for h in range(HV):
        ri = lax.broadcasted_iota(jnp.int32, (ndir, width), 0)
        ci = lax.broadcasted_iota(jnp.int32, (ndir, width), 1)
        left_sel = jnp.where(ci == (ri // ND) * SUB + h * ND + lax.rem(ri, ND), 1.0, 0.0)
        rj = lax.broadcasted_iota(jnp.int32, (width, LANES), 0)
        cj = lax.broadcasted_iota(jnp.int32, (width, LANES), 1)
        right_sel = jnp.where(
            jnp.logical_and(rj == (cj // ND) * SUB + h * ND + lax.rem(cj, ND), cj < ndir),
            1.0,
            0.0,
        )
        mid = jnp.dot(
            left_sel, g_all, precision=lax.Precision.HIGHEST, preferred_element_type=F32
        )
        fold = fold + jnp.dot(
            mid, right_sel, precision=lax.Precision.HIGHEST, preferred_element_type=F32
        )
    packed = fold[0:SUB]
    for k in range(1, ndir // SUB):
        packed = packed + pltpu.roll(fold[k * SUB : (k + 1) * SUB], ndir * k, 1)

    phase("n_ga")
    ga_src[...] = packed
    ga_buf[s] = packed

    def ga_copy(j, slot):
        peer = lax.rem(s + j, ns)
        return remote(
            ga_src, ga_buf.at[slot], sem_ga_send.at[j], sem_ga.at[slot], peer * 2 + c, d
        )

    for j in range(1, ns):
        ga_copy(j, s).start()
    for j in range(1, ns):
        ga_copy(j, lax.rem(s + j, ns)).wait_recv()
    total = ga_buf[0]
    for j in range(1, ns):
        total = total + ga_buf[j]
    phase("n_gb")
    gb_src[...] = total
    gb_buf[me] = total

    def gb_copy(j, slot):
        q = lax.rem(me + j, nq)
        return remote(
            gb_src,
            gb_buf.at[slot],
            sem_gb_send.at[j],
            sem_gb.at[slot],
            s * 2 + lax.rem(q, 2),
            q // 2,
        )

    for j in range(1, nq):
        gb_copy(j, me).start()
    for j in range(1, nq):
        gb_copy(j, lax.rem(me + j, nq)).wait_recv()
    total = gb_buf[0]
    for j in range(1, nq):
        total = total + gb_buf[j]
    total = total * (1.0 / cells)
    for k in range(ndir // SUB):
        row = total if k == 0 else pltpu.roll(total, LANES - ndir * k, 1)
        gram[k * SUB : (k + 1) * SUB] = row

    phase("o_drain")
    swap.wait_recv()
    swap.wait_send()
    for cp in part_copies():
        cp.wait_send()

    @pl.when(has_cross)
    def _():
        for cp in cross_copies():
            cp.wait_send()

    def red_sent(r, a):
        for j in range(1, ns):
            red_copy(r, j, s).wait_send()
        return a

    lax.fori_loop(0, NRED, red_sent, 0)

    def batch_sent(q, a):
        strip_do(f_strip(q), sent=True)
        for l in range(per):
            for j in range(1, nq):
                gram_copy(q, l, lax.rem(me + j, nq), me).wait_send()
        return a

    lax.fori_loop(0, NB, batch_sent, 0)
    for j in range(1, ns):
        ga_copy(j, s).wait_send()
    for j in range(1, nq):
        gb_copy(j, me).wait_send()
    phase()


PN = 4
EN = 2


def last_kernel(gram, h_in, r_out, h_out, buf, sems):
    into = pltpu.make_async_copy(h_in, buf, sems.at[0])
    into.start()
    n = r_out.shape[0]
    lane = lax.broadcasted_iota(jnp.int32, (1, LANES), 1)
    a = gram[...]
    into.wait()
    out = pltpu.make_async_copy(buf, h_out, sems.at[1])
    out.start()
    for j in range(n):
        col = jnp.broadcast_to(a[:, j : j + 1], (n, LANES))
        inv = 1.0 / jnp.sqrt(col[j : j + 1])
        row = a[j : j + 1] * inv
        r_out[j : j + 1] = jnp.where(lane >= j, row, 0.0)[:, 0:n]
        if j + 1 < n:
            a = a - (col * inv) * row
    out.wait()


def solution(mesh):
    ns = mesh.shape["tile"] // 2
    nd = mesh.shape["dir"]
    nq = 2 * nd
    ndir = nq * NDEV

    def body(probes, bs, obs, perm, mat, storage, alpha, bulk, shear):
        ny, nz = probes.shape[2:]
        yh = ny // HV
        per = NL // nq
        cells = OWN * 2 * ns * ny * nz
        vm = pl.BlockSpec(memory_space=pltpu.VMEM)
        sm = pl.BlockSpec(memory_space=pltpu.SMEM)
        anywhere = pl.BlockSpec(memory_space=pl.ANY)

        def compact(kind=F32):
            return pltpu.VMEM((LT, ny, nz), kind)

        def wide(rows=yh, pre=()):
            return pltpu.VMEM((*pre, LT, rows, SUB, nz), F32)

        dma = pltpu.SemaphoreType.DMA
        field = wide(pre=(NB,))
        scratch = [
            pltpu.VMEM(probes.shape, F32),
            pltpu.VMEM((NDEV, LT, ny, nz), F32),
            compact(),
            compact(),
            compact(),
            compact(jnp.int32),
            compact(),
            compact(),
            compact(),
            compact(),
            pltpu.VMEM((10, ny + SUB, nz), F32),
            *[wide(), wide(), wide(yh + 1), wide(), wide()] * 2,
            wide(),
            wide(),
            field,
            field,
            field,
            field,
            wide(pre=(NB, 3)),
            wide(pre=(NB, 3)),
            field,
            field,
            pltpu.VMEM((NB, NL, yh, SUB, nz), F32),
            pltpu.VMEM((NDEV, OWN, ny, nz), F32),
            pltpu.VMEM((nq, NB, per, yh, SUB, nz), F32),
            pltpu.VMEM((NB, 2, SUB, nz), F32),
            pltpu.VMEM((NRED, 1, nz), F32),
            pltpu.VMEM((NRED, ns, 1, nz), F32),
            pltpu.VMEM((SUB, nz), F32),
            pltpu.VMEM((ns, SUB, nz), F32),
            pltpu.VMEM((SUB, nz), F32),
            pltpu.VMEM((nq, SUB, nz), F32),
            dma((5 + 14,)),
            dma((5,)),
            dma((2, 7)),
            dma((NRED, ns)),
            dma((NRED, ns)),
            dma((ns,)),
            dma((ns,)),
            dma((nq,)),
            dma((nq,)),
            dma((NB, per, nq)),
            dma((NB, per, nq)),
            dma((2,)),
            dma((NB, 2)),
            dma((NB, 2)),
            dma((NB, 2)),
            dma((NB, 2)),
        ]
        hess, gram = pl.pallas_call(
            functools.partial(kernel, ns, nd, cells),
            out_shape=(
                jax.ShapeDtypeStruct(probes.shape, F32),
                jax.ShapeDtypeStruct((ndir, nz), F32),
            ),
            in_specs=[vm] * 5 + [sm] * 4,
            out_specs=(vm, vm),
            scratch_shapes=scratch,
            compiler_params=pltpu.CompilerParams(
                collective_id=0, has_side_effects=True, vmem_limit_bytes=67043328
            ),
            name="solve",
        )(probes, bs, obs, perm, mat, storage, alpha, bulk, shear)
        r_factor, hess = pl.pallas_call(
            last_kernel,
            out_shape=(
                jax.ShapeDtypeStruct((ndir, ndir), F32),
                jax.ShapeDtypeStruct(probes.shape, F32),
            ),
            in_specs=[vm, anywhere],
            out_specs=(vm, anywhere),
            scratch_shapes=[pltpu.VMEM(probes.shape, F32), dma((2,))],
            name="factor",
        )(gram, hess)
        return hess, r_factor

    return jax.shard_map(
        body,
        mesh=mesh,
        in_specs=(
            P("dir", "tile", None, None),
            P("tile", None, None),
            P("tile", None, None),
            P("tile", None, None),
            P("tile", None, None),
            P(),
            P(),
            P(),
            P(),
        ),
        out_specs=(P("dir", "tile", None, None), P()),
        check_vma=False,
    )
```

```python
import functools

import jax
import jax.numpy as jnp
from jax import lax
from jax.experimental import pallas as pl
from jax.experimental.pallas import tpu as pltpu
from jax.sharding import PartitionSpec as P

MESH = pl.DeviceIdType.MESH
F32 = jnp.float32
NCLASS = 8
LANES = 128
SUB = 8
OWN = 8
NL = 16
K = 6
O = K
E = K + NL
LT = NL + 2 * K
NB = 2
HV = 4
ND = SUB // HV
NDEV = NB * ND
NEAR = 2
NRED = 6 * NB


def kernel(
    ns,
    nd,
    cells,
    probes_at,
    bs_at,
    obs_at,
    perm_at,
    mat_at,
    t_storage,
    t_alpha,
    t_bulk,
    t_shear,
    hess,
    gram,
    probes,
    bs_in,
    obs_in,
    perm_in,
    mat_in,
    fraw,
    praw,
    c_bs,
    c_obs,
    c_perm,
    c_mat,
    c_diag,
    c_stab,
    c_hb,
    c_shear,
    c_tmp,
    pd,
    px,
    py,
    pz,
    pm,
    ed,
    ex,
    ey,
    ez,
    em,
    hb,
    st,
    f,
    w,
    v,
    p1,
    b,
    we,
    r2,
    w2,
    ybuf,
    hraw,
    hin,
    hout,
    grecv,
    wts,
    red_src,
    red_buf,
    ga_src,
    ga_buf,
    gb_src,
    gb_buf,
    sem_init_send,
    sem_part,
    sem_halo,
    sem_red_send,
    sem_red,
    sem_ga,
    sem_gb,
    sem_g_send,
    sem_g,
    sem_h,
    sem_f_send,
    sem_f,
    sem_r_send,
    sem_r,
    sem_in,
    sem_out,
):
    scope = []

    def phase(name=None):
        if scope:
            scope.pop().__exit__(None, None, None)
        if name is not None:
            scope.append(jax.named_scope(name))
            scope[0].__enter__()

    phase("a_start")
    ny = probes.shape[2]
    yh = ny // HV
    t = lax.axis_index("tile")
    d = lax.axis_index("dir")
    s = t // 2
    c = lax.rem(t, 2)
    partner = s * 2 + (1 - c)
    has_low = s > 0
    has_high = s < ns - 1

    barrier = pltpu.get_barrier_semaphore()

    def greet(tile, dr):
        pl.semaphore_signal(barrier, inc=1, device_id=(tile, dr), device_id_type=MESH)

    cross = jnp.where(c == 0, s - 1, s + 1)
    has_cross = jnp.where(c == 0, has_low, has_high)
    for j in range(1, ns):
        greet(lax.rem(s + j, ns) * 2 + c, d)
    greet(partner, d)
    for j in range(1, nd):
        dj = lax.rem(d + j, nd)
        greet(t, dj)
        greet(partner, dj)

    @pl.when(has_cross)
    def _():
        greet(cross * 2 + (1 - c), d)

    loads = [
        pltpu.make_async_copy(src, dst, sem_in.at[i])
        for i, (src, dst) in enumerate(
            (
                (mat_at, mat_in),
                (bs_at, bs_in),
                (probes_at, probes),
                (perm_at, perm_in),
                (obs_at, obs_in),
            )
        )
    ]
    for cp in loads:
        cp.start()

    own_at = O + OWN * c
    zero8 = jnp.zeros((SUB, LANES), F32)
    zc = jnp.zeros((ny, LANES), F32)
    zi = jnp.zeros((ny, LANES), jnp.int32)

    def zero_side(lo):
        def layer(i, carry):
            l = lo + i
            c_perm[l] = zc
            c_obs[l] = zc
            c_mat[l] = zi
            for dd in range(NDEV):
                praw[dd, l] = zc
            for q in range(NB):
                for y in range(yh):
                    w[q, l, y] = zero8
                    v[q, l, y] = zero8
                    r2[q, l, y] = zero8
                    w2[q, l, y] = zero8
                    for k in range(3):
                        we[q, k, l, y] = zero8
            return carry

        lax.fori_loop(0, K, layer, 0)

    @pl.when(jnp.logical_not(has_low))
    def _():
        zero_side(0)

    @pl.when(jnp.logical_not(has_high))
    def _():
        zero_side(E)

    for cp in loads:
        cp.wait()

    def products(l, a):
        sens = bs_in[l]
        for dd in range(2 * NDEV):
            fraw[dd, l] = probes[dd, l] * sens
        c_bs[own_at + l] = sens
        c_obs[own_at + l] = obs_in[l]
        c_perm[own_at + l] = perm_in[l]
        c_mat[own_at + l] = mat_in[l]
        return a

    lax.fori_loop(0, OWN, products, 0)

    lane = lax.broadcasted_iota(jnp.int32, (SUB, LANES), 1)
    sub = lax.broadcasted_iota(jnp.int32, (SUB, LANES), 0)
    part_of = sub // ND
    lane_c = lax.broadcasted_iota(jnp.int32, (ny, LANES), 1)
    row_c = lax.broadcasted_iota(jnp.int32, (ny, LANES), 0)
    last_z = lane == LANES - 1
    first_z = lane == 0

    def tables(lo, n):
        def layer(i, carry):
            l = lo + i
            m = c_mat[l]
            inside = jnp.logical_and(
                jnp.logical_or(has_low, l >= O), jnp.logical_or(has_high, l < E)
            )
            gate = jnp.where(inside, F32(1.0), F32(0.0))

            def look(table):
                val = jnp.full((ny, LANES), table[0], F32)
                for k in range(1, NCLASS):
                    val = jnp.where(m == k, table[k], val)
                return val

            biot = look(t_alpha)
            stab = biot * biot / look(t_bulk)
            c_stab[l] = stab
            c_diag[l] = (look(t_storage) + stab) * gate
            c_hb[l] = 0.5 * biot * gate
            c_shear[l] = look(t_shear) * gate
            return carry

        lax.fori_loop(0, n, layer, 0)

    phase("a_tables")
    tables(own_at, OWN)

    phase("b_barrier")
    pl.semaphore_wait(barrier, (ns - 1) + 1 + 2 * (nd - 1) + jnp.where(has_cross, 1, 0))

    def remote(src, dst, ssem, rsem, tile, dr):
        return pltpu.make_async_remote_copy(
            src_ref=src,
            dst_ref=dst,
            send_sem=ssem,
            recv_sem=rsem,
            device_id=(tile, dr),
            device_id_type=MESH,
        )

    def part_copies():
        pairs = ((perm_in, c_perm), (mat_in, c_mat), (None, praw), (bs_in, c_bs), (obs_in, c_obs))
        out = []
        for i, (src, dst) in enumerate(pairs):
            if src is None:
                src = fraw.at[pl.ds(NDEV * (1 - c), NDEV)]
                dst = dst.at[:, pl.ds(own_at, OWN)]
            else:
                dst = dst.at[pl.ds(own_at, OWN)]
            out.append(remote(src, dst, sem_init_send.at[i], sem_part.at[i], partner, d))
        return out

    def halo_copies(side, slab, near, far, cores, only=None):
        jobs = []
        for n, (src, dst) in enumerate(((perm_in, c_perm), (mat_in, c_mat), (None, praw))):
            jobs.append((n, src, dst, *near, NEAR))
        for n, (src, dst) in enumerate(((perm_in, c_perm), (mat_in, c_mat), (None, praw))):
            jobs.append((3 + n, src, dst, *far, K - NEAR))
        jobs.append((6, obs_in, c_obs, *near, NEAR))
        out = []
        for n, src, dst, at, to, size in jobs:
            if only is not None and n not in only:
                continue
            for core in cores:
                if src is None:
                    a = fraw.at[pl.ds(NDEV * core, NDEV), pl.ds(at, size)]
                    z = praw.at[:, pl.ds(to, size)]
                else:
                    a = src.at[pl.ds(at, size)]
                    z = dst.at[pl.ds(to, size)]
                out.append(
                    remote(
                        a,
                        z,
                        sem_init_send.at[5 + 2 * n + core],
                        sem_halo.at[side, n],
                        slab * 2 + core,
                        d,
                    )
                )
        return out

    def cross_copies():
        return halo_copies(
            1 - c,
            cross,
            ((OWN - NEAR) * c, jnp.where(c == 0, E, O - NEAR)),
            (jnp.where(c == 0, NEAR, OWN - K), jnp.where(c == 0, E + NEAR, 0)),
            (0, 1),
        )

    phase("c_sends")

    @pl.when(has_cross)
    def _():
        for cp in cross_copies():
            cp.start()

    for cp in part_copies():
        cp.start()

    def wait_halo(only):
        @pl.when(has_low)
        def _():
            for cp in halo_copies(0, s, (OWN - NEAR, O - NEAR), (OWN - K, 0), (0,), only):
                cp.wait_recv()

        @pl.when(has_high)
        def _():
            for cp in halo_copies(1, s, (0, E), (NEAR, E + NEAR), (0,), only):
                cp.wait_recv()

    def wide_row(read, y):
        val = jnp.broadcast_to(read(y), (SUB, LANES))
        for h in range(1, HV):
            more = jnp.broadcast_to(read(y + h * yh), (SUB, LANES))
            val = jnp.where(part_of >= h, more, val)
        return val

    def row_of(ref, l, y):
        return wide_row(lambda y: ref[l, pl.ds(y, 1), :], y)

    def spread_rows(dst, l, idx, rows=None):
        for y in range(yh if rows is None else rows):
            dst[l, y] = row_of(c_tmp, idx, y)

    def faces_layer(l, src, diag, dd, dx, dy, dz, dm, at):
        mid = src[l]
        xp = 0.5 * (mid + src[l + 1])
        xm = 0.5 * (mid + src[l - 1])
        up = jnp.where(row_c == ny - 1, 0.0, pltpu.roll(mid, ny - 1, 0))
        dn = jnp.where(row_c == 0, 0.0, pltpu.roll(mid, 1, 0))
        yp = 0.5 * (mid + up)
        ym = 0.5 * (mid + dn)
        rt = jnp.where(lane_c == LANES - 1, 0.0, pltpu.roll(mid, LANES - 1, 1))
        lf = jnp.where(lane_c == 0, 0.0, pltpu.roll(mid, 1, 1))
        zp = 0.5 * (mid + rt)
        zm = 0.5 * (mid + lf)
        total = xp + xm + yp + ym + zp + zm
        if diag is not None:
            total = total + diag[l]
        c_tmp[at, 0:ny] = total
        c_tmp[at + 1, 0:ny] = xp
        c_tmp[at + 2, 0:ny] = ym
        c_tmp[at + 2, ny : ny + SUB] = jnp.broadcast_to(
            0.5 * mid[ny - 1 : ny], (SUB, LANES)
        )
        c_tmp[at + 3, 0:ny] = jnp.where(lane_c == LANES - 1, 0.0, zp)
        c_tmp[at + 4, 0:ny] = jnp.where(lane_c == 0, 0.0, zm)
        return lambda: (
            spread_rows(dd, l, at),
            spread_rows(dx, l, at + 1),
            spread_rows(dy, l, at + 2, yh + 1),
            spread_rows(dz, l, at + 3),
            spread_rows(dm, l, at + 4),
        )

    def faces(lo, n):
        def layer(i, carry):
            l = lo + i
            done = (
                faces_layer(l, c_perm, c_diag, pd, px, py, pz, pm, 0),
                faces_layer(l, c_shear, None, ed, ex, ey, ez, em, 5),
            )
            for y in range(yh):
                hb[l, y] = row_of(c_hb, l, y)
                st[l, y] = row_of(c_stab, l, y)
            for make in done:
                make()
            return carry

        lax.fori_loop(0, n, layer, 0)

    def x_faces(l):
        c_tmp[1, 0:ny] = 0.5 * (c_perm[l] + c_perm[l + 1])
        c_tmp[6, 0:ny] = 0.5 * (c_shear[l] + c_shear[l + 1])
        spread_rows(px, l, 1)
        spread_rows(ex, l, 6)

    def source(lo, n, raw=praw, first=0, shift=0, layers=LT):
        flat = raw.reshape(raw.shape[0] * layers * ny, LANES)

        def layer(i, carry):
            l = lo + i
            for q in range(NB):
                for y in range(yh):
                    base = ((first + q * ND) * layers + (l - shift)) * ny + y
                    f[q, l, y] = jnp.concatenate(
                        [
                            flat[pl.ds(base + h * yh, ND, stride=layers * ny), :]
                            for h in range(HV)
                        ],
                        axis=0,
                    )
            return carry

        lax.fori_loop(0, n, layer, 0)

    phase("d_own")
    faces(own_at + 1, OWN - 2)
    source(own_at, OWN, fraw, NDEV * c, own_at, OWN)
    phase("d_wait_part")
    for cp in part_copies():
        cp.wait_recv()
    phase("d_other")
    other_at = O + OWN * (1 - c)
    tables(other_at, OWN)
    faces(jnp.where(c == 0, O + OWN - 1, O + 1), OWN)
    source(other_at, OWN)
    phase("d_wait_near")
    wait_halo((0, 1, 2))
    phase("d_near")
    tables(O - NEAR, NEAR)
    tables(E, NEAR)
    faces(O - 1, 2)
    faces(E - 1, 2)
    x_faces(O - 2)
    source(O - NEAR, NEAR)
    source(E, NEAR)

    def far_layers():
        wait_halo((3, 4, 5))
        tables(0, K - NEAR)
        tables(E + NEAR, K - NEAR)
        faces(1, K - NEAR)
        faces(E + 1, K - NEAR)
        x_faces(0)
        source(0, K - NEAR)
        source(E + NEAR, K - NEAR)

    class Rows:
        def __init__(self, ref, l0, pre=()):
            self.ref, self.l0, self.pre, self.got = ref, l0, pre, {}

        def load(self, g, y):
            return self.ref[(*self.pre, self.l0 + g, y)]

        def __call__(self, g, y):
            if (g, y) not in self.got:
                if y == -1:
                    self.got[g, y] = jnp.where(
                        part_of > 0, pltpu.roll(self(g, yh - 1), ND, 0), 0.0
                    )
                elif y == yh:
                    self.got[g, y] = jnp.where(
                        part_of < HV - 1, pltpu.roll(self(g, 0), SUB - ND, 0), 0.0
                    )
                else:
                    self.got[g, y] = self.load(g, y)
            return self.got[g, y]

    class Made(Rows):
        def __init__(self, make):
            self.make, self.got = make, {}

        def load(self, g, y):
            return self.make(g, y)

    def left(x):
        return pltpu.roll(x, 1, 1)

    def right(x):
        return pltpu.roll(x, LANES - 1, 1)

    p_ops = (pd, px, py, pz, pm)
    e_ops = (ed, ex, ey, ez, em)

    def group(ops, vals, l0, n, emit):
        cd, cx, cy, cz, cm = (Rows(o, l0).load for o in ops)
        cx, cy = Rows(ops[1], l0), Made(cy)
        for y in range(yh):
            for g in range(n):
                co = [
                    op(g, y) for op in (cd, cz, cm)
                ]
                c_up = ops[2][l0 + g, y + 1]
                c_dn = ops[2][l0 + g, y]
                for k, val in enumerate(vals):
                    x = val(g, y)
                    out = co[0] * x
                    out = out - co[1] * right(x)
                    out = out - co[2] * left(x)
                    out = out - cx(g, y) * val(g + 1, y)
                    out = out - cx(g - 1, y) * val(g - 1, y)
                    out = out - c_up * val(g, y + 1)
                    out = out - c_dn * val(g, y - 1)
                    emit(k, g, y, x, out)

    def own_loop(n, body, init):
        return lax.fori_loop(0, NL // n, lambda i, a: body(O + i * n, n, a), init)

    def halo_loop(k, n, body, far=0):
        trips = (k - far) // n

        @pl.when(has_low)
        def _():
            lax.fori_loop(0, trips, lambda i, a: body(O - k + i * n, n, a), 0)

        @pl.when(has_high)
        def _():
            lax.fori_loop(0, trips, lambda i, a: body(E + far + i * n, n, a), 0)

    def pres(q, comps):
        return [(q,)] if comps is None else [(q, k) for k in range(comps)]

    def first_pass(q, ops, src, dst, comps, n):
        pre = pres(q, comps)

        def body(l0, n, acc):
            acc = list(acc)

            def emit(k, g, y, x, out):
                dst[(*pre[k], l0 + g, y)] = out
                acc[0] = acc[0] + x * x
                acc[1] = acc[1] + x * out
                acc[2] = acc[2] + out * out

            group(ops, [Rows(src, l0, k) for k in pre], l0, n, emit)
            return tuple(acc)

        return own_loop(n, body, (zero8,) * 3)

    def halo_pass(q, ops, src, dst, comps, k, n, far=0):
        pre = pres(q, comps)

        def body(l0, n, acc):
            def emit(kk, g, y, x, out):
                dst[(*pre[kk], l0 + g, y)] = out

            group(ops, [Rows(src, l0, kk) for kk in pre], l0, n, emit)
            return acc

        halo_loop(k, n, body, far)

    def second_pass(q, ops, src, comps, n, dst=None):
        pre = pres(q, comps)

        def body(l0, n, acc):
            acc = list(acc)

            def emit(k, g, y, x, out):
                acc[0] = acc[0] + x * out
                if dst is not None:
                    dst[q, l0 + g, y] = out

            group(ops, [Rows(src, l0, k) for k in pre], l0, n, emit)
            return tuple(acc)

        return own_loop(n, body, (zero8,))

    GAP = LANES // SUB
    packed_at = lane // GAP == sub

    def red_copy(r, j, slot):
        peer = lax.rem(s + j, ns)
        return remote(
            red_src.at[r],
            red_buf.at[r, slot],
            sem_red_send.at[r],
            sem_red.at[r],
            peer * 2 + c,
            d,
        )

    def whole(block, ssem, rsem):
        return remote(block, block, ssem, rsem, partner, d)

    def red_all(r):
        return whole(red_buf.at[r, pl.ds(0, ns - 1)], sem_red_send.at[r], sem_red.at[r])

    def red_start(r, moments):
        row = jnp.zeros((SUB, LANES), F32)
        for m, acc in enumerate(moments):
            total = jnp.sum(acc, axis=1, keepdims=True)
            row = row + jnp.where(
                jnp.logical_and(packed_at, lax.rem(lane, GAP) == m), total, 0.0
            )
        packed = jnp.sum(row, axis=0, keepdims=True)
        red_src[r] = packed
        red_buf[r, s] = packed
        for j in range(1, ns):
            red_copy(r, j, s).start()

    def red_wait(r):
        red_all(r).wait_recv()
        total = red_buf[r, 0]
        for j in range(1, ns):
            total = total + red_buf[r, j]
        full = jnp.where(packed_at, jnp.broadcast_to(total, (SUB, LANES)), 0.0)
        out = []
        for m in range(4):
            val = jnp.sum(
                jnp.where(lax.rem(lane, GAP) == m, full, 0.0), axis=1, keepdims=True
            )
            val = jnp.broadcast_to(val, (SUB, LANES))
            both = val
            for h in range(1, HV):
                both = both + pltpu.roll(val, ND * h, 0)
            out.append(both)
        return out

    def weights(moments):
        m0, m1, m2, m3 = moments
        a0 = m0 / m1
        rr = a0 * a0 * m2 - m0
        beta1 = 1.0 + rr / m0
        dw = beta1 * beta1 * m1 - 2.0 * beta1 * a0 * m2 + a0 * a0 * m3
        a1 = rr / dw
        return a0 + a1 * beta1, -a1 * a0

    def strip(q, buf, at, to, size, ssem, rsem):
        low = remote(
            buf.at[q, pl.ds(O + at, size)],
            buf.at[q, pl.ds(E + to, size)],
            ssem.at[q, 0],
            rsem.at[q, 1],
            jnp.where(has_low, t - 2, t + 2),
            d,
        )
        high = remote(
            buf.at[q, pl.ds(E - at - size, size)],
            buf.at[q, pl.ds(O - to - size, size)],
            ssem.at[q, 1],
            rsem.at[q, 0],
            jnp.where(has_high, t + 2, t - 2),
            d,
        )
        return low, high

    def strip_do(args, start=False, recv=False, sent=False):
        low, high = strip(*args)

        @pl.when(has_low)
        def _():
            if start:
                low.start()
            if recv:
                high.wait_recv()
            if sent:
                low.wait_send()

        @pl.when(has_high)
        def _():
            if start:
                high.start()
            if recv:
                low.wait_recv()
            if sent:
                high.wait_send()

    def f_strip(q):
        return q, f, NEAR, NEAR, K - NEAR, sem_f_send, sem_f

    def r_strip(q):
        return q, r2, 2, 2, 1, sem_r_send, sem_r

    me = d * 2 + c
    nq = 2 * nd
    per = NL // nq

    def gram_copy(bt, l, q, slot):
        return remote(
            ybuf.at[bt, per * q + l],
            grecv.at[slot, bt, l],
            sem_g_send.at[bt, l],
            sem_g.at[bt, l],
            s * 2 + lax.rem(q, 2),
            q // 2,
        )

    def gram_all(bt, l):
        return whole(
            grecv.at[pl.ds(0, nq - 1), bt, l], sem_g_send.at[bt, l], sem_g.at[bt, l]
        )

    def each(stage, *args):
        def go(q, a):
            stage(q, *args)
            return a

        lax.fori_loop(0, NB, go, 0)

    def save(q, at, pair):
        for i in range(2):
            wts[q, at + i] = pair[i]

    def begin(q, base):
        mo = first_pass(q, p_ops, f, w, None, PN)
        halo_pass(q, p_ops, f, w, None, 1, 1)
        (m3,) = second_pass(q, p_ops, w, None, PN, v)
        red_start(base + q, (*mo, m3))

    def begin_far(q, idx):
        @pl.when(idx > 0)
        def _():
            strip_do(f_strip(q), recv=True)

        halo_pass(q, p_ops, f, w, None, K - 1, K - 2, 1)
        halo_pass(q, p_ops, w, v, None, 2, 2)

    def displace(q, base):
        y0, y1 = weights(red_wait(base + q))
        save(q, 0, (y0, y1))

        def press(i, a):
            for g in range(2):
                l = 1 + 2 * i + g
                for y in range(yh):
                    p1[q, l, y] = y0 * f[q, l, y] + y1 * w[q, l, y]
            return a

        lax.fori_loop(0, (LT - 2) // 2, press, 0)

        def grad(i, a):
            l0 = 2 + 4 * i
            val = Rows(p1, l0, (q,))
            for y in range(yh):
                for g in range(4):
                    coef = hb[l0 + g, y]
                    x = val(g, y)
                    b[q, 0, l0 + g, y] = coef * (val(g + 1, y) - val(g - 1, y))
                    b[q, 1, l0 + g, y] = coef * (val(g, y + 1) - val(g, y - 1))
                    b[q, 2, l0 + g, y] = coef * (
                        jnp.where(last_z, 0.0, right(x)) - jnp.where(first_z, 0.0, left(x))
                    )
            return a

        lax.fori_loop(0, (LT - 4) // 4, grad, 0)
        mo = first_pass(q, e_ops, b, we, 3, EN)
        halo_pass(q, e_ops, b, we, 3, 1, 1)
        (m3,) = second_pass(q, e_ops, we, 3, EN)
        red_start(base + NB + q, (*mo, m3))

    def displace_far(q):
        halo_pass(q, e_ops, b, we, 3, K - 3, 2, 1)

    def again(q, base, idx):
        z0, z1 = weights(red_wait(base + NB + q))
        y0, y1 = wts[q, 0], wts[q, 1]

        def resid(l0, n, a):
            def flow(k):
                def make(g, y):
                    l = l0 + g
                    return hb[l, y] * (z0 * b[q, k, l, y] + z1 * we[q, k, l, y])

                return Made(make)

            fx, fy, fz = flow(0), flow(1), flow(2)
            for y in range(yh):
                for g in range(n):
                    l = l0 + g
                    tz = fz(g, y)
                    div = fx(g - 1, y) - fx(g + 1, y)
                    div = div + (fy(g, y - 1) - fy(g, y + 1))
                    div = div + (
                        jnp.where(first_z, 0.0, left(tz)) - jnp.where(last_z, 0.0, right(tz))
                    )
                    image = y0 * w[q, l, y] + y1 * v[q, l, y]
                    r2[q, l, y] = f[q, l, y] - div + st[l, y] * p1[q, l, y] - image
            return a

        own_loop(4, resid, 0)
        halo_loop(2, 2, resid)
        mo = first_pass(q, p_ops, r2, w2, None, PN)

        @pl.when(idx == 0)
        def _():
            strip_do(r_strip(q), start=True)

        halo_pass(q, p_ops, r2, w2, None, 1, 1)
        (m3,) = second_pass(q, p_ops, w2, None, PN)
        red_start(base + 2 * NB + q, (*mo, m3))

    def again_far(q):
        strip_do(r_strip(q), recv=True, sent=True)
        halo_pass(q, p_ops, r2, w2, None, 2, 1, 1)

    def close(q, base, idx):
        x0, x1 = weights(red_wait(base + 2 * NB + q))

        def total(l, y):
            return p1[q, l, y] + x0 * r2[q, l, y] + x1 * w2[q, l, y]

        @pl.when(idx == 0)
        def _():
            def update(i, a):
                for g in range(2):
                    l = O - NEAR + 2 * i + g
                    for y in range(yh):
                        f[q, l, y] = total(l, y) * row_of(c_obs, l, y)
                return a

            lax.fori_loop(0, NL // 2 + NEAR, update, 0)
            strip_do(f_strip(q), start=True)

        @pl.when(idx > 0)
        def _():
            def finish(i, a):
                for g in range(2):
                    l = 2 * i + g
                    for y in range(yh):
                        ybuf[q, l, y] = total(O + l, y) * row_of(c_bs, O + l, y)
                return a

            lax.fori_loop(0, NL // 2, finish, 0)
            for l in range(per):
                for j in range(1, nq):
                    gram_copy(q, l, lax.rem(me + j, nq), me).start()

    def solve(idx, a):
        base = idx * NB * 3
        with jax.named_scope("g_P1"):
            each(begin, base)

        @pl.when(idx == 0)
        def _():
            far_layers()

        with jax.named_scope("g_far"):
            each(begin_far, idx)
        with jax.named_scope("h_E"):
            each(displace, base)
        with jax.named_scope("h_Efar"):
            each(displace_far)
        with jax.named_scope("i_P2"):
            each(again, base, idx)

        with jax.named_scope("j_far"):

            @pl.when(idx == 0)
            def _():
                each(again_far)
                wait_halo((6,))

        with jax.named_scope("k_close"):
            each(close, base, idx)
        return a

    phase()
    lax.fori_loop(0, 2, solve, 0)

    phase("l_unpack")

    def unpack(dst, at):
        flat = dst.reshape(NDEV * OWN * ny, LANES)

        def layer(i, a):
            for q in range(NB):
                for y in range(yh):
                    val = ybuf[q, at + i, y]
                    for h in range(HV):
                        row = (q * ND * OWN + i) * ny + h * yh + y
                        flat[pl.ds(row, ND, stride=OWN * ny), :] = val[h * ND : (h + 1) * ND]
            return a

        lax.fori_loop(0, OWN, layer, 0)

    def own_gram(i, a):
        for q in range(NB):
            for y in range(yh):
                grecv[me, q, i, y] = ybuf[q, per * me + i, y]
        return a

    unpack(hraw, OWN * (1 - c))
    unpack(hout, OWN * c)
    swap = remote(hraw, hin, sem_h.at[0], sem_h.at[1], partner, d)
    swap.start()
    lax.fori_loop(0, per, own_gram, 0)
    put = pltpu.make_async_copy(hout, hess.at[pl.ds(NDEV * c, NDEV)], sem_out.at[0])
    put.start()
    put_in = pltpu.make_async_copy(hin, hess.at[pl.ds(NDEV * (1 - c), NDEV)], sem_out.at[1])

    width = nq * NB * SUB
    g_all = jnp.zeros((width, width), F32)
    for l in range(per):
        phase("m_gramwait")
        for q in range(NB):
            gram_all(q, l).wait_recv()
        if l == 0:
            swap.wait_recv()
            put_in.start()
        phase("m_gramdot")
        for y in range(0, yh, 2):
            z = jnp.concatenate(
                [grecv[:, :, l, y + i].reshape(width, LANES) for i in range(2)], axis=1
            )
            g_all = g_all + lax.dot_general(
                z,
                z,
                (((1,), (1,)), ((), ())),
                precision=lax.Precision.HIGHEST,
                preferred_element_type=F32,
            )
    phase("m_fold")
    ndir = nq * NDEV
    fold = jnp.zeros((ndir, LANES), F32)
    for h in range(HV):
        ri = lax.broadcasted_iota(jnp.int32, (ndir, width), 0)
        ci = lax.broadcasted_iota(jnp.int32, (ndir, width), 1)
        left_sel = jnp.where(ci == (ri // ND) * SUB + h * ND + lax.rem(ri, ND), 1.0, 0.0)
        rj = lax.broadcasted_iota(jnp.int32, (width, LANES), 0)
        cj = lax.broadcasted_iota(jnp.int32, (width, LANES), 1)
        right_sel = jnp.where(
            jnp.logical_and(rj == (cj // ND) * SUB + h * ND + lax.rem(cj, ND), cj < ndir),
            1.0,
            0.0,
        )
        mid = jnp.dot(
            left_sel, g_all, precision=lax.Precision.HIGHEST, preferred_element_type=F32
        )
        fold = fold + jnp.dot(
            mid, right_sel, precision=lax.Precision.HIGHEST, preferred_element_type=F32
        )
    packed = fold[0:SUB]
    for k in range(1, ndir // SUB):
        packed = packed + pltpu.roll(fold[k * SUB : (k + 1) * SUB], ndir * k, 1)

    phase("n_ga")
    ga_src[...] = packed
    ga_buf[s] = packed

    def ga_copy(j, slot):
        peer = lax.rem(s + j, ns)
        return remote(
            ga_src, ga_buf.at[slot], sem_ga.at[0], sem_ga.at[1], peer * 2 + c, d
        )

    for j in range(1, ns):
        ga_copy(j, s).start()
    ga_all = whole(ga_buf.at[pl.ds(0, ns - 1)], sem_ga.at[0], sem_ga.at[1])
    ga_all.wait_recv()
    total = ga_buf[0]
    for j in range(1, ns):
        total = total + ga_buf[j]
    phase("n_gb")
    gb_src[...] = total
    gb_buf[me] = total

    def gb_copy(j, slot):
        q = lax.rem(me + j, nq)
        return remote(
            gb_src,
            gb_buf.at[slot],
            sem_gb.at[0],
            sem_gb.at[1],
            s * 2 + lax.rem(q, 2),
            q // 2,
        )

    for j in range(1, nq):
        gb_copy(j, me).start()
    gb_all = whole(gb_buf.at[pl.ds(0, nq - 1)], sem_gb.at[0], sem_gb.at[1])
    gb_all.wait_recv()
    total = gb_buf[0]
    for j in range(1, nq):
        total = total + gb_buf[j]
    total = total * (1.0 / cells)
    for k in range(ndir // SUB):
        row = total if k == 0 else pltpu.roll(total, LANES - ndir * k, 1)
        gram[k * SUB : (k + 1) * SUB] = row

    phase("o_drain")
    swap.wait_send()
    put.wait()
    put_in.wait()
    for cp in part_copies():
        cp.wait_send()

    @pl.when(has_cross)
    def _():
        for cp in cross_copies():
            cp.wait_send()

    def red_sent(r, a):
        red_all(r).wait_send()
        return a

    lax.fori_loop(0, NRED, red_sent, 0)

    def batch_sent(q, a):
        strip_do(f_strip(q), sent=True)
        for l in range(per):
            gram_all(q, l).wait_send()
        return a

    lax.fori_loop(0, NB, batch_sent, 0)
    ga_all.wait_send()
    gb_all.wait_send()
    phase()


PN = 4
EN = 4


AHEAD = 3


def last_kernel(gram, h_in, r_out, h_out, buf, sems):
    parts = h_in.shape[0] // 2
    at = [pl.ds(2 * i, 2) for i in range(parts)]
    into = [pltpu.make_async_copy(h_in.at[p], buf.at[p], sems.at[0, i]) for i, p in enumerate(at)]
    out = [pltpu.make_async_copy(buf.at[p], h_out.at[p], sems.at[1, i]) for i, p in enumerate(at)]
    for cp in into:
        cp.start()
    n = r_out.shape[0]
    lane = lax.broadcasted_iota(jnp.int32, (1, LANES), 1)
    a = gram[...]

    def wide(x, j):
        return jnp.broadcast_to(x[:, j : j + 1], (n, LANES))

    cols = {j: (wide(a, j), 0) for j in range(AHEAD)}
    done = []
    for j in range(n):
        col, first = cols.pop(j)
        for m in range(first, j):
            col = col - done[m] * done[m][j : j + 1]
        inv = lax.rsqrt(col[j : j + 1])
        inv = inv * (1.5 - 0.5 * col[j : j + 1] * inv * inv)
        col = col * inv
        done.append(col)
        row = a[j : j + 1] * inv
        r_out[j : j + 1] = jnp.where(lane >= j, row, 0.0)[:, 0:n]
        a = a - col * row
        if j + AHEAD < n:
            cols[j + AHEAD] = (wide(a, j + AHEAD), j + 1)
        if j % 4 == 3 and j // 4 < parts:
            into[j // 4].wait()
            out[j // 4].start()
    for cp in out:
        cp.wait()


def solution(mesh):
    ns = mesh.shape["tile"] // 2
    nd = mesh.shape["dir"]
    nq = 2 * nd
    ndir = nq * NDEV

    def body(probes, bs, obs, perm, mat, storage, alpha, bulk, shear):
        ny, nz = probes.shape[2:]
        yh = ny // HV
        per = NL // nq
        cells = OWN * 2 * ns * ny * nz
        vm = pl.BlockSpec(memory_space=pltpu.VMEM)
        sm = pl.BlockSpec(memory_space=pltpu.SMEM)
        anywhere = pl.BlockSpec(memory_space=pl.ANY)

        def compact(kind=F32):
            return pltpu.VMEM((LT, ny, nz), kind)

        def wide(rows=yh, pre=()):
            return pltpu.VMEM((*pre, LT, rows, SUB, nz), F32)

        dma = pltpu.SemaphoreType.DMA
        field = wide(pre=(NB,))
        scratch = [
            pltpu.VMEM(probes.shape, F32),
            *[pltpu.VMEM(x.shape, x.dtype) for x in (bs, obs, perm, mat)],
            pltpu.VMEM(probes.shape, F32),
            pltpu.VMEM((NDEV, LT, ny, nz), F32),
            compact(),
            compact(),
            compact(),
            compact(jnp.int32),
            compact(),
            compact(),
            compact(),
            compact(),
            pltpu.VMEM((10, ny + SUB, nz), F32),
            *[wide(), wide(), wide(yh + 1), wide(), wide()] * 2,
            wide(),
            wide(),
            field,
            field,
            field,
            field,
            wide(pre=(NB, 3)),
            wide(pre=(NB, 3)),
            field,
            field,
            pltpu.VMEM((NB, NL, yh, SUB, nz), F32),
            *[pltpu.VMEM((NDEV, OWN, ny, nz), F32)] * 3,
            pltpu.VMEM((nq, NB, per, yh, SUB, nz), F32),
            pltpu.VMEM((NB, 2, SUB, nz), F32),
            pltpu.VMEM((NRED, 1, nz), F32),
            pltpu.VMEM((NRED, ns, 1, nz), F32),
            pltpu.VMEM((SUB, nz), F32),
            pltpu.VMEM((ns, SUB, nz), F32),
            pltpu.VMEM((SUB, nz), F32),
            pltpu.VMEM((nq, SUB, nz), F32),
            dma((5 + 14,)),
            dma((5,)),
            dma((2, 7)),
            dma((NRED,)),
            dma((NRED,)),
            dma((2,)),
            dma((2,)),
            dma((NB, per)),
            dma((NB, per)),
            dma((2,)),
            dma((NB, 2)),
            dma((NB, 2)),
            dma((NB, 2)),
            dma((NB, 2)),
            dma((5,)),
            dma((2,)),
        ]
        hess, gram = pl.pallas_call(
            functools.partial(kernel, ns, nd, cells),
            out_shape=(
                jax.ShapeDtypeStruct(probes.shape, F32),
                jax.ShapeDtypeStruct((ndir, nz), F32),
            ),
            in_specs=[anywhere] * 5 + [sm] * 4,
            out_specs=(anywhere, vm),
            scratch_shapes=scratch,
            compiler_params=pltpu.CompilerParams(
                collective_id=0, has_side_effects=True, vmem_limit_bytes=67043328
            ),
            name="solve",
        )(probes, bs, obs, perm, mat, storage, alpha, bulk, shear)
        r_factor, hess = pl.pallas_call(
            last_kernel,
            out_shape=(
                jax.ShapeDtypeStruct((ndir, ndir), F32),
                jax.ShapeDtypeStruct(probes.shape, F32),
            ),
            in_specs=[vm, anywhere],
            out_specs=(vm, anywhere),
            scratch_shapes=[pltpu.VMEM(probes.shape, F32), dma((2, probes.shape[0] // 2))],
            name="factor",
        )(gram, hess)
        return hess, r_factor

    return jax.shard_map(
        body,
        mesh=mesh,
        in_specs=(
            P("dir", "tile", None, None),
            P("tile", None, None),
            P("tile", None, None),
            P("tile", None, None),
            P("tile", None, None),
            P(),
            P(),
            P(),
            P(),
        ),
        out_specs=(P("dir", "tile", None, None), P()),
        check_vma=False,
    )
```

```python
import functools

import jax
import jax.numpy as jnp
from jax import lax
from jax.experimental import pallas as pl
from jax.experimental.pallas import tpu as pltpu
from jax.sharding import PartitionSpec as P

MESH = pl.DeviceIdType.MESH
F32 = jnp.float32
NCLASS = 8
LANES = 128
SUB = 8
OWN = 8
NL = 16
K = 6
O = K
E = K + NL
LT = NL + 2 * K
NB = 4
HV = 8
ND = SUB // HV
NDEV = NB * ND
NEAR = 2
NRED = 6 * NB


def kernel(
    ns,
    nd,
    cells,
    probes_at,
    bs_at,
    obs_at,
    perm_at,
    mat_at,
    t_storage,
    t_alpha,
    t_bulk,
    t_shear,
    hess,
    gram,
    probes,
    bs_in,
    obs_in,
    perm_in,
    mat_in,
    fraw,
    praw,
    c_bs,
    c_obs,
    c_perm,
    c_mat,
    c_diag,
    c_stab,
    c_hb,
    c_shear,
    c_tmp,
    pd,
    px,
    py,
    pz,
    pm,
    ed,
    ex,
    ey,
    ez,
    em,
    hb,
    st,
    f,
    w,
    v,
    p1,
    b,
    we,
    r2,
    w2,
    ybuf,
    hraw,
    hin,
    hout,
    grecv,
    wts,
    red_src,
    red_buf,
    ga_src,
    ga_buf,
    gb_src,
    gb_buf,
    sem_init_send,
    sem_part,
    sem_halo,
    sem_red_send,
    sem_red,
    sem_ga,
    sem_gb,
    sem_g_send,
    sem_g,
    sem_h,
    sem_f_send,
    sem_f,
    sem_r_send,
    sem_r,
    sem_in,
    sem_out,
):
    scope = []

    def phase(name=None):
        if scope:
            scope.pop().__exit__(None, None, None)
        if name is not None:
            scope.append(jax.named_scope(name))
            scope[0].__enter__()

    phase("a_start")
    ny = probes.shape[2]
    yh = ny // HV
    t = lax.axis_index("tile")
    d = lax.axis_index("dir")
    s = t // 2
    c = lax.rem(t, 2)
    partner = s * 2 + (1 - c)
    has_low = s > 0
    has_high = s < ns - 1

    barrier = pltpu.get_barrier_semaphore()

    def greet(tile, dr):
        pl.semaphore_signal(barrier, inc=1, device_id=(tile, dr), device_id_type=MESH)

    cross = jnp.where(c == 0, s - 1, s + 1)
    has_cross = jnp.where(c == 0, has_low, has_high)
    for j in range(1, ns):
        greet(lax.rem(s + j, ns) * 2 + c, d)
    greet(partner, d)
    for j in range(1, nd):
        dj = lax.rem(d + j, nd)
        greet(t, dj)
        greet(partner, dj)

    @pl.when(has_cross)
    def _():
        greet(cross * 2 + (1 - c), d)

    loads = [
        pltpu.make_async_copy(src, dst, sem_in.at[i])
        for i, (src, dst) in enumerate(
            (
                (mat_at, mat_in),
                (bs_at, bs_in),
                (probes_at, probes),
                (perm_at, perm_in),
                (obs_at, obs_in),
            )
        )
    ]
    for cp in loads:
        cp.start()

    own_at = O + OWN * c
    zero8 = jnp.zeros((SUB, LANES), F32)
    zc = jnp.zeros((ny, LANES), F32)
    zi = jnp.zeros((ny, LANES), jnp.int32)

    def zero_side(lo):
        def layer(i, carry):
            l = lo + i
            c_perm[l] = zc
            c_obs[l] = zc
            c_mat[l] = zi
            for dd in range(NDEV):
                praw[dd, l] = zc
            for q in range(NB):
                for y in range(yh):
                    w[q, l, y] = zero8
                    v[q, l, y] = zero8
                    r2[q, l, y] = zero8
                    w2[q, l, y] = zero8
                    for k in range(3):
                        we[q, k, l, y] = zero8
            return carry

        lax.fori_loop(0, K, layer, 0)

    @pl.when(jnp.logical_not(has_low))
    def _():
        zero_side(0)

    @pl.when(jnp.logical_not(has_high))
    def _():
        zero_side(E)

    for cp in loads:
        cp.wait()

    def products(l, a):
        sens = bs_in[l]
        for dd in range(2 * NDEV):
            fraw[dd, l] = probes[dd, l] * sens
        c_bs[own_at + l] = sens
        c_obs[own_at + l] = obs_in[l]
        c_perm[own_at + l] = perm_in[l]
        c_mat[own_at + l] = mat_in[l]
        return a

    lax.fori_loop(0, OWN, products, 0)

    lane = lax.broadcasted_iota(jnp.int32, (SUB, LANES), 1)
    sub = lax.broadcasted_iota(jnp.int32, (SUB, LANES), 0)
    part_of = sub // ND
    lane_c = lax.broadcasted_iota(jnp.int32, (ny, LANES), 1)
    row_c = lax.broadcasted_iota(jnp.int32, (ny, LANES), 0)
    last_z = lane == LANES - 1
    first_z = lane == 0

    def tables(lo, n):
        def layer(i, carry):
            l = lo + i
            m = c_mat[l]
            inside = jnp.logical_and(
                jnp.logical_or(has_low, l >= O), jnp.logical_or(has_high, l < E)
            )
            gate = jnp.where(inside, F32(1.0), F32(0.0))

            def look(table):
                val = jnp.full((ny, LANES), table[0], F32)
                for k in range(1, NCLASS):
                    val = jnp.where(m == k, table[k], val)
                return val

            biot = look(t_alpha)
            stab = biot * biot / look(t_bulk)
            c_stab[l] = stab
            c_diag[l] = (look(t_storage) + stab) * gate
            c_hb[l] = 0.5 * biot * gate
            c_shear[l] = look(t_shear) * gate
            return carry

        lax.fori_loop(0, n, layer, 0)

    phase("a_tables")
    tables(own_at, OWN)

    phase("b_barrier")
    pl.semaphore_wait(barrier, (ns - 1) + 1 + 2 * (nd - 1) + jnp.where(has_cross, 1, 0))

    def remote(src, dst, ssem, rsem, tile, dr):
        return pltpu.make_async_remote_copy(
            src_ref=src,
            dst_ref=dst,
            send_sem=ssem,
            recv_sem=rsem,
            device_id=(tile, dr),
            device_id_type=MESH,
        )

    def part_copies():
        pairs = ((perm_in, c_perm), (mat_in, c_mat), (None, praw), (bs_in, c_bs), (obs_in, c_obs))
        out = []
        for i, (src, dst) in enumerate(pairs):
            if src is None:
                src = fraw.at[pl.ds(NDEV * (1 - c), NDEV)]
                dst = dst.at[:, pl.ds(own_at, OWN)]
            else:
                dst = dst.at[pl.ds(own_at, OWN)]
            out.append(remote(src, dst, sem_init_send.at[i], sem_part.at[i], partner, d))
        return out

    def halo_copies(side, slab, near, far, cores, only=None):
        jobs = []
        for n, (src, dst) in enumerate(((perm_in, c_perm), (mat_in, c_mat), (None, praw))):
            jobs.append((n, src, dst, *near, NEAR))
        for n, (src, dst) in enumerate(((perm_in, c_perm), (mat_in, c_mat), (None, praw))):
            jobs.append((3 + n, src, dst, *far, K - NEAR))
        jobs.append((6, obs_in, c_obs, *near, NEAR))
        out = []
        for n, src, dst, at, to, size in jobs:
            if only is not None and n not in only:
                continue
            for core in cores:
                if src is None:
                    a = fraw.at[pl.ds(NDEV * core, NDEV), pl.ds(at, size)]
                    z = praw.at[:, pl.ds(to, size)]
                else:
                    a = src.at[pl.ds(at, size)]
                    z = dst.at[pl.ds(to, size)]
                out.append(
                    remote(
                        a,
                        z,
                        sem_init_send.at[5 + 2 * n + core],
                        sem_halo.at[side, n],
                        slab * 2 + core,
                        d,
                    )
                )
        return out

    def cross_copies():
        return halo_copies(
            1 - c,
            cross,
            ((OWN - NEAR) * c, jnp.where(c == 0, E, O - NEAR)),
            (jnp.where(c == 0, NEAR, OWN - K), jnp.where(c == 0, E + NEAR, 0)),
            (0, 1),
        )

    phase("c_sends")

    @pl.when(has_cross)
    def _():
        for cp in cross_copies():
            cp.start()

    for cp in part_copies():
        cp.start()

    def wait_halo(only):
        @pl.when(has_low)
        def _():
            for cp in halo_copies(0, s, (OWN - NEAR, O - NEAR), (OWN - K, 0), (0,), only):
                cp.wait_recv()

        @pl.when(has_high)
        def _():
            for cp in halo_copies(1, s, (0, E), (NEAR, E + NEAR), (0,), only):
                cp.wait_recv()

    def row_of(ref, l, y):
        return ref[l, pl.ds(y, HV, stride=yh), :]

    def spread_rows(dst, l, idx, rows=None):
        for y in range(yh if rows is None else rows):
            dst[l, y] = row_of(c_tmp, idx, y)

    def faces_layer(l, src, diag, dd, dx, dy, dz, dm, at):
        mid = src[l]
        xp = 0.5 * (mid + src[l + 1])
        xm = 0.5 * (mid + src[l - 1])
        up = jnp.where(row_c == ny - 1, 0.0, pltpu.roll(mid, ny - 1, 0))
        dn = jnp.where(row_c == 0, 0.0, pltpu.roll(mid, 1, 0))
        yp = 0.5 * (mid + up)
        ym = 0.5 * (mid + dn)
        rt = jnp.where(lane_c == LANES - 1, 0.0, pltpu.roll(mid, LANES - 1, 1))
        lf = jnp.where(lane_c == 0, 0.0, pltpu.roll(mid, 1, 1))
        zp = 0.5 * (mid + rt)
        zm = 0.5 * (mid + lf)
        total = xp + xm + yp + ym + zp + zm
        if diag is not None:
            total = total + diag[l]
        c_tmp[at, 0:ny] = total
        c_tmp[at + 1, 0:ny] = xp
        c_tmp[at + 2, 0:ny] = ym
        c_tmp[at + 2, ny : ny + SUB] = jnp.broadcast_to(
            0.5 * mid[ny - 1 : ny], (SUB, LANES)
        )
        c_tmp[at + 3, 0:ny] = jnp.where(lane_c == LANES - 1, 0.0, zp)
        c_tmp[at + 4, 0:ny] = jnp.where(lane_c == 0, 0.0, zm)
        return lambda: (
            spread_rows(dd, l, at),
            spread_rows(dx, l, at + 1),
            spread_rows(dy, l, at + 2, yh + 1),
            spread_rows(dz, l, at + 3),
            spread_rows(dm, l, at + 4),
        )

    def faces(lo, n):
        def layer(i, carry):
            l = lo + i
            done = (
                faces_layer(l, c_perm, c_diag, pd, px, py, pz, pm, 0),
                faces_layer(l, c_shear, None, ed, ex, ey, ez, em, 5),
            )
            for y in range(yh):
                hb[l, y] = row_of(c_hb, l, y)
                st[l, y] = row_of(c_stab, l, y)
            for make in done:
                make()
            return carry

        lax.fori_loop(0, n, layer, 0)

    def x_faces(l):
        c_tmp[1, 0:ny] = 0.5 * (c_perm[l] + c_perm[l + 1])
        c_tmp[6, 0:ny] = 0.5 * (c_shear[l] + c_shear[l + 1])
        spread_rows(px, l, 1)
        spread_rows(ex, l, 6)

    def source(lo, n, raw=praw, first=0, shift=0, layers=LT):
        flat = raw.reshape(raw.shape[0] * layers * ny, LANES)

        def layer(i, carry):
            l = lo + i
            for q in range(NB):
                for y in range(yh):
                    row = ((first + q) * layers + (l - shift)) * ny + y
                    f[q, l, y] = flat[pl.ds(row, HV, stride=yh), :]
            return carry

        lax.fori_loop(0, n, layer, 0)

    phase("d_own")
    faces(own_at + 1, OWN - 2)
    source(own_at, OWN, fraw, NDEV * c, own_at, OWN)
    phase("d_wait_part")
    parts = part_copies()
    for i in (0, 1):
        parts[i].wait_recv()
    phase("d_other")
    other_at = O + OWN * (1 - c)
    tables(other_at, OWN)
    faces(jnp.where(c == 0, O + OWN - 1, O + 1), OWN)
    for i in (2, 3, 4):
        parts[i].wait_recv()
    source(other_at, OWN)
    phase("d_wait_near")
    wait_halo((0, 1))
    tables(O - NEAR, NEAR)
    tables(E, NEAR)
    faces(O - 1, 2)
    faces(E - 1, 2)
    x_faces(O - 2)
    phase("d_near")
    wait_halo((2,))
    source(O - NEAR, NEAR)
    source(E, NEAR)

    def far_layers():
        wait_halo((3, 4))
        tables(0, K - NEAR)
        tables(E + NEAR, K - NEAR)
        faces(1, K - NEAR)
        faces(E + 1, K - NEAR)
        x_faces(0)
        wait_halo((5,))
        source(0, K - NEAR)
        source(E + NEAR, K - NEAR)

    class Rows:
        def __init__(self, ref, l0, pre=()):
            self.ref, self.l0, self.pre, self.got = ref, l0, pre, {}

        def load(self, g, y):
            return self.ref[(*self.pre, self.l0 + g, y)]

        def __call__(self, g, y):
            if (g, y) not in self.got:
                if y == -1:
                    self.got[g, y] = jnp.where(
                        part_of > 0, pltpu.roll(self(g, yh - 1), ND, 0), 0.0
                    )
                elif y == yh:
                    self.got[g, y] = jnp.where(
                        part_of < HV - 1, pltpu.roll(self(g, 0), SUB - ND, 0), 0.0
                    )
                else:
                    self.got[g, y] = self.load(g, y)
            return self.got[g, y]

    class Made(Rows):
        def __init__(self, make):
            self.make, self.got = make, {}

        def load(self, g, y):
            return self.make(g, y)

    def left(x):
        return pltpu.roll(x, 1, 1)

    def right(x):
        return pltpu.roll(x, LANES - 1, 1)

    p_ops = (pd, px, py, pz, pm)
    e_ops = (ed, ex, ey, ez, em)

    def group(ops, vals, l0, n, emit):
        cd, cx, cy, cz, cm = (Rows(o, l0).load for o in ops)
        cx, cy = Rows(ops[1], l0), Made(cy)
        for y in range(yh):
            for g in range(n):
                co = [
                    op(g, y) for op in (cd, cz, cm)
                ]
                c_up = ops[2][l0 + g, y + 1]
                c_dn = ops[2][l0 + g, y]
                for k, val in enumerate(vals):
                    x = val(g, y)
                    out = co[0] * x
                    out = out - co[1] * right(x)
                    out = out - co[2] * left(x)
                    out = out - cx(g, y) * val(g + 1, y)
                    out = out - cx(g - 1, y) * val(g - 1, y)
                    out = out - c_up * val(g, y + 1)
                    out = out - c_dn * val(g, y - 1)
                    emit(k, g, y, x, out)

    def own_loop(n, body, init):
        return lax.fori_loop(0, NL // n, lambda i, a: body(O + i * n, n, a), init)

    def both_halos(k, far, body, outs):
        n = k - far
        body(O - k, n)
        body(E + far, n)

        def clear(at):
            for ref, pre in outs:
                for g in range(n):
                    for y in range(yh):
                        ref[(*pre, at + g, y)] = zero8

        @pl.when(jnp.logical_not(has_low))
        def _():
            clear(O - k)

        @pl.when(jnp.logical_not(has_high))
        def _():
            clear(E + far)

    def pres(q, comps):
        return [(q,)] if comps is None else [(q, k) for k in range(comps)]

    def first_pass(q, ops, src, dst, comps, n):
        pre = pres(q, comps)

        def body(l0, n, acc):
            acc = list(acc)

            def emit(k, g, y, x, out):
                dst[(*pre[k], l0 + g, y)] = out
                acc[0] = acc[0] + x * x
                acc[1] = acc[1] + x * out
                acc[2] = acc[2] + out * out

            group(ops, [Rows(src, l0, k) for k in pre], l0, n, emit)
            return tuple(acc)

        return own_loop(n, body, (zero8,) * 3)

    def halo_pass(q, ops, src, dst, comps, k, far=0):
        pre = pres(q, comps)

        def body(l0, n):
            def emit(kk, g, y, x, out):
                dst[(*pre[kk], l0 + g, y)] = out

            group(ops, [Rows(src, l0, kk) for kk in pre], l0, n, emit)

        both_halos(k, far, body, [(dst, p) for p in pre])

    def second_pass(q, ops, src, comps, n, dst=None):
        pre = pres(q, comps)

        def body(l0, n, acc):
            acc = list(acc)

            def emit(k, g, y, x, out):
                acc[0] = acc[0] + x * out
                if dst is not None:
                    dst[q, l0 + g, y] = out

            group(ops, [Rows(src, l0, k) for k in pre], l0, n, emit)
            return tuple(acc)

        return own_loop(n, body, (zero8,))

    def red_copy(r, j, slot):
        peer = lax.rem(s + j, ns)
        return remote(
            red_src.at[r],
            red_buf.at[r, slot],
            sem_red_send.at[r],
            sem_red.at[r],
            peer * 2 + c,
            d,
        )

    def whole(block, ssem, rsem):
        return remote(block, block, ssem, rsem, partner, d)

    def red_all(r):
        return whole(red_buf.at[r, pl.ds(0, ns - 1)], sem_red_send.at[r], sem_red.at[r])

    def red_start(r, moments):
        packed = jnp.concatenate([jnp.sum(acc, axis=0, keepdims=True) for acc in moments], axis=0)
        red_src[r] = packed
        red_buf[r, s] = packed
        for j in range(1, ns):
            red_copy(r, j, s).start()

    def red_wait(r):
        red_all(r).wait_recv()
        sums = [red_buf[r, j] for j in range(ns)]
        while len(sums) > 1:
            sums = [x + y for x, y in zip(sums[::2], sums[1::2])]
        total = jnp.sum(sums[0], axis=1, keepdims=True)
        return [jnp.broadcast_to(total[m : m + 1], (SUB, LANES)) for m in range(4)]

    def weights(moments):
        m0, m1, m2, m3 = moments
        a0 = m0 / m1
        rr = a0 * a0 * m2 - m0
        beta1 = 1.0 + rr / m0
        dw = beta1 * beta1 * m1 - 2.0 * beta1 * a0 * m2 + a0 * a0 * m3
        a1 = rr / dw
        return a0 + a1 * beta1, -a1 * a0

    def strip(q, buf, at, to, size, ssem, rsem):
        low = remote(
            buf.at[q, pl.ds(O + at, size)],
            buf.at[q, pl.ds(E + to, size)],
            ssem.at[q, 0],
            rsem.at[q, 1],
            jnp.where(has_low, t - 2, t + 2),
            d,
        )
        high = remote(
            buf.at[q, pl.ds(E - at - size, size)],
            buf.at[q, pl.ds(O - to - size, size)],
            ssem.at[q, 1],
            rsem.at[q, 0],
            jnp.where(has_high, t + 2, t - 2),
            d,
        )
        return low, high

    def strip_do(args, start=False, recv=False, sent=False):
        low, high = strip(*args)

        @pl.when(has_low)
        def _():
            if start:
                low.start()
            if recv:
                high.wait_recv()
            if sent:
                low.wait_send()

        @pl.when(has_high)
        def _():
            if start:
                high.start()
            if recv:
                low.wait_recv()
            if sent:
                high.wait_send()

    def f_strip(q):
        return q, f, NEAR, NEAR, K - NEAR, sem_f_send, sem_f

    def r_strip(q):
        return q, r2, 2, 2, 1, sem_r_send, sem_r

    me = d * 2 + c
    nq = 2 * nd
    per = NL // nq

    def gram_copy(bt, l, q, slot):
        return remote(
            ybuf.at[bt, per * q + l],
            grecv.at[slot, bt, l],
            sem_g_send.at[bt, l],
            sem_g.at[bt, l],
            s * 2 + lax.rem(q, 2),
            q // 2,
        )

    def gram_all(bt, l):
        return whole(
            grecv.at[pl.ds(0, nq - 1), bt, l], sem_g_send.at[bt, l], sem_g.at[bt, l]
        )

    def each(stage, *args):
        def go(q, a):
            stage(q, *args)
            return a

        lax.fori_loop(0, NB, go, 0)

    def save(q, at, pair):
        for i in range(2):
            wts[q, at + i] = pair[i]

    def begin(q, base):
        mo = first_pass(q, p_ops, f, w, None, PN)
        halo_pass(q, p_ops, f, w, None, 1)
        (m3,) = second_pass(q, p_ops, w, None, PN, v)
        red_start(base + q, (*mo, m3))

    def begin_far(q, idx):
        @pl.when(idx > 0)
        def _():
            strip_do(f_strip(q), recv=True)

        halo_pass(q, p_ops, f, w, None, K - 1, 1)
        halo_pass(q, p_ops, w, v, None, 2)

    def displace(q, base):
        y0, y1 = weights(red_wait(base + q))
        save(q, 0, (y0, y1))

        def press(i, a):
            for g in range(13):
                l = 1 + 13 * i + g
                for y in range(yh):
                    p1[q, l, y] = y0 * f[q, l, y] + y1 * w[q, l, y]
            return a

        lax.fori_loop(0, (LT - 2) // 13, press, 0)

        def grad(i, a):
            l0 = 2 + 8 * i
            val = Rows(p1, l0, (q,))
            for y in range(yh):
                for g in range(8):
                    coef = hb[l0 + g, y]
                    x = val(g, y)
                    b[q, 0, l0 + g, y] = coef * (val(g + 1, y) - val(g - 1, y))
                    b[q, 1, l0 + g, y] = coef * (val(g, y + 1) - val(g, y - 1))
                    b[q, 2, l0 + g, y] = coef * (
                        jnp.where(last_z, 0.0, right(x)) - jnp.where(first_z, 0.0, left(x))
                    )
            return a

        lax.fori_loop(0, (LT - 4) // 8, grad, 0)
        mo = first_pass(q, e_ops, b, we, 3, EN)
        halo_pass(q, e_ops, b, we, 3, 1)
        (m3,) = second_pass(q, e_ops, we, 3, EN)
        red_start(base + NB + q, (*mo, m3))

    def displace_far(q):
        halo_pass(q, e_ops, b, we, 3, K - 3, 1)

    def again(q, base, idx):
        z0, z1 = weights(red_wait(base + NB + q))
        y0, y1 = wts[q, 0], wts[q, 1]

        def resid(l0, n, a):
            def flow(k):
                def make(g, y):
                    l = l0 + g
                    return hb[l, y] * (z0 * b[q, k, l, y] + z1 * we[q, k, l, y])

                return Made(make)

            fx, fy, fz = flow(0), flow(1), flow(2)
            for y in range(yh):
                for g in range(n):
                    l = l0 + g
                    tz = fz(g, y)
                    div = fx(g - 1, y) - fx(g + 1, y)
                    div = div + (fy(g, y - 1) - fy(g, y + 1))
                    div = div + (
                        jnp.where(first_z, 0.0, left(tz)) - jnp.where(last_z, 0.0, right(tz))
                    )
                    image = y0 * w[q, l, y] + y1 * v[q, l, y]
                    r2[q, l, y] = f[q, l, y] - div + st[l, y] * p1[q, l, y] - image
            return a

        own_loop(8, resid, 0)
        both_halos(2, 0, lambda l0, n: resid(l0, n, 0), [(r2, (q,))])
        mo = first_pass(q, p_ops, r2, w2, None, PN)

        @pl.when(idx == 0)
        def _():
            strip_do(r_strip(q), start=True)

        halo_pass(q, p_ops, r2, w2, None, 1)
        (m3,) = second_pass(q, p_ops, w2, None, PN)
        red_start(base + 2 * NB + q, (*mo, m3))

    def again_far(q):
        strip_do(r_strip(q), recv=True, sent=True)
        halo_pass(q, p_ops, r2, w2, None, 2, 1)

    def close(q, base, idx):
        x0, x1 = weights(red_wait(base + 2 * NB + q))

        def total(l, y):
            return p1[q, l, y] + x0 * r2[q, l, y] + x1 * w2[q, l, y]

        @pl.when(idx == 0)
        def _():
            def update(i, a):
                for g in range(4):
                    l = O - NEAR + 4 * i + g
                    for y in range(yh):
                        f[q, l, y] = total(l, y) * row_of(c_obs, l, y)
                return a

            lax.fori_loop(0, (NL + 2 * NEAR) // 4, update, 0)
            strip_do(f_strip(q), start=True)
            begin(q, base + NB * 3)

        @pl.when(idx > 0)
        def _():
            def finish(i, a):
                for g in range(4):
                    l = 4 * i + g
                    for y in range(yh):
                        ybuf[q, l, y] = total(O + l, y) * row_of(c_bs, O + l, y)
                return a

            lax.fori_loop(0, NL // 4, finish, 0)
            for l in range(per):
                for j in range(1, nq):
                    gram_copy(q, l, lax.rem(me + j, nq), me).start()

    def solve(idx, a):
        base = idx * NB * 3
        @pl.when(idx == 0)
        def _():
            far_layers()

        with jax.named_scope("g_far"):
            each(begin_far, idx)
        with jax.named_scope("h_E"):
            each(displace, base)
        with jax.named_scope("h_Efar"):
            each(displace_far)
        with jax.named_scope("i_P2"):
            each(again, base, idx)

        with jax.named_scope("j_far"):

            @pl.when(idx == 0)
            def _():
                each(again_far)
                wait_halo((6,))

        with jax.named_scope("k_close"):
            each(close, base, idx)
        return a

    phase("g_P1")
    each(begin, 0)
    phase()
    lax.fori_loop(0, 2, solve, 0)

    phase("l_unpack")

    def unpack(dst, at):
        flat = dst.reshape(NDEV * OWN * ny, LANES)

        def layer(i, a):
            for q in range(NB):
                for y in range(yh):
                    row = (q * OWN + i) * ny + y
                    flat[pl.ds(row, HV, stride=yh), :] = ybuf[q, at + i, y]
            return a

        lax.fori_loop(0, OWN, layer, 0)

    def own_gram(i, a):
        for q in range(NB):
            for y in range(yh):
                grecv[me, q, i, y] = ybuf[q, per * me + i, y]
        return a

    unpack(hraw, OWN * (1 - c))
    unpack(hout, OWN * c)
    swap = remote(hraw, hin, sem_h.at[0], sem_h.at[1], partner, d)
    swap.start()
    lax.fori_loop(0, per, own_gram, 0)
    put = pltpu.make_async_copy(hout, hess.at[pl.ds(NDEV * c, NDEV)], sem_out.at[0])
    put.start()
    put_in = pltpu.make_async_copy(hin, hess.at[pl.ds(NDEV * (1 - c), NDEV)], sem_out.at[1])

    ndir = nq * NDEV
    step = per * yh * SUB
    gflat = grecv.reshape(ndir * step, LANES)
    g_all = jnp.zeros((ndir, ndir), F32)
    for l in range(per):
        phase("m_gramwait")
        for q in range(NB):
            gram_all(q, l).wait_recv()
        if l == 0:
            swap.wait_recv()
            put_in.start()
        phase("m_gramdot")
        for y in range(yh):
            z = jnp.concatenate(
                [
                    gflat[pl.ds((l * yh + y) * SUB + h, ndir, stride=step), :]
                    for h in range(SUB)
                ],
                axis=1,
            )
            g_all = g_all + lax.dot_general(
                z,
                z,
                (((1,), (1,)), ((), ())),
                precision=lax.Precision.HIGHEST,
                preferred_element_type=F32,
            )
    packed = jnp.concatenate(
        [g_all[k * SUB : (k + 1) * SUB] for k in range(ndir // SUB)], axis=1
    )

    phase("n_ga")
    ga_src[...] = packed
    ga_buf[s] = packed

    def ga_copy(j, slot):
        peer = lax.rem(s + j, ns)
        return remote(
            ga_src, ga_buf.at[slot], sem_ga.at[0], sem_ga.at[1], peer * 2 + c, d
        )

    for j in range(1, ns):
        ga_copy(j, s).start()
    ga_all = whole(ga_buf.at[pl.ds(0, ns - 1)], sem_ga.at[0], sem_ga.at[1])
    ga_all.wait_recv()
    total = ga_buf[0]
    for j in range(1, ns):
        total = total + ga_buf[j]
    phase("n_gb")
    gb_src[...] = total
    gb_buf[me] = total

    def gb_copy(j, slot):
        q = lax.rem(me + j, nq)
        return remote(
            gb_src,
            gb_buf.at[slot],
            sem_gb.at[0],
            sem_gb.at[1],
            s * 2 + lax.rem(q, 2),
            q // 2,
        )

    for j in range(1, nq):
        gb_copy(j, me).start()
    gb_all = whole(gb_buf.at[pl.ds(0, nq - 1)], sem_gb.at[0], sem_gb.at[1])
    gb_all.wait_recv()
    total = gb_buf[0]
    for j in range(1, nq):
        total = total + gb_buf[j]
    total = total * (1.0 / cells)
    for k in range(ndir // SUB):
        row = total if k == 0 else pltpu.roll(total, LANES - ndir * k, 1)
        gram[k * SUB : (k + 1) * SUB] = row

    phase("o_drain")
    swap.wait_send()
    put.wait()
    put_in.wait()
    for cp in part_copies():
        cp.wait_send()

    @pl.when(has_cross)
    def _():
        for cp in cross_copies():
            cp.wait_send()

    def red_sent(r, a):
        red_all(r).wait_send()
        return a

    lax.fori_loop(0, NRED, red_sent, 0)

    def batch_sent(q, a):
        strip_do(f_strip(q), sent=True)
        for l in range(per):
            gram_all(q, l).wait_send()
        return a

    lax.fori_loop(0, NB, batch_sent, 0)
    ga_all.wait_send()
    gb_all.wait_send()
    phase()


PN = 8
EN = 8


AHEAD = 3


def last_kernel(gram, h_in, r_out, h_out, buf, sems):
    parts = h_in.shape[0] // 2
    at = [pl.ds(2 * i, 2) for i in range(parts)]
    into = [pltpu.make_async_copy(h_in.at[p], buf.at[p], sems.at[0, i]) for i, p in enumerate(at)]
    out = [pltpu.make_async_copy(buf.at[p], h_out.at[p], sems.at[1, i]) for i, p in enumerate(at)]
    for cp in into:
        cp.start()
    n = r_out.shape[0]
    lane = lax.broadcasted_iota(jnp.int32, (1, LANES), 1)
    a = gram[...]

    def wide(x, j):
        return jnp.broadcast_to(x[:, j : j + 1], (n, LANES))

    cols = {j: (wide(a, j), 0) for j in range(AHEAD)}
    done = []
    for j in range(n):
        col, first = cols.pop(j)
        for m in range(first, j):
            col = col - done[m] * done[m][j : j + 1]
        inv = lax.rsqrt(col[j : j + 1])
        inv = inv * (1.5 - 0.5 * col[j : j + 1] * inv * inv)
        col = col * inv
        done.append(col)
        row = a[j : j + 1] * inv
        r_out[j : j + 1] = jnp.where(lane >= j, row, 0.0)[:, 0:n]
        a = a - col * row
        if j + AHEAD < n:
            cols[j + AHEAD] = (wide(a, j + AHEAD), j + 1)
        if j % 4 == 3 and j // 4 < parts:
            into[j // 4].wait()
            out[j // 4].start()
    for cp in out:
        cp.wait()


def solution(mesh):
    ns = mesh.shape["tile"] // 2
    nd = mesh.shape["dir"]
    nq = 2 * nd
    ndir = nq * NDEV

    def body(probes, bs, obs, perm, mat, storage, alpha, bulk, shear):
        ny, nz = probes.shape[2:]
        yh = ny // HV
        per = NL // nq
        cells = OWN * 2 * ns * ny * nz
        vm = pl.BlockSpec(memory_space=pltpu.VMEM)
        sm = pl.BlockSpec(memory_space=pltpu.SMEM)
        anywhere = pl.BlockSpec(memory_space=pl.ANY)

        def compact(kind=F32):
            return pltpu.VMEM((LT, ny, nz), kind)

        def wide(rows=yh, pre=()):
            return pltpu.VMEM((*pre, LT, rows, SUB, nz), F32)

        dma = pltpu.SemaphoreType.DMA
        field = wide(pre=(NB,))
        scratch = [
            pltpu.VMEM(probes.shape, F32),
            *[pltpu.VMEM(x.shape, x.dtype) for x in (bs, obs, perm, mat)],
            pltpu.VMEM(probes.shape, F32),
            pltpu.VMEM((NDEV, LT, ny, nz), F32),
            compact(),
            compact(),
            compact(),
            compact(jnp.int32),
            compact(),
            compact(),
            compact(),
            compact(),
            pltpu.VMEM((10, ny + SUB, nz), F32),
            *[wide(), wide(), wide(yh + 1), wide(), wide()] * 2,
            wide(),
            wide(),
            field,
            field,
            field,
            field,
            wide(pre=(NB, 3)),
            wide(pre=(NB, 3)),
            field,
            field,
            pltpu.VMEM((NB, NL, yh, SUB, nz), F32),
            *[pltpu.VMEM((NDEV, OWN, ny, nz), F32)] * 3,
            pltpu.VMEM((nq, NB, per, yh, SUB, nz), F32),
            pltpu.VMEM((NB, 2, SUB, nz), F32),
            pltpu.VMEM((NRED, 4, nz), F32),
            pltpu.VMEM((NRED, ns, 4, nz), F32),
            pltpu.VMEM((SUB, nz), F32),
            pltpu.VMEM((ns, SUB, nz), F32),
            pltpu.VMEM((SUB, nz), F32),
            pltpu.VMEM((nq, SUB, nz), F32),
            dma((5 + 14,)),
            dma((5,)),
            dma((2, 7)),
            dma((NRED,)),
            dma((NRED,)),
            dma((2,)),
            dma((2,)),
            dma((NB, per)),
            dma((NB, per)),
            dma((2,)),
            dma((NB, 2)),
            dma((NB, 2)),
            dma((NB, 2)),
            dma((NB, 2)),
            dma((5,)),
            dma((2,)),
        ]
        hess, gram = pl.pallas_call(
            functools.partial(kernel, ns, nd, cells),
            out_shape=(
                jax.ShapeDtypeStruct(probes.shape, F32),
                jax.ShapeDtypeStruct((ndir, nz), F32),
            ),
            in_specs=[anywhere] * 5 + [sm] * 4,
            out_specs=(anywhere, vm),
            scratch_shapes=scratch,
            compiler_params=pltpu.CompilerParams(
                collective_id=0, has_side_effects=True, vmem_limit_bytes=67043328
            ),
            name="solve",
        )(probes, bs, obs, perm, mat, storage, alpha, bulk, shear)
        r_factor, hess = pl.pallas_call(
            last_kernel,
            out_shape=(
                jax.ShapeDtypeStruct((ndir, ndir), F32),
                jax.ShapeDtypeStruct(probes.shape, F32),
            ),
            in_specs=[vm, anywhere],
            out_specs=(vm, anywhere),
            scratch_shapes=[pltpu.VMEM(probes.shape, F32), dma((2, probes.shape[0] // 2))],
            name="factor",
        )(gram, hess)
        return hess, r_factor

    return jax.shard_map(
        body,
        mesh=mesh,
        in_specs=(
            P("dir", "tile", None, None),
            P("tile", None, None),
            P("tile", None, None),
            P("tile", None, None),
            P("tile", None, None),
            P(),
            P(),
            P(),
            P(),
        ),
        out_specs=(P("dir", "tile", None, None), P()),
        check_vma=False,
    )
```

```python
import functools

import jax
import jax.numpy as jnp
from jax import lax
from jax.experimental import pallas as pl
from jax.experimental.pallas import tpu as pltpu
from jax.sharding import PartitionSpec as P

MESH = pl.DeviceIdType.MESH
F32 = jnp.float32
NCLASS = 8
LANES = 128
SUB = 8
OWN = 8
NL = 16
K = 6
O = K
E = K + NL
LT = NL + 2 * K
NB = 4
HV = 8
ND = SUB // HV
NDEV = NB * ND
NEAR = 2
NRED = 6 * NB


def kernel(
    ns,
    nd,
    cells,
    probes_at,
    bs_at,
    obs_at,
    perm_at,
    mat_at,
    t_storage,
    t_alpha,
    t_bulk,
    t_shear,
    hess,
    gram,
    probes,
    bs_in,
    obs_in,
    perm_in,
    mat_in,
    fraw,
    praw,
    c_bs,
    c_obs,
    c_perm,
    c_mat,
    c_diag,
    c_stab,
    c_hb,
    c_shear,
    c_tmp,
    pd,
    px,
    py,
    pz,
    pm,
    ed,
    ex,
    ey,
    ez,
    em,
    hb,
    st,
    f,
    w,
    v,
    p1,
    b,
    we,
    r2,
    w2,
    ybuf,
    hraw,
    hin,
    hout,
    grecv,
    wts,
    red_src,
    red_buf,
    ga_src,
    ga_buf,
    gb_src,
    gb_buf,
    sem_init_send,
    sem_part,
    sem_halo,
    sem_red_send,
    sem_red,
    sem_ga,
    sem_gb,
    sem_g_send,
    sem_g,
    sem_h,
    sem_f_send,
    sem_f,
    sem_r_send,
    sem_r,
    sem_in,
    sem_out,
):
    scope = []

    def phase(name=None):
        if scope:
            scope.pop().__exit__(None, None, None)
        if name is not None:
            scope.append(jax.named_scope(name))
            scope[0].__enter__()

    phase("a_start")
    ny = probes.shape[2]
    yh = ny // HV
    t = lax.axis_index("tile")
    d = lax.axis_index("dir")
    s = t // 2
    c = lax.rem(t, 2)
    partner = s * 2 + (1 - c)
    has_low = s > 0
    has_high = s < ns - 1

    barrier = pltpu.get_barrier_semaphore()

    def greet(tile, dr):
        pl.semaphore_signal(barrier, inc=1, device_id=(tile, dr), device_id_type=MESH)

    cross = jnp.where(c == 0, s - 1, s + 1)
    has_cross = jnp.where(c == 0, has_low, has_high)
    for j in range(1, ns):
        greet(lax.rem(s + j, ns) * 2 + c, d)
    greet(partner, d)
    for j in range(1, nd):
        dj = lax.rem(d + j, nd)
        greet(t, dj)
        greet(partner, dj)

    @pl.when(has_cross)
    def _():
        greet(cross * 2 + (1 - c), d)

    loads = [
        pltpu.make_async_copy(src, dst, sem_in.at[i])
        for i, (src, dst) in enumerate(
            (
                (mat_at, mat_in),
                (bs_at, bs_in),
                (probes_at, probes),
                (perm_at, perm_in),
                (obs_at, obs_in),
            )
        )
    ]
    for cp in loads:
        cp.start()

    own_at = O + OWN * c
    zero8 = jnp.zeros((SUB, LANES), F32)
    zc = jnp.zeros((ny, LANES), F32)
    zi = jnp.zeros((ny, LANES), jnp.int32)

    def zero_side(lo):
        def layer(i, carry):
            l = lo + i
            c_perm[l] = zc
            c_obs[l] = zc
            c_mat[l] = zi
            for dd in range(NDEV):
                praw[dd, l] = zc
            for q in range(NB):
                for y in range(yh):
                    w[q, l, y] = zero8
                    v[q, l, y] = zero8
                    r2[q, l, y] = zero8
                    w2[q, l, y] = zero8
                    for k in range(3):
                        we[q, k, l, y] = zero8
            return carry

        lax.fori_loop(0, K, layer, 0)

    @pl.when(jnp.logical_not(has_low))
    def _():
        zero_side(0)

    @pl.when(jnp.logical_not(has_high))
    def _():
        zero_side(E)

    for cp in loads:
        cp.wait()

    def products(l, a):
        sens = bs_in[l]
        for dd in range(2 * NDEV):
            fraw[dd, l] = probes[dd, l] * sens
        c_bs[own_at + l] = sens
        c_obs[own_at + l] = obs_in[l]
        c_perm[own_at + l] = perm_in[l]
        c_mat[own_at + l] = mat_in[l]
        return a

    lax.fori_loop(0, OWN, products, 0)

    lane = lax.broadcasted_iota(jnp.int32, (SUB, LANES), 1)
    sub = lax.broadcasted_iota(jnp.int32, (SUB, LANES), 0)
    part_of = sub // ND
    lane_c = lax.broadcasted_iota(jnp.int32, (ny, LANES), 1)
    row_c = lax.broadcasted_iota(jnp.int32, (ny, LANES), 0)
    last_z = lane == LANES - 1
    first_z = lane == 0

    def tables(lo, n):
        def layer(i, carry):
            l = lo + i
            m = c_mat[l]
            inside = jnp.logical_and(
                jnp.logical_or(has_low, l >= O), jnp.logical_or(has_high, l < E)
            )
            gate = jnp.where(inside, F32(1.0), F32(0.0))

            def look(table):
                val = jnp.full((ny, LANES), table[0], F32)
                for k in range(1, NCLASS):
                    val = jnp.where(m == k, table[k], val)
                return val

            biot = look(t_alpha)
            stab = biot * biot / look(t_bulk)
            c_stab[l] = stab
            c_diag[l] = (look(t_storage) + stab) * gate
            c_hb[l] = 0.5 * biot * gate
            c_shear[l] = look(t_shear) * gate
            return carry

        lax.fori_loop(0, n, layer, 0)

    phase("a_tables")
    tables(own_at, OWN)

    phase("b_barrier")
    pl.semaphore_wait(barrier, (ns - 1) + 1 + 2 * (nd - 1) + jnp.where(has_cross, 1, 0))

    def remote(src, dst, ssem, rsem, tile, dr):
        return pltpu.make_async_remote_copy(
            src_ref=src,
            dst_ref=dst,
            send_sem=ssem,
            recv_sem=rsem,
            device_id=(tile, dr),
            device_id_type=MESH,
        )

    def part_copies():
        pairs = ((perm_in, c_perm), (mat_in, c_mat), (None, praw), (bs_in, c_bs), (obs_in, c_obs))
        out = []
        for i, (src, dst) in enumerate(pairs):
            if src is None:
                src = fraw.at[pl.ds(NDEV * (1 - c), NDEV)]
                dst = dst.at[:, pl.ds(own_at, OWN)]
            else:
                dst = dst.at[pl.ds(own_at, OWN)]
            out.append(remote(src, dst, sem_init_send.at[i], sem_part.at[i], partner, d))
        return out

    def halo_copies(side, slab, near, far, cores, only=None):
        jobs = []
        for n, (src, dst) in enumerate(((perm_in, c_perm), (mat_in, c_mat), (None, praw))):
            jobs.append((n, src, dst, *near, NEAR))
        for n, (src, dst) in enumerate(((perm_in, c_perm), (mat_in, c_mat), (None, praw))):
            jobs.append((3 + n, src, dst, *far, K - NEAR))
        jobs.append((6, obs_in, c_obs, *near, NEAR))
        out = []
        for n, src, dst, at, to, size in jobs:
            if only is not None and n not in only:
                continue
            for core in cores:
                if src is None:
                    a = fraw.at[pl.ds(NDEV * core, NDEV), pl.ds(at, size)]
                    z = praw.at[:, pl.ds(to, size)]
                else:
                    a = src.at[pl.ds(at, size)]
                    z = dst.at[pl.ds(to, size)]
                out.append(
                    remote(
                        a,
                        z,
                        sem_init_send.at[5 + 2 * n + core],
                        sem_halo.at[side, n],
                        slab * 2 + core,
                        d,
                    )
                )
        return out

    def cross_copies():
        return halo_copies(
            1 - c,
            cross,
            ((OWN - NEAR) * c, jnp.where(c == 0, E, O - NEAR)),
            (jnp.where(c == 0, NEAR, OWN - K), jnp.where(c == 0, E + NEAR, 0)),
            (0, 1),
        )

    phase("c_sends")

    @pl.when(has_cross)
    def _():
        for cp in cross_copies():
            cp.start()

    for cp in part_copies():
        cp.start()

    def wait_halo(only):
        @pl.when(has_low)
        def _():
            for cp in halo_copies(0, s, (OWN - NEAR, O - NEAR), (OWN - K, 0), (0,), only):
                cp.wait_recv()

        @pl.when(has_high)
        def _():
            for cp in halo_copies(1, s, (0, E), (NEAR, E + NEAR), (0,), only):
                cp.wait_recv()

    def row_of(ref, l, y):
        return ref[l, pl.ds(y, HV, stride=yh), :]

    def spread_rows(dst, l, idx, rows=None):
        for y in range(yh if rows is None else rows):
            dst[l, y] = row_of(c_tmp, idx, y)

    def faces_layer(l, src, diag, dd, dx, dy, dz, dm, at):
        mid = src[l]
        xp = 0.5 * (mid + src[l + 1])
        xm = 0.5 * (mid + src[l - 1])
        up = jnp.where(row_c == ny - 1, 0.0, pltpu.roll(mid, ny - 1, 0))
        dn = jnp.where(row_c == 0, 0.0, pltpu.roll(mid, 1, 0))
        yp = 0.5 * (mid + up)
        ym = 0.5 * (mid + dn)
        rt = jnp.where(lane_c == LANES - 1, 0.0, pltpu.roll(mid, LANES - 1, 1))
        lf = jnp.where(lane_c == 0, 0.0, pltpu.roll(mid, 1, 1))
        zp = 0.5 * (mid + rt)
        zm = 0.5 * (mid + lf)
        total = xp + xm + yp + ym + zp + zm
        if diag is not None:
            total = total + diag[l]
        c_tmp[at, 0:ny] = total
        c_tmp[at + 1, 0:ny] = xp
        c_tmp[at + 2, 0:ny] = ym
        c_tmp[at + 2, ny : ny + SUB] = jnp.broadcast_to(
            0.5 * mid[ny - 1 : ny], (SUB, LANES)
        )
        c_tmp[at + 3, 0:ny] = jnp.where(lane_c == LANES - 1, 0.0, zp)
        c_tmp[at + 4, 0:ny] = jnp.where(lane_c == 0, 0.0, zm)
        return lambda: (
            spread_rows(dd, l, at),
            spread_rows(dx, l, at + 1),
            spread_rows(dy, l, at + 2, yh + 1),
            spread_rows(dz, l, at + 3),
            spread_rows(dm, l, at + 4),
        )

    def faces(lo, n):
        def layer(i, carry):
            l = lo + i
            done = (
                faces_layer(l, c_perm, c_diag, pd, px, py, pz, pm, 0),
                faces_layer(l, c_shear, None, ed, ex, ey, ez, em, 5),
            )
            for y in range(yh):
                hb[l, y] = row_of(c_hb, l, y)
                st[l, y] = row_of(c_stab, l, y)
            for make in done:
                make()
            return carry

        lax.fori_loop(0, n, layer, 0)

    def x_faces(l):
        c_tmp[1, 0:ny] = 0.5 * (c_perm[l] + c_perm[l + 1])
        c_tmp[6, 0:ny] = 0.5 * (c_shear[l] + c_shear[l + 1])
        spread_rows(px, l, 1)
        spread_rows(ex, l, 6)

    def source(lo, n, raw=praw, first=0, shift=0, layers=LT):
        flat = raw.reshape(raw.shape[0] * layers * ny, LANES)

        def layer(i, carry):
            l = lo + i
            for q in range(NB):
                for y in range(yh):
                    row = ((first + q) * layers + (l - shift)) * ny + y
                    f[q, l, y] = flat[pl.ds(row, HV, stride=yh), :]
            return carry

        lax.fori_loop(0, n, layer, 0)

    phase("d_own")
    faces(own_at + 1, OWN - 2)
    source(own_at, OWN, fraw, NDEV * c, own_at, OWN)
    phase("d_wait_part")
    parts = part_copies()
    for i in (0, 1):
        parts[i].wait_recv()
    phase("d_other")
    other_at = O + OWN * (1 - c)
    tables(other_at, OWN)
    faces(jnp.where(c == 0, O + OWN - 1, O + 1), OWN)
    for i in (2, 3, 4):
        parts[i].wait_recv()
    source(other_at, OWN)
    phase("d_wait_near")
    wait_halo((0, 1))
    tables(O - NEAR, NEAR)
    tables(E, NEAR)
    faces(O - 1, 2)
    faces(E - 1, 2)
    x_faces(O - 2)
    phase("d_near")
    wait_halo((2,))
    source(O - NEAR, NEAR)
    source(E, NEAR)

    def far_layers():
        wait_halo((3, 4))
        tables(0, K - NEAR)
        tables(E + NEAR, K - NEAR)
        faces(1, K - NEAR)
        faces(E + 1, K - NEAR)
        x_faces(0)
        wait_halo((5,))
        source(0, K - NEAR)
        source(E + NEAR, K - NEAR)

    class Rows:
        def __init__(self, ref, l0, pre=()):
            self.ref, self.l0, self.pre, self.got = ref, l0, pre, {}

        def load(self, g, y):
            return self.ref[(*self.pre, self.l0 + g, y)]

        def __call__(self, g, y):
            if (g, y) not in self.got:
                if y == -1:
                    self.got[g, y] = jnp.where(
                        part_of > 0, pltpu.roll(self(g, yh - 1), ND, 0), 0.0
                    )
                elif y == yh:
                    self.got[g, y] = jnp.where(
                        part_of < HV - 1, pltpu.roll(self(g, 0), SUB - ND, 0), 0.0
                    )
                else:
                    self.got[g, y] = self.load(g, y)
            return self.got[g, y]

    class Made(Rows):
        def __init__(self, make):
            self.make, self.got = make, {}

        def load(self, g, y):
            return self.make(g, y)

    def left(x):
        return pltpu.roll(x, 1, 1)

    def right(x):
        return pltpu.roll(x, LANES - 1, 1)

    p_ops = (pd, px, py, pz, pm)
    e_ops = (ed, ex, ey, ez, em)

    def group(ops, vals, l0, n, emit):
        cd, cx, cy, cz, cm = (Rows(o, l0).load for o in ops)
        cx, cy = Rows(ops[1], l0), Made(cy)
        for y in range(yh):
            for g in range(n):
                co = [
                    op(g, y) for op in (cd, cz, cm)
                ]
                c_up = ops[2][l0 + g, y + 1]
                c_dn = ops[2][l0 + g, y]
                for k, val in enumerate(vals):
                    x = val(g, y)
                    out = co[0] * x
                    out = out - co[1] * right(x)
                    out = out - co[2] * left(x)
                    out = out - cx(g, y) * val(g + 1, y)
                    out = out - cx(g - 1, y) * val(g - 1, y)
                    out = out - c_up * val(g, y + 1)
                    out = out - c_dn * val(g, y - 1)
                    emit(k, g, y, x, out)

    def own_loop(n, body, init):
        return lax.fori_loop(0, NL // n, lambda i, a: body(O + i * n, n, a), init)

    def both_halos(k, far, body, outs):
        n = k - far
        body(O - k, n)
        body(E + far, n)

        def clear(at):
            for ref, pre in outs:
                for g in range(n):
                    for y in range(yh):
                        ref[(*pre, at + g, y)] = zero8

        @pl.when(jnp.logical_not(has_low))
        def _():
            clear(O - k)

        @pl.when(jnp.logical_not(has_high))
        def _():
            clear(E + far)

    def pres(q, comps):
        return [(q,)] if comps is None else [(q, k) for k in range(comps)]

    def first_pass(q, ops, src, dst, comps, n):
        pre = pres(q, comps)

        def body(l0, n, acc):
            acc = list(acc)

            def emit(k, g, y, x, out):
                dst[(*pre[k], l0 + g, y)] = out
                acc[0] = acc[0] + x * x
                acc[1] = acc[1] + x * out
                acc[2] = acc[2] + out * out

            group(ops, [Rows(src, l0, k) for k in pre], l0, n, emit)
            return tuple(acc)

        return own_loop(n, body, (zero8,) * 3)

    def halo_pass(q, ops, src, dst, comps, k, far=0):
        pre = pres(q, comps)

        def body(l0, n):
            def emit(kk, g, y, x, out):
                dst[(*pre[kk], l0 + g, y)] = out

            group(ops, [Rows(src, l0, kk) for kk in pre], l0, n, emit)

        both_halos(k, far, body, [(dst, p) for p in pre])

    def second_pass(q, ops, src, comps, n, dst=None):
        pre = pres(q, comps)

        def body(l0, n, acc):
            acc = list(acc)

            def emit(k, g, y, x, out):
                acc[0] = acc[0] + x * out
                if dst is not None:
                    dst[q, l0 + g, y] = out

            group(ops, [Rows(src, l0, k) for k in pre], l0, n, emit)
            return tuple(acc)

        return own_loop(n, body, (zero8,))

    def red_copy(r, j, slot):
        peer = lax.rem(s + j, ns)
        return remote(
            red_src.at[r],
            red_buf.at[r, slot],
            sem_red_send.at[r],
            sem_red.at[r],
            peer * 2 + c,
            d,
        )

    def whole(block, ssem, rsem):
        return remote(block, block, ssem, rsem, partner, d)

    def red_all(r):
        return whole(red_buf.at[r, pl.ds(0, ns - 1)], sem_red_send.at[r], sem_red.at[r])

    def red_start(r, moments):
        packed = jnp.concatenate([jnp.sum(acc, axis=0, keepdims=True) for acc in moments], axis=0)
        red_src[r] = packed
        red_buf[r, s] = packed
        for j in range(1, ns):
            red_copy(r, j, s).start()

    def red_wait(r):
        red_all(r).wait_recv()
        sums = [red_buf[r, j] for j in range(ns)]
        while len(sums) > 1:
            sums = [x + y for x, y in zip(sums[::2], sums[1::2])]
        total = jnp.sum(sums[0], axis=1, keepdims=True)
        return [jnp.broadcast_to(total[m : m + 1], (SUB, LANES)) for m in range(4)]

    def weights(moments):
        m0, m1, m2, m3 = moments
        a0 = m0 / m1
        rr = a0 * a0 * m2 - m0
        beta1 = 1.0 + rr / m0
        dw = beta1 * beta1 * m1 - 2.0 * beta1 * a0 * m2 + a0 * a0 * m3
        a1 = rr / dw
        return a0 + a1 * beta1, -a1 * a0

    def strip(q, buf, at, to, size, ssem, rsem):
        low = remote(
            buf.at[q, pl.ds(O + at, size)],
            buf.at[q, pl.ds(E + to, size)],
            ssem.at[q, 0],
            rsem.at[q, 1],
            jnp.where(has_low, t - 2, t + 2),
            d,
        )
        high = remote(
            buf.at[q, pl.ds(E - at - size, size)],
            buf.at[q, pl.ds(O - to - size, size)],
            ssem.at[q, 1],
            rsem.at[q, 0],
            jnp.where(has_high, t + 2, t - 2),
            d,
        )
        return low, high

    def strip_do(args, start=False, recv=False, sent=False):
        low, high = strip(*args)

        @pl.when(has_low)
        def _():
            if start:
                low.start()
            if recv:
                high.wait_recv()
            if sent:
                low.wait_send()

        @pl.when(has_high)
        def _():
            if start:
                high.start()
            if recv:
                low.wait_recv()
            if sent:
                high.wait_send()

    def f_strip(q):
        return q, f, NEAR, NEAR, K - NEAR, sem_f_send, sem_f

    def r_strip(q):
        return q, r2, 2, 2, 1, sem_r_send, sem_r

    me = d * 2 + c
    nq = 2 * nd
    per = NL // nq

    def gram_copy(bt, l, q, slot):
        return remote(
            ybuf.at[bt, per * q + l],
            grecv.at[slot, bt, l],
            sem_g_send.at[bt, l],
            sem_g.at[bt, l],
            s * 2 + lax.rem(q, 2),
            q // 2,
        )

    def gram_all(bt, l):
        return whole(
            grecv.at[pl.ds(0, nq - 1), bt, l], sem_g_send.at[bt, l], sem_g.at[bt, l]
        )

    def each(stage, *args):
        def go(q, a):
            stage(q, *args)
            return a

        lax.fori_loop(0, NB, go, 0)

    def save(q, at, pair):
        for i in range(2):
            wts[q, at + i] = pair[i]

    def begin(q, base):
        mo = first_pass(q, p_ops, f, w, None, PN)
        halo_pass(q, p_ops, f, w, None, 1)
        (m3,) = second_pass(q, p_ops, w, None, PN, v)
        red_start(base + q, (*mo, m3))

    def begin_far(q, idx):
        @pl.when(idx > 0)
        def _():
            strip_do(f_strip(q), recv=True)

        halo_pass(q, p_ops, f, w, None, K - 1, 1)
        halo_pass(q, p_ops, w, v, None, 2)

    def displace(q, base):
        y0, y1 = weights(red_wait(base + q))
        save(q, 0, (y0, y1))

        def press(i, a):
            for g in range(13):
                l = 1 + 13 * i + g
                for y in range(yh):
                    p1[q, l, y] = y0 * f[q, l, y] + y1 * w[q, l, y]
            return a

        lax.fori_loop(0, (LT - 2) // 13, press, 0)

        def grad(i, a):
            l0 = 2 + 8 * i
            val = Rows(p1, l0, (q,))
            for y in range(yh):
                for g in range(8):
                    coef = hb[l0 + g, y]
                    x = val(g, y)
                    b[q, 0, l0 + g, y] = coef * (val(g + 1, y) - val(g - 1, y))
                    b[q, 1, l0 + g, y] = coef * (val(g, y + 1) - val(g, y - 1))
                    b[q, 2, l0 + g, y] = coef * (
                        jnp.where(last_z, 0.0, right(x)) - jnp.where(first_z, 0.0, left(x))
                    )
            return a

        lax.fori_loop(0, (LT - 4) // 8, grad, 0)
        mo = first_pass(q, e_ops, b, we, 3, EN)
        halo_pass(q, e_ops, b, we, 3, 1)
        (m3,) = second_pass(q, e_ops, we, 3, EN)
        red_start(base + NB + q, (*mo, m3))

    def displace_far(q):
        halo_pass(q, e_ops, b, we, 3, K - 3, 1)

    def again(q, base, idx):
        z0, z1 = weights(red_wait(base + NB + q))
        y0, y1 = wts[q, 0], wts[q, 1]

        def resid(l0, n, a):
            def flow(k):
                def make(g, y):
                    l = l0 + g
                    return hb[l, y] * (z0 * b[q, k, l, y] + z1 * we[q, k, l, y])

                return Made(make)

            fx, fy, fz = flow(0), flow(1), flow(2)
            for y in range(yh):
                for g in range(n):
                    l = l0 + g
                    tz = fz(g, y)
                    div = fx(g - 1, y) - fx(g + 1, y)
                    div = div + (fy(g, y - 1) - fy(g, y + 1))
                    div = div + (
                        jnp.where(first_z, 0.0, left(tz)) - jnp.where(last_z, 0.0, right(tz))
                    )
                    image = y0 * w[q, l, y] + y1 * v[q, l, y]
                    r2[q, l, y] = f[q, l, y] - div + st[l, y] * p1[q, l, y] - image
            return a

        own_loop(8, resid, 0)
        both_halos(2, 0, lambda l0, n: resid(l0, n, 0), [(r2, (q,))])
        mo = first_pass(q, p_ops, r2, w2, None, PN)

        @pl.when(idx == 0)
        def _():
            strip_do(r_strip(q), start=True)

        halo_pass(q, p_ops, r2, w2, None, 1)
        (m3,) = second_pass(q, p_ops, w2, None, PN)
        red_start(base + 2 * NB + q, (*mo, m3))

    def again_far(q):
        strip_do(r_strip(q), recv=True, sent=True)
        halo_pass(q, p_ops, r2, w2, None, 2, 1)

    def close(q, base, idx):
        @pl.when(idx == 0)
        def _():
            again_far(q)

        x0, x1 = weights(red_wait(base + 2 * NB + q))

        def total(l, y):
            return p1[q, l, y] + x0 * r2[q, l, y] + x1 * w2[q, l, y]

        @pl.when(idx == 0)
        def _():
            def update(i, a):
                for g in range(4):
                    l = O - NEAR + 4 * i + g
                    for y in range(yh):
                        f[q, l, y] = total(l, y) * row_of(c_obs, l, y)
                return a

            lax.fori_loop(0, (NL + 2 * NEAR) // 4, update, 0)
            strip_do(f_strip(q), start=True)
            begin(q, base + NB * 3)

        @pl.when(idx > 0)
        def _():
            def finish(i, a):
                for g in range(4):
                    l = 4 * i + g
                    for y in range(yh):
                        ybuf[q, l, y] = total(O + l, y) * row_of(c_bs, O + l, y)
                return a

            lax.fori_loop(0, NL // 4, finish, 0)
            for l in range(per):
                for j in range(1, nq):
                    gram_copy(q, l, lax.rem(me + j, nq), me).start()

    def solve(idx, a):
        base = idx * NB * 3
        @pl.when(idx == 0)
        def _():
            far_layers()

        with jax.named_scope("g_far"):
            each(begin_far, idx)
        with jax.named_scope("h_E"):
            each(displace, base)
        with jax.named_scope("h_Efar"):
            each(displace_far)
        with jax.named_scope("i_P2"):
            each(again, base, idx)

        with jax.named_scope("j_far"):

            @pl.when(idx == 0)
            def _():
                wait_halo((6,))

        with jax.named_scope("k_close"):
            each(close, base, idx)
        return a

    phase("g_P1")
    each(begin, 0)
    phase()
    lax.fori_loop(0, 2, solve, 0)

    phase("l_unpack")

    def unpack(dst, at):
        flat = dst.reshape(NDEV * OWN * ny, LANES)

        def layer(i, a):
            for q in range(NB):
                for y in range(yh):
                    row = (q * OWN + i) * ny + y
                    flat[pl.ds(row, HV, stride=yh), :] = ybuf[q, at + i, y]
            return a

        lax.fori_loop(0, OWN, layer, 0)

    def own_gram(i, a):
        for q in range(NB):
            for y in range(yh):
                grecv[me, q, i, y] = ybuf[q, per * me + i, y]
        return a

    unpack(hraw, OWN * (1 - c))
    unpack(hout, OWN * c)
    swap = remote(hraw, hin, sem_h.at[0], sem_h.at[1], partner, d)
    swap.start()
    lax.fori_loop(0, per, own_gram, 0)
    put = pltpu.make_async_copy(hout, hess.at[pl.ds(NDEV * c, NDEV)], sem_out.at[0])
    put.start()
    put_in = pltpu.make_async_copy(hin, hess.at[pl.ds(NDEV * (1 - c), NDEV)], sem_out.at[1])

    ndir = nq * NDEV
    step = per * yh * SUB
    gflat = grecv.reshape(ndir * step, LANES)
    g_all = jnp.zeros((ndir, ndir), F32)
    for l in range(per):
        phase("m_gramwait")
        for q in range(NB):
            gram_all(q, l).wait_recv()
        if l == 0:
            swap.wait_recv()
            put_in.start()
        phase("m_gramdot")
        for y in range(yh):
            z = jnp.concatenate(
                [
                    gflat[pl.ds((l * yh + y) * SUB + h, ndir, stride=step), :]
                    for h in range(SUB)
                ],
                axis=1,
            )
            g_all = g_all + lax.dot_general(
                z,
                z,
                (((1,), (1,)), ((), ())),
                precision=lax.Precision.HIGHEST,
                preferred_element_type=F32,
            )
    packed = jnp.concatenate(
        [g_all[k * SUB : (k + 1) * SUB] for k in range(ndir // SUB)], axis=1
    )

    phase("n_ga")
    ga_src[...] = packed
    ga_buf[s] = packed

    def ga_copy(j, slot):
        peer = lax.rem(s + j, ns)
        return remote(
            ga_src, ga_buf.at[slot], sem_ga.at[0], sem_ga.at[1], peer * 2 + c, d
        )

    for j in range(1, ns):
        ga_copy(j, s).start()
    ga_all = whole(ga_buf.at[pl.ds(0, ns - 1)], sem_ga.at[0], sem_ga.at[1])
    ga_all.wait_recv()
    total = ga_buf[0]
    for j in range(1, ns):
        total = total + ga_buf[j]
    phase("n_gb")
    gb_src[...] = total
    gb_buf[me] = total

    def gb_copy(j, slot):
        q = lax.rem(me + j, nq)
        return remote(
            gb_src,
            gb_buf.at[slot],
            sem_gb.at[0],
            sem_gb.at[1],
            s * 2 + lax.rem(q, 2),
            q // 2,
        )

    for j in range(1, nq):
        gb_copy(j, me).start()
    gb_all = whole(gb_buf.at[pl.ds(0, nq - 1)], sem_gb.at[0], sem_gb.at[1])
    gb_all.wait_recv()
    total = gb_buf[0]
    for j in range(1, nq):
        total = total + gb_buf[j]
    total = total * (1.0 / cells)
    for k in range(ndir // SUB):
        row = total if k == 0 else pltpu.roll(total, LANES - ndir * k, 1)
        gram[k * SUB : (k + 1) * SUB] = row

    phase("o_drain")
    swap.wait_send()
    put.wait()
    put_in.wait()
    for cp in part_copies():
        cp.wait_send()

    @pl.when(has_cross)
    def _():
        for cp in cross_copies():
            cp.wait_send()

    def red_sent(r, a):
        red_all(r).wait_send()
        return a

    lax.fori_loop(0, NRED, red_sent, 0)

    def batch_sent(q, a):
        strip_do(f_strip(q), sent=True)
        for l in range(per):
            gram_all(q, l).wait_send()
        return a

    lax.fori_loop(0, NB, batch_sent, 0)
    ga_all.wait_send()
    gb_all.wait_send()
    phase()


PN = 16
EN = 8


AHEAD = 3


def last_kernel(gram, h_in, r_out, h_out, buf, sems):
    parts = h_in.shape[0] // 2
    at = [pl.ds(2 * i, 2) for i in range(parts)]
    into = [pltpu.make_async_copy(h_in.at[p], buf.at[p], sems.at[0, i]) for i, p in enumerate(at)]
    out = [pltpu.make_async_copy(buf.at[p], h_out.at[p], sems.at[1, i]) for i, p in enumerate(at)]
    for cp in into:
        cp.start()
    n = r_out.shape[0]
    lane = lax.broadcasted_iota(jnp.int32, (1, LANES), 1)
    a = gram[...]

    def wide(x, j):
        return jnp.broadcast_to(x[:, j : j + 1], (n, LANES))

    cols = {j: (wide(a, j), 0) for j in range(AHEAD)}
    done = []
    for j in range(n):
        col, first = cols.pop(j)
        for m in range(first, j):
            col = col - done[m] * done[m][j : j + 1]
        inv = lax.rsqrt(col[j : j + 1])
        inv = inv * (1.5 - 0.5 * col[j : j + 1] * inv * inv)
        col = col * inv
        done.append(col)
        row = a[j : j + 1] * inv
        r_out[j : j + 1] = jnp.where(lane >= j, row, 0.0)[:, 0:n]
        a = a - col * row
        if j + AHEAD < n:
            cols[j + AHEAD] = (wide(a, j + AHEAD), j + 1)
        if j % 4 == 3 and j // 4 < parts:
            into[j // 4].wait()
            out[j // 4].start()
    for cp in out:
        cp.wait()


def solution(mesh):
    ns = mesh.shape["tile"] // 2
    nd = mesh.shape["dir"]
    nq = 2 * nd
    ndir = nq * NDEV

    def body(probes, bs, obs, perm, mat, storage, alpha, bulk, shear):
        ny, nz = probes.shape[2:]
        yh = ny // HV
        per = NL // nq
        cells = OWN * 2 * ns * ny * nz
        vm = pl.BlockSpec(memory_space=pltpu.VMEM)
        sm = pl.BlockSpec(memory_space=pltpu.SMEM)
        anywhere = pl.BlockSpec(memory_space=pl.ANY)

        def compact(kind=F32):
            return pltpu.VMEM((LT, ny, nz), kind)

        def wide(rows=yh, pre=()):
            return pltpu.VMEM((*pre, LT, rows, SUB, nz), F32)

        dma = pltpu.SemaphoreType.DMA
        field = wide(pre=(NB,))
        scratch = [
            pltpu.VMEM(probes.shape, F32),
            *[pltpu.VMEM(x.shape, x.dtype) for x in (bs, obs, perm, mat)],
            pltpu.VMEM(probes.shape, F32),
            pltpu.VMEM((NDEV, LT, ny, nz), F32),
            compact(),
            compact(),
            compact(),
            compact(jnp.int32),
            compact(),
            compact(),
            compact(),
            compact(),
            pltpu.VMEM((10, ny + SUB, nz), F32),
            *[wide(), wide(), wide(yh + 1), wide(), wide()] * 2,
            wide(),
            wide(),
            field,
            field,
            field,
            field,
            wide(pre=(NB, 3)),
            wide(pre=(NB, 3)),
            field,
            field,
            pltpu.VMEM((NB, NL, yh, SUB, nz), F32),
            *[pltpu.VMEM((NDEV, OWN, ny, nz), F32)] * 3,
            pltpu.VMEM((nq, NB, per, yh, SUB, nz), F32),
            pltpu.VMEM((NB, 2, SUB, nz), F32),
            pltpu.VMEM((NRED, 4, nz), F32),
            pltpu.VMEM((NRED, ns, 4, nz), F32),
            pltpu.VMEM((SUB, nz), F32),
            pltpu.VMEM((ns, SUB, nz), F32),
            pltpu.VMEM((SUB, nz), F32),
            pltpu.VMEM((nq, SUB, nz), F32),
            dma((5 + 14,)),
            dma((5,)),
            dma((2, 7)),
            dma((NRED,)),
            dma((NRED,)),
            dma((2,)),
            dma((2,)),
            dma((NB, per)),
            dma((NB, per)),
            dma((2,)),
            dma((NB, 2)),
            dma((NB, 2)),
            dma((NB, 2)),
            dma((NB, 2)),
            dma((5,)),
            dma((2,)),
        ]
        hess, gram = pl.pallas_call(
            functools.partial(kernel, ns, nd, cells),
            out_shape=(
                jax.ShapeDtypeStruct(probes.shape, F32),
                jax.ShapeDtypeStruct((ndir, nz), F32),
            ),
            in_specs=[anywhere] * 5 + [sm] * 4,
            out_specs=(anywhere, vm),
            scratch_shapes=scratch,
            compiler_params=pltpu.CompilerParams(
                collective_id=0, has_side_effects=True, vmem_limit_bytes=67043328,
            ),
            name="solve",
        )(probes, bs, obs, perm, mat, storage, alpha, bulk, shear)
        r_factor, hess = pl.pallas_call(
            last_kernel,
            out_shape=(
                jax.ShapeDtypeStruct((ndir, ndir), F32),
                jax.ShapeDtypeStruct(probes.shape, F32),
            ),
            in_specs=[vm, anywhere],
            out_specs=(vm, anywhere),
            scratch_shapes=[pltpu.VMEM(probes.shape, F32), dma((2, probes.shape[0] // 2))],
            name="factor",
        )(gram, hess)
        return hess, r_factor

    return jax.shard_map(
        body,
        mesh=mesh,
        in_specs=(
            P("dir", "tile", None, None),
            P("tile", None, None),
            P("tile", None, None),
            P("tile", None, None),
            P("tile", None, None),
            P(),
            P(),
            P(),
            P(),
        ),
        out_specs=(P("dir", "tile", None, None), P()),
        check_vma=False,
    )
```

```python
import functools

import jax
import jax.numpy as jnp
from jax import lax
from jax.experimental import pallas as pl
from jax.experimental.pallas import tpu as pltpu
from jax.sharding import PartitionSpec as P

MESH = pl.DeviceIdType.MESH
F32 = jnp.float32
NCLASS = 8
LANES = 128
SUB = 8
OWN = 8
NL = 16
K = 6
O = K
E = K + NL
LT = NL + 2 * K
NB = 4
HV = 8
ND = SUB // HV
NDEV = NB * ND
NEAR = 2
NRED = 6 * NB


def kernel(
    ns,
    nd,
    cells,
    probes_at,
    bs_at,
    obs_at,
    perm_at,
    mat_at,
    t_storage,
    t_alpha,
    t_bulk,
    t_shear,
    hess,
    gram,
    probes,
    bs_in,
    obs_in,
    perm_in,
    mat_in,
    fraw,
    praw,
    c_bs,
    c_obs,
    c_perm,
    c_mat,
    c_diag,
    c_stab,
    c_hb,
    c_shear,
    c_tmp,
    pd,
    px,
    py,
    pz,
    pm,
    ed,
    ex,
    ey,
    ez,
    em,
    hb,
    st,
    f,
    w,
    v,
    p1,
    b,
    we,
    r2,
    w2,
    ybuf,
    hraw,
    hin,
    hout,
    grecv,
    wts,
    red_src,
    red_buf,
    ga_src,
    ga_buf,
    gb_src,
    gb_buf,
    sem_init_send,
    sem_part,
    sem_halo,
    sem_red_send,
    sem_red,
    sem_ga,
    sem_gb,
    sem_g_send,
    sem_g,
    sem_h,
    sem_f_send,
    sem_f,
    sem_r_send,
    sem_r,
    sem_in,
    sem_out,
):
    scope = []

    def phase(name=None):
        if scope:
            scope.pop().__exit__(None, None, None)
        if name is not None:
            scope.append(jax.named_scope(name))
            scope[0].__enter__()

    phase("a_start")
    ny = probes.shape[2]
    yh = ny // HV
    t = lax.axis_index("tile")
    d = lax.axis_index("dir")
    s = t // 2
    c = lax.rem(t, 2)
    partner = s * 2 + (1 - c)
    has_low = s > 0
    has_high = s < ns - 1

    barrier = pltpu.get_barrier_semaphore()

    def greet(tile, dr):
        pl.semaphore_signal(barrier, inc=1, device_id=(tile, dr), device_id_type=MESH)

    cross = jnp.where(c == 0, s - 1, s + 1)
    has_cross = jnp.where(c == 0, has_low, has_high)
    for j in range(1, ns):
        greet(lax.rem(s + j, ns) * 2 + c, d)
    greet(partner, d)
    for j in range(1, nd):
        dj = lax.rem(d + j, nd)
        greet(t, dj)
        greet(partner, dj)

    @pl.when(has_cross)
    def _():
        greet(cross * 2 + (1 - c), d)

    loads = [
        pltpu.make_async_copy(src, dst, sem_in.at[i])
        for i, (src, dst) in enumerate(
            (
                (mat_at, mat_in),
                (bs_at, bs_in),
                (probes_at, probes),
                (perm_at, perm_in),
                (obs_at, obs_in),
            )
        )
    ]
    for cp in loads:
        cp.start()

    own_at = O + OWN * c
    zero8 = jnp.zeros((SUB, LANES), F32)
    zc = jnp.zeros((ny, LANES), F32)
    zi = jnp.zeros((ny, LANES), jnp.int32)

    def zero_side(lo):
        def layer(i, carry):
            l = lo + i
            c_perm[l] = zc
            c_obs[l] = zc
            c_mat[l] = zi
            for dd in range(NDEV):
                praw[dd, l] = zc
            for q in range(NB):
                for y in range(yh):
                    w[q, l, y] = zero8
                    v[q, l, y] = zero8
                    r2[q, l, y] = zero8
                    w2[q, l, y] = zero8
                    for k in range(3):
                        we[q, k, l, y] = zero8
            return carry

        lax.fori_loop(0, K, layer, 0)

    @pl.when(jnp.logical_not(has_low))
    def _():
        zero_side(0)

    @pl.when(jnp.logical_not(has_high))
    def _():
        zero_side(E)

    for cp in loads:
        cp.wait()

    def products(l, a):
        sens = bs_in[l]
        for dd in range(2 * NDEV):
            fraw[dd, l] = probes[dd, l] * sens
        c_bs[own_at + l] = sens
        c_obs[own_at + l] = obs_in[l]
        c_perm[own_at + l] = perm_in[l]
        c_mat[own_at + l] = mat_in[l]
        return a

    lax.fori_loop(0, OWN, products, 0)

    lane = lax.broadcasted_iota(jnp.int32, (SUB, LANES), 1)
    sub = lax.broadcasted_iota(jnp.int32, (SUB, LANES), 0)
    part_of = sub // ND
    lane_c = lax.broadcasted_iota(jnp.int32, (ny, LANES), 1)
    row_c = lax.broadcasted_iota(jnp.int32, (ny, LANES), 0)
    last_z = lane == LANES - 1
    first_z = lane == 0

    def tables(lo, n):
        def layer(i, carry):
            l = lo + i
            m = c_mat[l]
            inside = jnp.logical_and(
                jnp.logical_or(has_low, l >= O), jnp.logical_or(has_high, l < E)
            )
            gate = jnp.where(inside, F32(1.0), F32(0.0))

            def look(table):
                val = jnp.full((ny, LANES), table[0], F32)
                for k in range(1, NCLASS):
                    val = jnp.where(m == k, table[k], val)
                return val

            biot = look(t_alpha)
            stab = biot * biot / look(t_bulk)
            c_stab[l] = stab
            c_diag[l] = (look(t_storage) + stab) * gate
            c_hb[l] = 0.5 * biot * gate
            c_shear[l] = look(t_shear) * gate
            return carry

        lax.fori_loop(0, n, layer, 0)

    phase("a_tables")
    tables(own_at, OWN)

    phase("b_barrier")
    pl.semaphore_wait(barrier, (ns - 1) + 1 + 2 * (nd - 1) + jnp.where(has_cross, 1, 0))

    def remote(src, dst, ssem, rsem, tile, dr):
        return pltpu.make_async_remote_copy(
            src_ref=src,
            dst_ref=dst,
            send_sem=ssem,
            recv_sem=rsem,
            device_id=(tile, dr),
            device_id_type=MESH,
        )

    def part_copies():
        pairs = ((perm_in, c_perm), (mat_in, c_mat), (None, praw), (bs_in, c_bs), (obs_in, c_obs))
        out = []
        for i, (src, dst) in enumerate(pairs):
            if src is None:
                src = fraw.at[pl.ds(NDEV * (1 - c), NDEV)]
                dst = dst.at[:, pl.ds(own_at, OWN)]
            else:
                dst = dst.at[pl.ds(own_at, OWN)]
            out.append(remote(src, dst, sem_init_send.at[i], sem_part.at[i], partner, d))
        return out

    def halo_copies(side, slab, near, far, cores, only=None):
        jobs = []
        for n, (src, dst) in enumerate(((perm_in, c_perm), (mat_in, c_mat), (None, praw))):
            jobs.append((n, src, dst, *near, NEAR))
        for n, (src, dst) in enumerate(((perm_in, c_perm), (mat_in, c_mat), (None, praw))):
            jobs.append((3 + n, src, dst, *far, K - NEAR))
        jobs.append((6, obs_in, c_obs, *near, NEAR))
        out = []
        for n, src, dst, at, to, size in jobs:
            if only is not None and n not in only:
                continue
            for core in cores:
                if src is None:
                    a = fraw.at[pl.ds(NDEV * core, NDEV), pl.ds(at, size)]
                    z = praw.at[:, pl.ds(to, size)]
                else:
                    a = src.at[pl.ds(at, size)]
                    z = dst.at[pl.ds(to, size)]
                out.append(
                    remote(
                        a,
                        z,
                        sem_init_send.at[5 + 2 * n + core],
                        sem_halo.at[side, n],
                        slab * 2 + core,
                        d,
                    )
                )
        return out

    def cross_copies():
        return halo_copies(
            1 - c,
            cross,
            ((OWN - NEAR) * c, jnp.where(c == 0, E, O - NEAR)),
            (jnp.where(c == 0, NEAR, OWN - K), jnp.where(c == 0, E + NEAR, 0)),
            (0, 1),
        )

    phase("c_sends")

    @pl.when(has_cross)
    def _():
        for cp in cross_copies():
            cp.start()

    for cp in part_copies():
        cp.start()

    def wait_halo(only):
        @pl.when(has_low)
        def _():
            for cp in halo_copies(0, s, (OWN - NEAR, O - NEAR), (OWN - K, 0), (0,), only):
                cp.wait_recv()

        @pl.when(has_high)
        def _():
            for cp in halo_copies(1, s, (0, E), (NEAR, E + NEAR), (0,), only):
                cp.wait_recv()

    def row_of(ref, l, y):
        return ref[l, pl.ds(y, HV, stride=yh), :]

    def spread_rows(dst, l, idx, rows=None):
        for y in range(yh if rows is None else rows):
            dst[l, y] = row_of(c_tmp, idx, y)

    def faces_layer(l, src, diag, dd, dx, dy, dz, dm, at):
        mid = src[l]
        xp = 0.5 * (mid + src[l + 1])
        xm = 0.5 * (mid + src[l - 1])
        up = jnp.where(row_c == ny - 1, 0.0, pltpu.roll(mid, ny - 1, 0))
        dn = jnp.where(row_c == 0, 0.0, pltpu.roll(mid, 1, 0))
        yp = 0.5 * (mid + up)
        ym = 0.5 * (mid + dn)
        rt = jnp.where(lane_c == LANES - 1, 0.0, pltpu.roll(mid, LANES - 1, 1))
        lf = jnp.where(lane_c == 0, 0.0, pltpu.roll(mid, 1, 1))
        zp = 0.5 * (mid + rt)
        zm = 0.5 * (mid + lf)
        total = xp + xm + yp + ym + zp + zm
        if diag is not None:
            total = total + diag[l]
        c_tmp[at, 0:ny] = total
        c_tmp[at + 1, 0:ny] = xp
        c_tmp[at + 2, 0:ny] = ym
        c_tmp[at + 2, ny : ny + SUB] = jnp.broadcast_to(
            0.5 * mid[ny - 1 : ny], (SUB, LANES)
        )
        c_tmp[at + 3, 0:ny] = jnp.where(lane_c == LANES - 1, 0.0, zp)
        c_tmp[at + 4, 0:ny] = jnp.where(lane_c == 0, 0.0, zm)
        return lambda: (
            spread_rows(dd, l, at),
            spread_rows(dx, l, at + 1),
            spread_rows(dy, l, at + 2, yh + 1),
            spread_rows(dz, l, at + 3),
            spread_rows(dm, l, at + 4),
        )

    def faces(lo, n):
        def layer(i, carry):
            l = lo + i
            done = (
                faces_layer(l, c_perm, c_diag, pd, px, py, pz, pm, 0),
                faces_layer(l, c_shear, None, ed, ex, ey, ez, em, 5),
            )
            for y in range(yh):
                hb[l, y] = row_of(c_hb, l, y)
                st[l, y] = row_of(c_stab, l, y)
            for make in done:
                make()
            return carry

        lax.fori_loop(0, n, layer, 0)

    def x_faces(l):
        c_tmp[1, 0:ny] = 0.5 * (c_perm[l] + c_perm[l + 1])
        c_tmp[6, 0:ny] = 0.5 * (c_shear[l] + c_shear[l + 1])
        spread_rows(px, l, 1)
        spread_rows(ex, l, 6)

    def source(lo, n, raw=praw, first=0, shift=0, layers=LT):
        flat = raw.reshape(raw.shape[0] * layers * ny, LANES)

        def layer(i, carry):
            l = lo + i
            for q in range(NB):
                for y in range(yh):
                    row = ((first + q) * layers + (l - shift)) * ny + y
                    f[q, l, y] = flat[pl.ds(row, HV, stride=yh), :]
            return carry

        lax.fori_loop(0, n, layer, 0)

    phase("d_own")
    faces(own_at + 1, OWN - 2)
    source(own_at, OWN, fraw, NDEV * c, own_at, OWN)
    phase("d_wait_part")
    parts = part_copies()
    for i in (0, 1):
        parts[i].wait_recv()
    phase("d_other")
    other_at = O + OWN * (1 - c)
    tables(other_at, OWN)
    faces(jnp.where(c == 0, O + OWN - 1, O + 1), OWN)
    for i in (2, 3, 4):
        parts[i].wait_recv()
    source(other_at, OWN)
    phase("d_wait_near")
    wait_halo((0, 1))
    tables(O - NEAR, NEAR)
    tables(E, NEAR)
    faces(O - 1, 2)
    faces(E - 1, 2)
    x_faces(O - 2)
    phase("d_near")
    wait_halo((2,))
    source(O - NEAR, NEAR)
    source(E, NEAR)

    def far_layers():
        wait_halo((3, 4))
        tables(0, K - NEAR)
        tables(E + NEAR, K - NEAR)
        faces(1, K - NEAR)
        faces(E + 1, K - NEAR)
        x_faces(0)
        wait_halo((5,))
        source(0, K - NEAR)
        source(E + NEAR, K - NEAR)

    class Rows:
        def __init__(self, ref, l0, pre=()):
            self.ref, self.l0, self.pre, self.got = ref, l0, pre, {}

        def load(self, g, y):
            return self.ref[(*self.pre, self.l0 + g, y)]

        def __call__(self, g, y):
            if (g, y) not in self.got:
                if y == -1:
                    self.got[g, y] = jnp.where(
                        part_of > 0, pltpu.roll(self(g, yh - 1), ND, 0), 0.0
                    )
                elif y == yh:
                    self.got[g, y] = jnp.where(
                        part_of < HV - 1, pltpu.roll(self(g, 0), SUB - ND, 0), 0.0
                    )
                else:
                    self.got[g, y] = self.load(g, y)
            return self.got[g, y]

    class Made(Rows):
        def __init__(self, make):
            self.make, self.got = make, {}

        def load(self, g, y):
            return self.make(g, y)

    def left(x):
        return pltpu.roll(x, 1, 1)

    def right(x):
        return pltpu.roll(x, LANES - 1, 1)

    p_ops = (pd, px, py, pz, pm)
    e_ops = (ed, ex, ey, ez, em)

    def group(ops, vals, l0, n, emit):
        cd, cx, cy, cz, cm = (Rows(o, l0).load for o in ops)
        cx, cy = Rows(ops[1], l0), Made(cy)
        for y in range(yh):
            for g in range(n):
                co = [
                    op(g, y) for op in (cd, cz, cm)
                ]
                c_up = ops[2][l0 + g, y + 1]
                c_dn = ops[2][l0 + g, y]
                for k, val in enumerate(vals):
                    x = val(g, y)
                    out = co[0] * x
                    out = out - co[1] * right(x)
                    out = out - co[2] * left(x)
                    out = out - cx(g, y) * val(g + 1, y)
                    out = out - cx(g - 1, y) * val(g - 1, y)
                    out = out - c_up * val(g, y + 1)
                    out = out - c_dn * val(g, y - 1)
                    emit(k, g, y, x, out)

    def own_loop(n, body, init):
        return lax.fori_loop(0, NL // n, lambda i, a: body(O + i * n, n, a), init)

    def both_halos(k, far, body, outs):
        n = k - far
        body(O - k, n)
        body(E + far, n)

        def clear(at):
            for ref, pre in outs:
                for g in range(n):
                    for y in range(yh):
                        ref[(*pre, at + g, y)] = zero8

        @pl.when(jnp.logical_not(has_low))
        def _():
            clear(O - k)

        @pl.when(jnp.logical_not(has_high))
        def _():
            clear(E + far)

    def pres(q, comps):
        return [(q,)] if comps is None else [(q, k) for k in range(comps)]

    def first_pass(q, ops, src, dst, comps, n):
        pre = pres(q, comps)

        def body(l0, n, acc):
            acc = list(acc)

            def emit(k, g, y, x, out):
                dst[(*pre[k], l0 + g, y)] = out
                acc[0] = acc[0] + x * x
                acc[1] = acc[1] + x * out
                acc[2] = acc[2] + out * out

            group(ops, [Rows(src, l0, k) for k in pre], l0, n, emit)
            return tuple(acc)

        return own_loop(n, body, (zero8,) * 3)

    def halo_pass(q, ops, src, dst, comps, k, far=0):
        pre = pres(q, comps)

        def body(l0, n):
            def emit(kk, g, y, x, out):
                dst[(*pre[kk], l0 + g, y)] = out

            group(ops, [Rows(src, l0, kk) for kk in pre], l0, n, emit)

        both_halos(k, far, body, [(dst, p) for p in pre])

    def second_pass(q, ops, src, comps, n, dst=None):
        pre = pres(q, comps)

        def body(l0, n, acc):
            acc = list(acc)

            def emit(k, g, y, x, out):
                acc[0] = acc[0] + x * out
                if dst is not None:
                    dst[q, l0 + g, y] = out

            group(ops, [Rows(src, l0, k) for k in pre], l0, n, emit)
            return tuple(acc)

        return own_loop(n, body, (zero8,))

    def red_copy(r, j, slot):
        peer = lax.rem(s + j, ns)
        return remote(
            red_src.at[r],
            red_buf.at[r, slot],
            sem_red_send.at[r],
            sem_red.at[r],
            peer * 2 + c,
            d,
        )

    def whole(block, ssem, rsem):
        return remote(block, block, ssem, rsem, partner, d)

    def red_all(r):
        return whole(red_buf.at[r, pl.ds(0, ns - 1)], sem_red_send.at[r], sem_red.at[r])

    def red_start(r, moments):
        packed = jnp.concatenate([jnp.sum(acc, axis=0, keepdims=True) for acc in moments], axis=0)
        red_src[r] = packed
        red_buf[r, s] = packed
        for j in range(1, ns):
            red_copy(r, j, s).start()

    def red_wait(r):
        red_all(r).wait_recv()
        sums = [red_buf[r, j] for j in range(ns)]
        while len(sums) > 1:
            sums = [x + y for x, y in zip(sums[::2], sums[1::2])]
        total = jnp.sum(sums[0], axis=1, keepdims=True)
        return [jnp.broadcast_to(total[m : m + 1], (SUB, LANES)) for m in range(4)]

    def weights(moments):
        m0, m1, m2, m3 = moments
        a0 = m0 / m1
        rr = a0 * a0 * m2 - m0
        beta1 = 1.0 + rr / m0
        dw = beta1 * beta1 * m1 - 2.0 * beta1 * a0 * m2 + a0 * a0 * m3
        a1 = rr / dw
        return a0 + a1 * beta1, -a1 * a0

    def strip(q, buf, at, to, size, ssem, rsem):
        low = remote(
            buf.at[q, pl.ds(O + at, size)],
            buf.at[q, pl.ds(E + to, size)],
            ssem.at[q, 0],
            rsem.at[q, 1],
            jnp.where(has_low, t - 2, t + 2),
            d,
        )
        high = remote(
            buf.at[q, pl.ds(E - at - size, size)],
            buf.at[q, pl.ds(O - to - size, size)],
            ssem.at[q, 1],
            rsem.at[q, 0],
            jnp.where(has_high, t + 2, t - 2),
            d,
        )
        return low, high

    def strip_do(args, start=False, recv=False, sent=False):
        low, high = strip(*args)

        @pl.when(has_low)
        def _():
            if start:
                low.start()
            if recv:
                high.wait_recv()
            if sent:
                low.wait_send()

        @pl.when(has_high)
        def _():
            if start:
                high.start()
            if recv:
                low.wait_recv()
            if sent:
                high.wait_send()

    def f_strip(q):
        return q, f, NEAR, NEAR, K - NEAR, sem_f_send, sem_f

    def r_strip(q):
        return q, r2, 2, 2, 1, sem_r_send, sem_r

    me = d * 2 + c
    nq = 2 * nd
    per = NL // nq

    def gram_copy(bt, l, q, slot):
        return remote(
            ybuf.at[bt, per * q + l],
            grecv.at[slot, bt, l],
            sem_g_send.at[bt, l],
            sem_g.at[bt, l],
            s * 2 + lax.rem(q, 2),
            q // 2,
        )

    def gram_all(bt, l):
        return whole(
            grecv.at[pl.ds(0, nq - 1), bt, l], sem_g_send.at[bt, l], sem_g.at[bt, l]
        )

    def each(stage, *args):
        def go(q, a):
            stage(q, *args)
            return a

        lax.fori_loop(0, NB, go, 0)

    def save(q, at, pair):
        for i in range(2):
            wts[q, at + i] = pair[i]

    def begin(q, base):
        mo = first_pass(q, p_ops, f, w, None, PN)
        halo_pass(q, p_ops, f, w, None, 1)
        (m3,) = second_pass(q, p_ops, w, None, PN, v)
        red_start(base + q, (*mo, m3))

    def begin_far(q, idx):
        @pl.when(idx > 0)
        def _():
            strip_do(f_strip(q), recv=True)

        halo_pass(q, p_ops, f, w, None, K - 1, 1)
        halo_pass(q, p_ops, w, v, None, 2)

    def displace(q, base):
        y0, y1 = weights(red_wait(base + q))
        save(q, 0, (y0, y1))

        def press(i, a):
            for g in range(13):
                l = 1 + 13 * i + g
                for y in range(yh):
                    p1[q, l, y] = y0 * f[q, l, y] + y1 * w[q, l, y]
            return a

        lax.fori_loop(0, (LT - 2) // 13, press, 0)

        def grad(i, a):
            l0 = 2 + 12 * i
            val = Rows(p1, l0, (q,))
            for y in range(yh):
                for g in range(12):
                    coef = hb[l0 + g, y]
                    x = val(g, y)
                    b[q, 0, l0 + g, y] = coef * (val(g + 1, y) - val(g - 1, y))
                    b[q, 1, l0 + g, y] = coef * (val(g, y + 1) - val(g, y - 1))
                    b[q, 2, l0 + g, y] = coef * (
                        jnp.where(last_z, 0.0, right(x)) - jnp.where(first_z, 0.0, left(x))
                    )
            return a

        lax.fori_loop(0, (LT - 4) // 12, grad, 0)
        mo = first_pass(q, e_ops, b, we, 3, EN)
        halo_pass(q, e_ops, b, we, 3, 1)
        (m3,) = second_pass(q, e_ops, we, 3, EN)
        red_start(base + NB + q, (*mo, m3))

    def displace_far(q):
        halo_pass(q, e_ops, b, we, 3, K - 3, 1)

    def again(q, base, idx):
        z0, z1 = weights(red_wait(base + NB + q))
        y0, y1 = wts[q, 0], wts[q, 1]

        def resid(l0, n, a):
            def flow(k):
                def make(g, y):
                    l = l0 + g
                    return hb[l, y] * (z0 * b[q, k, l, y] + z1 * we[q, k, l, y])

                return Made(make)

            fx, fy, fz = flow(0), flow(1), flow(2)
            for y in range(yh):
                for g in range(n):
                    l = l0 + g
                    tz = fz(g, y)
                    div = fx(g - 1, y) - fx(g + 1, y)
                    div = div + (fy(g, y - 1) - fy(g, y + 1))
                    div = div + (
                        jnp.where(first_z, 0.0, left(tz)) - jnp.where(last_z, 0.0, right(tz))
                    )
                    image = y0 * w[q, l, y] + y1 * v[q, l, y]
                    r2[q, l, y] = f[q, l, y] - div + st[l, y] * p1[q, l, y] - image
            return a

        own_loop(16, resid, 0)
        both_halos(2, 0, lambda l0, n: resid(l0, n, 0), [(r2, (q,))])
        mo = first_pass(q, p_ops, r2, w2, None, PN)

        @pl.when(idx == 0)
        def _():
            strip_do(r_strip(q), start=True)

        halo_pass(q, p_ops, r2, w2, None, 1)
        (m3,) = second_pass(q, p_ops, w2, None, PN)
        red_start(base + 2 * NB + q, (*mo, m3))

    def again_far(q):
        strip_do(r_strip(q), recv=True, sent=True)
        halo_pass(q, p_ops, r2, w2, None, 2, 1)

    def close(q, base, idx):
        @pl.when(idx == 0)
        def _():
            again_far(q)

        x0, x1 = weights(red_wait(base + 2 * NB + q))

        def total(l, y):
            return p1[q, l, y] + x0 * r2[q, l, y] + x1 * w2[q, l, y]

        @pl.when(idx == 0)
        def _():
            def update(i, a):
                for g in range(4):
                    l = O - NEAR + 4 * i + g
                    for y in range(yh):
                        f[q, l, y] = total(l, y) * row_of(c_obs, l, y)
                return a

            lax.fori_loop(0, (NL + 2 * NEAR) // 4, update, 0)
            strip_do(f_strip(q), start=True)
            begin(q, base + NB * 3)

        @pl.when(idx > 0)
        def _():
            def finish(i, a):
                for g in range(4):
                    l = 4 * i + g
                    for y in range(yh):
                        ybuf[q, l, y] = total(O + l, y) * row_of(c_bs, O + l, y)
                return a

            lax.fori_loop(0, NL // 4, finish, 0)
            for l in range(per):
                for j in range(1, nq):
                    gram_copy(q, l, lax.rem(me + j, nq), me).start()

    def solve(idx, a):
        base = idx * NB * 3
        @pl.when(idx == 0)
        def _():
            far_layers()

        with jax.named_scope("g_far"):
            each(begin_far, idx)
        with jax.named_scope("h_E"):
            each(displace, base)
        with jax.named_scope("h_Efar"):
            each(displace_far)
        with jax.named_scope("i_P2"):
            each(again, base, idx)

        with jax.named_scope("j_far"):

            @pl.when(idx == 0)
            def _():
                wait_halo((6,))

        with jax.named_scope("k_close"):
            each(close, base, idx)
        return a

    phase("g_P1")
    each(begin, 0)
    phase()
    lax.fori_loop(0, 2, solve, 0)

    phase("l_unpack")

    def unpack(dst, at):
        flat = dst.reshape(NDEV * OWN * ny, LANES)

        def layer(i, a):
            for q in range(NB):
                for y in range(yh):
                    row = (q * OWN + i) * ny + y
                    flat[pl.ds(row, HV, stride=yh), :] = ybuf[q, at + i, y]
            return a

        lax.fori_loop(0, OWN, layer, 0)

    def own_gram(i, a):
        for q in range(NB):
            for y in range(yh):
                grecv[me, q, i, y] = ybuf[q, per * me + i, y]
        return a

    unpack(hraw, OWN * (1 - c))
    unpack(hout, OWN * c)
    swap = remote(hraw, hin, sem_h.at[0], sem_h.at[1], partner, d)
    swap.start()
    lax.fori_loop(0, per, own_gram, 0)
    put = pltpu.make_async_copy(hout, hess.at[pl.ds(NDEV * c, NDEV)], sem_out.at[0])
    put.start()
    put_in = pltpu.make_async_copy(hin, hess.at[pl.ds(NDEV * (1 - c), NDEV)], sem_out.at[1])

    ndir = nq * NDEV
    step = per * yh * SUB
    gflat = grecv.reshape(ndir * step, LANES)
    g_all = jnp.zeros((ndir, ndir), F32)
    for l in range(per):
        phase("m_gramwait")
        for q in range(NB):
            gram_all(q, l).wait_recv()
        if l == 0:
            swap.wait_recv()
            put_in.start()
        phase("m_gramdot")
        for y in range(yh):
            z = jnp.concatenate(
                [
                    gflat[pl.ds((l * yh + y) * SUB + h, ndir, stride=step), :]
                    for h in range(SUB)
                ],
                axis=1,
            )
            g_all = g_all + lax.dot_general(
                z,
                z,
                (((1,), (1,)), ((), ())),
                precision=lax.Precision.HIGHEST,
                preferred_element_type=F32,
            )
    packed = jnp.concatenate(
        [g_all[k * SUB : (k + 1) * SUB] for k in range(ndir // SUB)], axis=1
    )

    phase("n_ga")
    ga_src[...] = packed
    ga_buf[s] = packed

    def ga_copy(j, slot):
        peer = lax.rem(s + j, ns)
        return remote(
            ga_src, ga_buf.at[slot], sem_ga.at[0], sem_ga.at[1], peer * 2 + c, d
        )

    for j in range(1, ns):
        ga_copy(j, s).start()
    ga_all = whole(ga_buf.at[pl.ds(0, ns - 1)], sem_ga.at[0], sem_ga.at[1])
    ga_all.wait_recv()
    total = ga_buf[0]
    for j in range(1, ns):
        total = total + ga_buf[j]
    phase("n_gb")
    gb_src[...] = total
    gb_buf[me] = total

    def gb_copy(j, slot):
        q = lax.rem(me + j, nq)
        return remote(
            gb_src,
            gb_buf.at[slot],
            sem_gb.at[0],
            sem_gb.at[1],
            s * 2 + lax.rem(q, 2),
            q // 2,
        )

    for j in range(1, nq):
        gb_copy(j, me).start()
    gb_all = whole(gb_buf.at[pl.ds(0, nq - 1)], sem_gb.at[0], sem_gb.at[1])
    gb_all.wait_recv()
    total = gb_buf[0]
    for j in range(1, nq):
        total = total + gb_buf[j]
    total = total * (1.0 / cells)
    for k in range(ndir // SUB):
        row = total if k == 0 else pltpu.roll(total, LANES - ndir * k, 1)
        gram[k * SUB : (k + 1) * SUB] = row

    phase("o_drain")
    swap.wait_send()
    put.wait()
    put_in.wait()
    for cp in part_copies():
        cp.wait_send()

    @pl.when(has_cross)
    def _():
        for cp in cross_copies():
            cp.wait_send()

    def red_sent(r, a):
        red_all(r).wait_send()
        return a

    lax.fori_loop(0, NRED, red_sent, 0)

    def batch_sent(q, a):
        strip_do(f_strip(q), sent=True)
        for l in range(per):
            gram_all(q, l).wait_send()
        return a

    lax.fori_loop(0, NB, batch_sent, 0)
    ga_all.wait_send()
    gb_all.wait_send()
    phase()


PN = 16
EN = 8


AHEAD = 3


def last_kernel(gram, h_in, r_out, h_out, buf, sems):
    parts = h_in.shape[0] // 2
    at = [pl.ds(2 * i, 2) for i in range(parts)]
    into = [pltpu.make_async_copy(h_in.at[p], buf.at[p], sems.at[0, i]) for i, p in enumerate(at)]
    out = [pltpu.make_async_copy(buf.at[p], h_out.at[p], sems.at[1, i]) for i, p in enumerate(at)]
    for cp in into:
        cp.start()
    n = r_out.shape[0]
    lane = lax.broadcasted_iota(jnp.int32, (1, LANES), 1)
    a = gram[...]

    def wide(x, j):
        return jnp.broadcast_to(x[:, j : j + 1], (n, LANES))

    cols = {j: (wide(a, j), 0) for j in range(AHEAD)}
    done = []
    for j in range(n):
        col, first = cols.pop(j)
        for m in range(first, j):
            col = col - done[m] * done[m][j : j + 1]
        inv = lax.rsqrt(col[j : j + 1])
        inv = inv * (1.5 - 0.5 * col[j : j + 1] * inv * inv)
        col = col * inv
        done.append(col)
        row = a[j : j + 1] * inv
        r_out[j : j + 1] = jnp.where(lane >= j, row, 0.0)[:, 0:n]
        a = a - col * row
        if j + AHEAD < n:
            cols[j + AHEAD] = (wide(a, j + AHEAD), j + 1)
        if j % 4 == 3 and j // 4 < parts:
            into[j // 4].wait()
            out[j // 4].start()
    for cp in out:
        cp.wait()


def solution(mesh):
    ns = mesh.shape["tile"] // 2
    nd = mesh.shape["dir"]
    nq = 2 * nd
    ndir = nq * NDEV

    def body(probes, bs, obs, perm, mat, storage, alpha, bulk, shear):
        ny, nz = probes.shape[2:]
        yh = ny // HV
        per = NL // nq
        cells = OWN * 2 * ns * ny * nz
        vm = pl.BlockSpec(memory_space=pltpu.VMEM)
        sm = pl.BlockSpec(memory_space=pltpu.SMEM)
        anywhere = pl.BlockSpec(memory_space=pl.ANY)

        def compact(kind=F32):
            return pltpu.VMEM((LT, ny, nz), kind)

        def wide(rows=yh, pre=()):
            return pltpu.VMEM((*pre, LT, rows, SUB, nz), F32)

        dma = pltpu.SemaphoreType.DMA
        field = wide(pre=(NB,))
        scratch = [
            pltpu.VMEM(probes.shape, F32),
            *[pltpu.VMEM(x.shape, x.dtype) for x in (bs, obs, perm, mat)],
            pltpu.VMEM(probes.shape, F32),
            pltpu.VMEM((NDEV, LT, ny, nz), F32),
            compact(),
            compact(),
            compact(),
            compact(jnp.int32),
            compact(),
            compact(),
            compact(),
            compact(),
            pltpu.VMEM((10, ny + SUB, nz), F32),
            *[wide(), wide(), wide(yh + 1), wide(), wide()] * 2,
            wide(),
            wide(),
            field,
            field,
            field,
            field,
            wide(pre=(NB, 3)),
            wide(pre=(NB, 3)),
            field,
            field,
            pltpu.VMEM((NB, NL, yh, SUB, nz), F32),
            *[pltpu.VMEM((NDEV, OWN, ny, nz), F32)] * 3,
            pltpu.VMEM((nq, NB, per, yh, SUB, nz), F32),
            pltpu.VMEM((NB, 2, SUB, nz), F32),
            pltpu.VMEM((NRED, 4, nz), F32),
            pltpu.VMEM((NRED, ns, 4, nz), F32),
            pltpu.VMEM((SUB, nz), F32),
            pltpu.VMEM((ns, SUB, nz), F32),
            pltpu.VMEM((SUB, nz), F32),
            pltpu.VMEM((nq, SUB, nz), F32),
            dma((5 + 14,)),
            dma((5,)),
            dma((2, 7)),
            dma((NRED,)),
            dma((NRED,)),
            dma((2,)),
            dma((2,)),
            dma((NB, per)),
            dma((NB, per)),
            dma((2,)),
            dma((NB, 2)),
            dma((NB, 2)),
            dma((NB, 2)),
            dma((NB, 2)),
            dma((5,)),
            dma((2,)),
        ]
        hess, gram = pl.pallas_call(
            functools.partial(kernel, ns, nd, cells),
            out_shape=(
                jax.ShapeDtypeStruct(probes.shape, F32),
                jax.ShapeDtypeStruct((ndir, nz), F32),
            ),
            in_specs=[anywhere] * 5 + [sm] * 4,
            out_specs=(anywhere, vm),
            scratch_shapes=scratch,
            compiler_params=pltpu.CompilerParams(
                collective_id=0, has_side_effects=True, vmem_limit_bytes=67043328,
            ),
            name="solve",
        )(probes, bs, obs, perm, mat, storage, alpha, bulk, shear)
        r_factor, hess = pl.pallas_call(
            last_kernel,
            out_shape=(
                jax.ShapeDtypeStruct((ndir, ndir), F32),
                jax.ShapeDtypeStruct(probes.shape, F32),
            ),
            in_specs=[vm, anywhere],
            out_specs=(vm, anywhere),
            scratch_shapes=[pltpu.VMEM(probes.shape, F32), dma((2, probes.shape[0] // 2))],
            name="factor",
        )(gram, hess)
        return hess, r_factor

    return jax.shard_map(
        body,
        mesh=mesh,
        in_specs=(
            P("dir", "tile", None, None),
            P("tile", None, None),
            P("tile", None, None),
            P("tile", None, None),
            P("tile", None, None),
            P(),
            P(),
            P(),
            P(),
        ),
        out_specs=(P("dir", "tile", None, None), P()),
        check_vma=False,
    )
```
